256 devices in a mesh: groups: 2 (over z), kv: 128 (over y, x, core).
Axes of the slice: x: 8, y: 8, z: 2, core: 2. Of those that a mesh axis runs over, the one named last changes fastest.
The devices are a block of a 8x8x16 slice.
Arguments:
- queries: bfloat16 [80, 18432], P('groups', 'kv'), parts along dimension 0, may hold values from -240 to 240
- latent_cache: bfloat16 [80, 16384, 576], P('groups', 'kv'), parts along dimension 0, may hold values from -6 to 6
- context_lengths: int32 [80], P('groups'), parts along dimension 0, may hold values from 128 to 16384, as said below
- value_up: bfloat16 [16384, 128], P('kv'), may hold values from -0.25 to 0.25
- out_proj: bfloat16 [4096, 7168], P('kv'), may hold values from -0.09375 to 0.09375
- residual: bfloat16 [80, 7168], P('groups', 'kv'), parts along dimension 0, may hold values from -0.75 to 0.75
- norm_gain: bfloat16 [7168], P('kv'), may hold values from 0.5 to 1.5
- expert_ids: int32 [80, 8], P('groups'), parts along dimension 0, may hold values from 0 to 255, all different within a row; in each aligned block of 40 rows (0 to 39, 40 to 79, ...) at most 2 rows name the same one
- gate_weights: float32 [80, 8], P('groups'), parts along dimension 0, may hold values from 0.05 to 0.5
Outputs:
- dispatched: bfloat16 [512, 2, 7168], P(('groups', 'kv')), parts along dimension 0
- slot_scale: float32 [512, 2], P(('groups', 'kv')), parts along dimension 0
- slot_gate: float32 [512, 2], P(('groups', 'kv')), parts along dimension 0
The draws below stay inside these ranges and needn't reach their ends.
There are 2 independent parts, one for each index of `groups`. The reference program is written for one: setup_inputs(seed, part) draws one part's arguments, and reference() takes and returns one part's arrays. A program takes and returns all parts, laid end to end along the dimension named above; an argument that names none is the same for every part. Nothing has to cross between parts.
Inputs may be any that keep to these rules, and one draw needn't show every extreme that they name: `context_lengths`: multiples of 128; some sequence is 16384 long. `expert_ids`: each token names 8 different experts; no expert is named by more than 2 tokens, a bound that some block reaches.
All inputs are finite; a program needn't handle non-finite values. Where the reference program divides by a largest or mean magnitude, that divisor is 1e-20 or more.
Results may differ from the reference program's by a relative error of at most 0.0069.
Values may be sent and summed in bfloat16 or wider, within the bound.
A program may use at most 64 MiB of HBM per device.

```python
import math
import jax
import jax.numpy as jnp
import numpy as np
from jax import lax

H = 32
LAT = 512
ROPE = 64
VD = 128
D = 7168
EXPERTS = 256
TOPK = 8
SEQS = 40
CTX_DEV = 128
BLOCK = 128
CTX = 16384
CAP = 2
N_KV = 128


def draw_queries(key, part):
    base_key = jax.random.fold_in(jax.random.fold_in(key, 11), 0)
    values = jnp.clip(jax.random.normal(base_key, (SEQS, H, LAT + ROPE), jnp.float32), -6.0, 6.0)
    return values.reshape(SEQS, H * (LAT + ROPE)).astype(jnp.bfloat16)


def draw_context_lengths(key, part):
    count_key, pick_key = jax.random.split(jax.random.fold_in(key, 7))
    blocks = jax.random.randint(count_key, (SEQS,), 1, CTX // BLOCK + 1)
    longest = jax.random.randint(pick_key, (), 0, SEQS)
    blocks = jnp.where(jnp.arange(SEQS) == longest, CTX // BLOCK, blocks)
    return (blocks * BLOCK).astype(jnp.int32)


def level_of(key, shape, cuts, least, high):
    def one(axis_at, shards_of):
        steps = jax.random.uniform(jax.random.fold_in(jax.random.fold_in(key, 6), axis_at), (shards_of,), jnp.float32, least / len(cuts), high / len(cuts))
        return jnp.repeat(jnp.exp(steps), shape[axis_at] // shards_of).reshape((-1,) + (1,) * (len(shape) - axis_at - 1))

    level = one(*cuts[0])
    for cut in cuts[1:]:
        level = level * one(*cut)
    return level


def assign_block(rng, own, number, rows, number_of, top, limit, skew):
    ranking = jax.random.permutation(rng, number_of)
    heavy_load, ordinary = shares(number_of, rows * top, limit, skew, True), shares(number_of, rows * top, limit, skew, False)
    places = jnp.arange(number_of)

    def named(lengths, rotation):
        used = int((lengths > 0).sum())
        fixed = max(1, used // 4)
        moved = fixed + (places - fixed + rotation * (used - fixed)) % max(1, number_of - fixed)
        return jnp.zeros((number_of,), jnp.int32).at[ranking[jnp.where(places < fixed, places, moved)]].set(jnp.asarray(lengths, jnp.int32))

    lengths = jnp.where(number % 4 == 0, named(heavy_load, number // 4), named(ordinary, number - number // 4 - 1))
    mixed = jax.random.permutation(jax.random.fold_in(own, 3), number_of)
    giver, sink = mixed[0:number_of // 2 * 2:2], mixed[1:number_of // 2 * 2:2]
    margin = jnp.minimum(lengths[giver] - 1, limit - lengths[sink]) // 2
    margin = jnp.where((giver == ranking[0]) | (sink == ranking[0]) | (lengths[sink] == 0), 0, jnp.maximum(margin, 0))
    moved = jax.random.randint(jax.random.fold_in(own, 4), (number_of // 2,), 0, 1 << 20) % (margin + 1)
    lengths = lengths.at[giver].add(-moved).at[sink].add(moved)
    labels = jnp.searchsorted(jnp.cumsum(lengths), jnp.arange(rows * top), side="right").astype(jnp.int32)
    listing = labels.reshape(top, rows).T
    listing = listing[jax.random.permutation(jax.random.fold_in(own, 1), rows)]
    rotation = jax.random.randint(jax.random.fold_in(own, 2), (rows, 1), 0, top)
    return jnp.take_along_axis(listing, (jnp.arange(top)[None, :] + rotation) % top, axis=1)


def shares(count, total, most, skew, full):
    loads = [(1 << 20) // math.isqrt(grade ** skew) + 1 for grade in range(1, count + 1)]
    largest = most if full else min(most, max(-(-total // count), total * loads[0] // sum(loads)))
    least = 1 if total - largest >= count - 1 else 0
    holding, rest = [largest] + [least] * (count - 1), total - largest - least * (count - 1)
    while rest > 0:
        candidates = [i for i in range(1, count) if holding[i] < largest] or [i for i in range(1, count) if holding[i] < most]
        whole, left = sum([loads[i] for i in candidates]), rest
        for i in candidates:
            addition = min(most - holding[i], max(1, left * loads[i] // whole), rest)
            holding[i] = holding[i] + addition
            rest = rest - addition
    return np.array(holding)


def gaussian(stream_key, extent, scale, reach, cuts=(), held_as=jnp.bfloat16):
    loudness = level_of(stream_key, extent, cuts, -0.22, 0.18) if cuts else 1.0
    entries = jax.random.normal(stream_key, extent, jnp.float32) * scale * loudness
    return jnp.minimum(jnp.maximum(entries, -reach), reach).astype(held_as)


def setup_inputs(seed: int = 0, part: int = 0) -> dict:
    key_list = jax.random.split(jax.random.key(seed), 10)
    part_splits = jax.random.split(jax.random.fold_in(key_list[9], part), 10)
    queries = draw_queries(jax.random.fold_in(jax.random.fold_in(key_list[9], part), 71), part)
    latent_cache = gaussian(part_splits[1], (SEQS, CTX, LAT + ROPE), 1.0, 6.0, ((1, 128),))
    context_lengths = draw_context_lengths(jax.random.fold_in(jax.random.fold_in(key_list[9], part), 71), part)
    value_up = gaussian(key_list[3], (H * LAT, VD), LAT ** -0.5, 0.25, ((0, 128),))
    out_proj = gaussian(key_list[4], (H * VD, D), (H * VD) ** -0.5, 0.09375, ((0, 128),))
    residual = gaussian(part_splits[5], (SEQS, D), 0.05, 0.75, ((1, 128),))
    norm_gain = jnp.clip(1.0 + 0.1 * jax.random.normal(key_list[6], (D,), jnp.float32), 0.5, 1.5).astype(jnp.bfloat16)
    expert_ids_keys = jax.random.split(jax.random.fold_in(part_splits[7], 1), SEQS // SEQS)
    expert_ids_turns = jax.random.permutation(jax.random.fold_in(part_splits[7], 3), SEQS // SEQS)
    expert_ids = jax.vmap(lambda own, number: assign_block(jax.random.fold_in(part_splits[7], 2), own, number, SEQS, EXPERTS, TOPK, CAP, 2))(expert_ids_keys, expert_ids_turns).reshape((SEQS, TOPK))
    gate_weights = jnp.clip(jax.random.uniform(part_splits[8], (SEQS, TOPK), jnp.float32, 0.05, 0.5), 0.05, 0.5)
    return dict(queries=queries, latent_cache=latent_cache, context_lengths=context_lengths, value_up=value_up, out_proj=out_proj, residual=residual, norm_gain=norm_gain, expert_ids=expert_ids, gate_weights=gate_weights)


score_scale = 192.0 ** (-0.5)
masked_score = -1e+30
small_eps = 1e-06

def slot_targets(expert_ids):
    flat_ids = expert_ids.reshape(-1).astype(jnp.int32)
    order_index = jnp.arange(flat_ids.shape[0], dtype=jnp.int32)
    same_before = (flat_ids[:, None] == flat_ids[None, :]) & (order_index[None, :] < order_index[:, None])
    rank_within = lax.optimization_barrier(jnp.sum(same_before.astype(jnp.int32), axis=1)).astype(jnp.int32)
    return flat_ids * CAP + rank_within

def reference(queries, latent_cache, context_lengths, value_up, out_proj, residual, norm_gain, expert_ids, gate_weights):
    query_rows = queries.reshape(SEQS, H, LAT + ROPE).astype(jnp.float32)
    shards = latent_cache.reshape(SEQS, N_KV, CTX_DEV, LAT + ROPE)

    def shard_step(running, shard_index):
        run_max, run_total, run_out = running
        cache_block = lax.dynamic_index_in_dim(shards, shard_index, 1, keepdims=False).astype(jnp.float32)
        scores = jnp.einsum('shq,scq->shc', query_rows, cache_block, precision=lax.Precision.HIGHEST) * score_scale
        position = shard_index * CTX_DEV + jnp.arange(CTX_DEV, dtype=jnp.int32)
        valid_mask = (position[None, :] < context_lengths[:, None])[:, None, :]
        scores = jnp.where(valid_mask, scores, masked_score)
        local_max = lax.optimization_barrier(jnp.max(scores, axis=2))
        weights = jnp.where(valid_mask, jnp.exp(scores - local_max[:, :, None]), 0.0)
        local_total = lax.optimization_barrier(jnp.sum(weights, axis=2))
        rounded = lax.optimization_barrier(weights.astype(jnp.bfloat16)).astype(jnp.float32)
        local_out = jnp.einsum('shc,scl->shl', rounded, cache_block[:, :, :LAT], precision=lax.Precision.HIGHEST)
        new_max = jnp.maximum(run_max, local_max)
        old_scale = jnp.exp(run_max - new_max)
        new_scale = jnp.exp(local_max - new_max)
        run_total = run_total * old_scale + local_total * new_scale
        run_out = run_out * old_scale[:, :, None] + local_out * new_scale[:, :, None]
        return ((new_max, run_total, run_out), None)
    start_state = (jnp.full((SEQS, H), masked_score, jnp.float32), jnp.zeros((SEQS, H), jnp.float32), jnp.zeros((SEQS, H, LAT), jnp.float32))
    final_state, unused = lax.scan(shard_step, start_state, jnp.arange(N_KV, dtype=jnp.int32))
    run_max, run_total, run_out = final_state
    merged = run_out / run_total[:, :, None]
    projector = value_up.reshape(H, LAT, VD).astype(jnp.float32)
    value_part = jnp.einsum('shl,hlv->shv', merged, projector, precision=lax.Precision.HIGHEST)
    value_rows = value_part.astype(jnp.bfloat16).reshape(SEQS, H * VD)
    attn_rows = jnp.dot(value_rows, out_proj, preferred_element_type=jnp.float32)
    summed = attn_rows + residual.astype(jnp.float32)
    inverse_rms = lax.rsqrt(lax.optimization_barrier(jnp.mean(summed * summed, axis=1)) + small_eps)
    normed = summed * inverse_rms[:, None] * norm_gain.astype(jnp.float32)
    peak_abs = lax.optimization_barrier(jnp.max(jnp.abs(normed), axis=1)) + small_eps
    coded_rows = (normed / peak_abs[:, None]).astype(jnp.bfloat16)
    targets = slot_targets(expert_ids)
    owner = jnp.arange(SEQS * TOPK, dtype=jnp.int32) // TOPK
    dispatched = jnp.zeros((EXPERTS * CAP, D), jnp.bfloat16).at[targets].set(coded_rows[owner])
    slot_scale = jnp.zeros((EXPERTS * CAP,), jnp.float32).at[targets].set(peak_abs[owner])
    slot_gate = jnp.zeros((EXPERTS * CAP,), jnp.float32).at[targets].set(gate_weights.reshape(-1))
    return (dispatched.reshape(EXPERTS, CAP, D), slot_scale.reshape(EXPERTS, CAP), slot_gate.reshape(EXPERTS, CAP))
```

```python
import functools

import jax
import jax.numpy as jnp
from jax import lax
from jax.experimental import pallas as pl
from jax.experimental.pallas import tpu as pltpu
from jax.sharding import Mesh
from jax.sharding import PartitionSpec as P

H = 32
LAT = 512
ROPE = 64
VD = 128
TOPK = 8
CAP = 2
SIDE = 8
QUARTERS = 4
ROWS = 24
KV = ("kv_0", "kv_1", "kv_2")
GROUPS_KV = ("groups", "kv_0", "kv_1", "kv_2")
MESH = pl.DeviceIdType.MESH
F32 = jnp.float32
BF16 = jnp.bfloat16

score_scale = 192.0 ** (-0.5)
masked_score = -1e30
small_eps = 1e-06

Q1, Q2, QD, O1, ML1, ML2, O2, A1, A2, A3 = range(10)
D_VU, D_RG, D_W, D_O, D_ML, D_F, D_X, D_V = range(8)


def lanes(shape):
    return lax.broadcasted_iota(jnp.int32, shape, len(shape) - 1)


def sublanes(shape):
    return lax.broadcasted_iota(jnp.int32, shape, len(shape) - 2)


def loop(count, body):
    def step(i, carry):
        body(i)
        return carry

    lax.fori_loop(0, count, step, 0)


def far_first(i):
    return SIDE // 2 + (1 - 2 * lax.rem(i, 2)) * lax.div(i + 1, 2)


def kernel(
    q_in, cache_in, ctx, vu_in, op_in, rg_in, ids_in, gate_in,
    disp_out, scale_out, gate_out,
    qraw, ext, qb, qa, cache, s0, r0, ml0, rml0, ow, mlw, s1, r1, ml1, rml1,
    ml2, rml2, fac, acc, ab, s2, r2, vu, vs, vr, rg, ta, tb, lhs, w,
    s3, r3, s4, r4, rf, ids, gate, pt, pick, y, fs, fr, xs, xr,
    loc, ssem, rsem, dsend, drecv,
):
    g = lax.axis_index("groups")
    yy = lax.axis_index("kv_0")
    xx = lax.axis_index("kv_1")
    c = lax.axis_index("kv_2")
    chip = yy * SIDE + xx
    dev = chip * 2 + c
    a = xx + c * (yy - xx)
    b = yy + c * (xx - yy)
    half_x = lax.rem(xx, 2)
    seqs, ctx_dev = cache.shape[0], cache.shape[1]
    half = seqs // 2
    width = w.shape[2]
    tiles = width // 128
    cols = SIDE * width

    def first(p):
        return (g, yy + c * (p - yy), xx + (1 - c) * (p - xx), c)

    def second(p):
        return (g, yy + (1 - c) * (p - yy), xx + c * (p - xx), c)

    partner = (g, yy, xx, 1 - c)
    neighbour = (g, yy, xx + 1 - 2 * half_x, c)

    def rcopy(src, dst, phase, to, frm, device):
        return pltpu.make_async_remote_copy(
            src_ref=src, dst_ref=dst, send_sem=ssem.at[phase, to], recv_sem=rsem.at[phase, frm],
            device_id=device, device_id_type=MESH,
        )

    def dcopy(src, dst, which, device):
        return pltpu.make_async_remote_copy(
            src_ref=src, dst_ref=dst, send_sem=dsend.at[which], recv_sem=drecv.at[which],
            device_id=device, device_id_type=MESH,
        )

    def peers(me, body):
        def one(i):
            body(lax.rem(me + far_first(i), SIDE))

        loop(SIDE - 1, one)

    def local(src, dst, k):
        return pltpu.make_async_copy(src, dst, loc.at[k])

    w_row = pl.multiple_of(half_x * 64 + c * 32, 32)
    q_load = local(q_in, qraw, 0)
    q_load.start()
    small = [
        local(vu_in, vu.at[c], 1),
        local(rg_in, rg.at[c], 2),
        local(ids_in, ids, 3),
        local(gate_in, gate, 4),
    ]
    for copy in small:
        copy.start()
    w_loads = [
        local(op_in.at[:, pl.ds(p * width, width)], w.at[p, pl.ds(w_row, 32), :], 5 + p)
        for p in range(SIDE)
    ]
    for copy in w_loads:
        copy.start()
    parts = 8
    each = seqs // parts
    k_loads = [
        local(cache_in.at[pl.ds(each * p, each)], cache.at[pl.ds(each * p, each)], 13 + p)
        for p in range(parts)
    ]
    for copy in k_loads:
        copy.start()

    barrier = pltpu.get_barrier_semaphore()
    pl.semaphore_signal(barrier, inc=1, device_id=partner, device_id_type=MESH)

    def greet(p):
        pl.semaphore_signal(barrier, inc=1, device_id=first(p), device_id_type=MESH)

    def greet_second(p):
        pl.semaphore_signal(barrier, inc=1, device_id=second(p), device_id_type=MESH)

    peers(a, greet)
    peers(b, greet_second)

    ext[...] = jnp.zeros(ext.shape, F32)
    q_load.wait()
    quarter = half_x * 2 + c
    ext[:, 0:16] = qraw[:, 128:144].astype(F32)
    main = pltpu.roll(qraw[:, 0:128].astype(F32), quarter * 16, 1)
    extra = jnp.zeros((8, 128), F32)
    for k in range(seqs // 8):
        extra = extra + pltpu.roll(ext[8 * k : 8 * k + 8, :], lax.rem(quarter + k, 8) * 16, 1)
    qb[c, b, a] = jnp.concatenate([main, extra], axis=0).astype(BF16)

    pl.semaphore_wait(barrier, 2 * (SIDE - 1) + 1)

    def q1(p):
        return rcopy(qb.at[c, b, a], qb.at[c, b, a], Q1, p, a, first(p))

    def q1_from(p):
        return rcopy(qb.at[c, b, p], qb.at[c, b, p], Q1, p, p, first(p))

    def q2(p):
        return rcopy(qb.at[c, b], qb.at[c, b], Q2, p, b, second(p))

    def q2_from(p):
        return rcopy(qb.at[c, p], qb.at[c, p], Q2, p, p, second(p))

    def qd(p):
        return rcopy(qb.at[c, p], qb.at[c, p], QD, p, p, partner)

    def qd_from(p):
        return rcopy(qb.at[1 - c, p], qb.at[1 - c, p], QD, p, p, partner)

    peers(a, lambda p: q1(p).start())

    for copy in small:
        copy.wait()
    for copy in w_loads:
        copy.wait()
    w_rows = w.at[:, pl.ds(w_row, 32), :]
    to_partner = [
        dcopy(vu.at[c], vu.at[c], D_VU, partner),
        dcopy(rg.at[c], rg.at[c], D_RG, partner),
        dcopy(w_rows, w_rows, D_W, partner),
    ]
    for copy in to_partner:
        copy.start()

    peers(a, lambda p: q1_from(p).wait_recv())
    peers(b, lambda p: q2(p).start())
    qd(b).start()

    for ref in (ml0, mlw, ab, ta, tb, pt):
        ref[...] = jnp.zeros(ref.shape, F32)
    idle_row = pl.multiple_of((1 - half_x) * 64, 64)

    def fill(p):
        w[p, pl.ds(idle_row, 64), :] = jnp.zeros((64, width), BF16)

        def block(k):
            start = pl.multiple_of(k * 16, 16)
            row = start + sublanes((16, width))
            column = p * width + lanes((16, width))
            target = chip * 112 + lax.rem(row, 64) + 56 * lax.div(row, 64)
            hit = jnp.where((column == target) & (lax.rem(row, 64) < 56), 1.0, 0.0)
            w[p, pl.ds(pl.multiple_of(128 + start, 16), 16), :] = hit.astype(BF16)

        loop(8, block)

    loop(SIDE, fill)

    idv = ids[...]
    gatev = gate[...]
    lane_s = lanes((seqs, 128))
    hits = jnp.zeros((seqs, 128), F32)
    hit_cols = []
    gates = []
    for j in range(4):
        expert = (dev if j < 2 else chip * 2 + 1 - c) * 2 + j % 2
        same = idv == expert
        hit = jnp.sum(jnp.where(same, 1.0, 0.0), axis=1, keepdims=True)
        hit_cols.append(hit)
        gates.append(jnp.sum(jnp.where(same, gatev, 0.0), axis=1, keepdims=True))
        hits = jnp.where(lane_s == j, hit, hits)
    lower = jnp.where(lanes((seqs, seqs)) < sublanes((seqs, seqs)), 1.0, 0.0)
    rank = jnp.dot(lower.astype(BF16), hits.astype(BF16), preferred_element_type=F32)
    table = jnp.zeros((seqs, 128), F32)
    gate_slots = jnp.zeros((2, CAP), F32)
    for j in range(4):
        for k in range(CAP):
            col = jnp.where(rank[:, j : j + 1] == float(k), hit_cols[j], 0.0)
            table = jnp.where(lane_s == (j // 2) * 8 + (j % 2) * CAP + k, col, table)
            if j < 2:
                total = jnp.sum(col * gates[j], axis=0, keepdims=True)
                here = (sublanes((2, CAP)) == j) & (lanes((2, CAP)) == k)
                gate_slots = jnp.where(here, total, gate_slots)
    gate_out[...] = gate_slots
    pt[0:seqs, :] = table
    own = jnp.where(c == 0, pt[0:ROWS, :], pt[half : half + ROWS, :])
    own = jnp.where(sublanes((ROWS, 128)) < half, own, 0.0)
    turned = jnp.concatenate([own, jnp.zeros((128 - ROWS, 128), F32)], axis=0).T
    pick[...] = turned[0:16, :]

    for copy in to_partner[:2]:
        copy.wait_recv()
    ta[:, 0:56] = rg[0].astype(F32)
    tb[:, 0:56] = rg[1].astype(F32)
    both = ta[...] + pltpu.roll(tb[...], 64, 1)
    ta[...] = both
    row = sublanes((ROWS, 128))
    mine = jnp.where(c == 0, ta[0:ROWS, :], ta[half : half + ROWS, :])
    gain_row = jnp.broadcast_to(ta[seqs : seqs + 1, :], (ROWS, 128))
    lhs[...] = jnp.where(row < half, mine, jnp.where(row == half, gain_row, 0.0))

    def pass_on(p):
        q2_from(p).wait_recv()
        qd(p).start()

    peers(b, pass_on)
    loop(SIDE, lambda p: qd_from(p).wait_recv())

    lane = lanes((seqs, 128))

    def assemble(h):
        hy = lax.div(h, 4)
        hg = lax.rem(h, 4)
        m = [
            qb[0, hy, 2 * hg].astype(F32),
            qb[1, 2 * hg, hy].astype(F32),
            qb[0, hy, 2 * hg + 1].astype(F32),
            qb[1, 2 * hg + 1, hy].astype(F32),
        ]
        lane8 = lanes((8, 128))
        extras = []
        for k in range(seqs // 8):
            picked = m[0][seqs:]
            for i in range(1, QUARTERS):
                picked = jnp.where(lax.div(lane8, 16) == (k + i) % 8, m[i][seqs:], picked)
            extras.append(pltpu.roll(picked, (128 - 16 * k) % 128, 1))
        e = jnp.concatenate(extras, axis=0)
        m = [v[:seqs] for v in m]
        whole = [
            m[0],
            jnp.where(lane < 16, e, m[1]),
            jnp.where(lane < 16, m[1], jnp.where(lane < 32, e, m[2])),
            jnp.where(lane < 32, m[2], jnp.where(lane < 48, e, m[3])),
            jnp.where(lane < 48, m[3], e),
        ]
        for t in range(5):
            qa[pl.ds(pl.multiple_of((h * 5 + t) * seqs, 8), seqs), :] = whole[t]

    loop(H, assemble)

    for copy in k_loads:
        copy.wait()
    position = dev * ctx_dev + lanes((1, ctx_dev))
    pitch = 5 * seqs

    def attend(s, by_column):
        pieces = []
        for t in range(5):
            groups = []
            for k in range(4):
                if by_column:
                    start, stride = k * pitch, 4 * pitch
                else:
                    start, stride = 8 * k * pitch, pitch
                groups.append(qa[pl.ds(start + t * seqs + s, 8, stride=stride), :])
            pieces.append(jnp.concatenate(groups, axis=0).astype(BF16))
        q = jnp.concatenate(pieces, axis=1)[:, : LAT + ROPE]
        scores = lax.dot_general(
            q, cache[s], (((1,), (1,)), ((), ())), preferred_element_type=F32
        )
        valid = position < ctx[s]
        scores = jnp.where(valid, scores * score_scale, masked_score)
        top = jnp.max(scores, axis=1, keepdims=True)
        weights = jnp.where(valid, jnp.exp(scores - top), 0.0)
        total = jnp.sum(weights, axis=1, keepdims=True)
        out = jnp.dot(weights.astype(BF16), cache[s, :, 0:LAT], preferred_element_type=F32)
        return top, total, out

    lane8 = lanes((8, 128))

    def note(ml, p, k, top, total):
        ml[p] = jnp.where(lane8 == k, top, jnp.where(lane8 == 64 + k, total, ml[p]))

    def by_column(dst, ml):
        def body(i):
            for u in range(4):
                s = i * 4 + u
                top, total, out = attend(s, True)
                for k in range(4):
                    rows = slice(8 * k, 8 * k + 8)
                    for d in range(2):
                        lo = out[rows, 256 * d : 256 * d + 128]
                        hi = out[rows, 256 * d + 128 : 256 * d + 256]
                        dst[2 * k + d, s] = jnp.concatenate([lo, hi], axis=0).astype(dst.dtype)
                        note(ml, 2 * k + d, s, top[rows], total[rows])

        loop(half // 4, body)

    def by_row(dst, ml):
        low = sublanes((8, 128)) < 4

        def merge(u, v, top_half):
            if top_half:
                return jnp.where(low, u, pltpu.roll(v, 4, 0))
            return jnp.where(low, pltpu.roll(u, 4, 0), v)

        def body(i):
            for u in range(2):
                pair = i * 2 + u
                t0, l0, o0 = attend(half + 2 * pair, False)
                t1, l1, o1 = attend(half + 2 * pair + 1, False)
                for k in range(4):
                    rows = slice(8 * k, 8 * k + 8)
                    wide = (8, 128)
                    for d in range(2):
                        top = merge(
                            jnp.broadcast_to(t0[rows], wide), jnp.broadcast_to(t1[rows], wide), d == 0
                        )
                        total = merge(
                            jnp.broadcast_to(l0[rows], wide), jnp.broadcast_to(l1[rows], wide), d == 0
                        )
                        p = 2 * k + d
                        for e in range(2):
                            blocks = [
                                merge(
                                    o0[rows, 128 * t : 128 * t + 128],
                                    o1[rows, 128 * t : 128 * t + 128],
                                    d == 0,
                                )
                                for t in (2 * e, 2 * e + 1)
                            ]
                            index = 2 * pair + e
                            dst[p, index] = jnp.concatenate(blocks, axis=0).astype(dst.dtype)
                            note(ml, p, index, top, total)

        loop(half // 4, body)

    o_partner = dcopy(s0, r0, D_O, partner)
    ml_partner = dcopy(ml0, rml0, D_ML, partner)

    @pl.when(c == 0)
    def _():
        by_row(s0, ml0)

    @pl.when(c == 1)
    def _():
        by_column(s0, ml0)

    ml_partner.start()
    o_partner.start()

    @pl.when(c == 0)
    def _():
        by_column(ow, mlw)

    @pl.when(c == 1)
    def _():
        by_row(ow, mlw)

    ml_partner.wait_recv()

    def mlsend(p):
        return rcopy(ml1.at[p], rml1.at[a], ML1, p, a, first(p))

    def ml_from(p):
        return rcopy(ml1.at[p], rml1.at[p], ML1, p, p, first(p))

    def osend(p):
        return rcopy(s1.at[p], r1.at[a], O1, p, a, first(p))

    def o_from(p):
        return rcopy(s1.at[p], r1.at[p], O1, p, p, first(p))

    def chip_max(p):
        here, there = mlw[p], rml0[p]
        top = jnp.maximum(here, there)
        total = jnp.exp(here - top) * pltpu.roll(here, 64, 1)
        total = total + jnp.exp(there - top) * pltpu.roll(there, 64, 1)
        ml1[p] = jnp.where(lane8 < 64, top, pltpu.roll(total, 64, 1))

    loop(SIDE, chip_max)
    peers(a, lambda p: mlsend(p).start())
    o_partner.wait_recv()

    def chip_sum(p):
        top = ml1[p]
        f_here = jnp.exp(mlw[p] - top)
        f_there = jnp.exp(rml0[p] - top)
        for k in range(half):
            fh = jnp.broadcast_to(f_here[:, k : k + 1], (8, 128))
            ft = jnp.broadcast_to(f_there[:, k : k + 1], (8, 128))
            fh = jnp.concatenate([fh, fh], axis=0)
            ft = jnp.concatenate([ft, ft], axis=0)
            s1[p, k] = (fh * ow[p, k] + ft * r0[p, k].astype(F32)).astype(BF16)

    def chip_send(p):
        chip_sum(p)
        osend(p).start()

    peers(a, chip_send)
    chip_sum(a)

    peers(a, lambda p: ml_from(p).wait_recv())
    rml1[a] = ml1[a]
    top = rml1[0]
    for p in range(1, SIDE):
        top = jnp.maximum(top, rml1[p])
    total = jnp.zeros((8, 128), F32)
    for p in range(SIDE):
        total = total + jnp.exp(rml1[p] - top) * pltpu.roll(rml1[p], 64, 1)
    packed = jnp.where(lane8 < 64, top, pltpu.roll(total, 64, 1))
    ml2[...] = packed

    def ml2_send(p):
        return rcopy(ml2, rml2.at[b], ML2, p, b, second(p))

    def ml2_from(p):
        return rcopy(ml2, rml2.at[p], ML2, p, p, second(p))

    peers(b, lambda p: ml2_send(p).start())
    peers(b, lambda p: ml2_from(p).wait_recv())
    rml2[b] = packed
    top = rml2[0]
    for p in range(1, SIDE):
        top = jnp.maximum(top, rml2[p])
    total = jnp.zeros((8, 128), F32)
    for p in range(SIDE):
        total = total + jnp.exp(rml2[p] - top) * pltpu.roll(rml2[p], 64, 1)
    for p in range(SIDE):
        fac[p] = jnp.exp(rml1[p] - top) / total

    def add(block, p, fresh):
        f = fac[p]
        for k in range(half):
            fk = jnp.broadcast_to(f[:, k : k + 1], (8, 128))
            term = jnp.concatenate([fk, fk], axis=0) * block[k].astype(F32)
            acc[k] = term if fresh else acc[k] + term

    add(s1.at[a], a, True)

    def take(p):
        o_from(p).wait_recv()
        add(r1.at[p], p, False)

    peers(a, take)

    @pl.when(c == 0)
    def _():
        for k in range(half):
            for d in range(2):
                ab[d * 192 + k * 8 : d * 192 + k * 8 + 8, :] = acc[k, 8 * d : 8 * d + 8, :]
        for j in range(SIDE):
            s2[j] = jnp.concatenate(
                [ab[pl.ds(d * 192 + j, ROWS, stride=8), :] for d in range(2)], axis=0
            ).astype(BF16)

    @pl.when(c == 1)
    def _():
        for k in range(half):
            for d in range(2):
                base = ((k % 2) * 2 + d) * 96 + (k // 2) * 8
                ab[base : base + 8, :] = acc[k, 8 * d : 8 * d + 8, :]
        for j in range(SIDE):
            s2[j] = jnp.concatenate(
                [ab[pl.ds(((j % 2) * 2 + d) * 96 + j // 2, ROWS, stride=4), :] for d in range(2)],
                axis=0,
            ).astype(BF16)

    def o2_send(p):
        return rcopy(s2.at[p], r2.at[b], O2, p, b, second(p))

    def o2_from(p):
        return rcopy(s2.at[p], r2.at[p], O2, p, p, second(p))

    peers(b, lambda p: o2_send(p).start())
    peers(b, lambda p: o2_from(p).wait_recv())
    r2[b] = s2[b]
    merged = r2[0].astype(F32)
    for p in range(1, SIDE):
        merged = merged + r2[p].astype(F32)

    part = jnp.zeros((ROWS, VD), F32)
    for k in range(2):
        block = merged[ROWS * k : ROWS * (k + 1)]
        high = block.astype(BF16)
        low = (block - high.astype(F32)).astype(BF16)
        part = part + jnp.dot(high, vu[k], preferred_element_type=F32)
        part = part + jnp.dot(low, vu[k], preferred_element_type=F32)
    vs[...] = part
    swap = dcopy(vs, vr, D_V, neighbour)
    swap.start()
    to_partner[2].wait_recv()
    swap.wait_recv()
    left = jnp.concatenate([(part + vr[...]).astype(BF16), lhs[...].astype(BF16)], axis=1)

    def a1_send(p):
        return rcopy(s3.at[p], r3.at[a], A1, p, a, first(p))

    def a1_from(p):
        return rcopy(s3.at[p], r3.at[p], A1, p, p, first(p))

    def a2_send(p):
        return rcopy(s4, r4.at[b], A2, p, b, second(p))

    def a2_from(p):
        return rcopy(s4, r4.at[p], A2, p, p, second(p))

    def a3_send(p):
        return rcopy(rf.at[a], rf.at[a], A3, p, a, first(p))

    def a3_from(p):
        return rcopy(rf.at[p], rf.at[p], A3, p, p, first(p))

    def project(p):
        out = jnp.dot(left, w[p], preferred_element_type=F32)
        blocks = [out[:, 128 * t : 128 * t + 128] for t in range(tiles)]
        blocks.append(jnp.zeros((8, 128), F32))
        s3[p] = jnp.concatenate(blocks, axis=0).astype(BF16)

    def project_send(p):
        project(p)
        a1_send(p).start()

    peers(a, project_send)
    project(a)
    peers(a, lambda p: a1_from(p).wait_recv())
    r3[a] = s3[a]
    total = r3[0].astype(F32)
    for p in range(1, SIDE):
        total = total + r3[p].astype(F32)
    s4[...] = total.astype(BF16)
    peers(b, lambda p: a2_send(p).start())
    peers(b, lambda p: a2_from(p).wait_recv())
    r4[b] = s4[...]
    total = r4[0].astype(F32)
    for p in range(1, SIDE):
        total = total + r4[p].astype(F32)
    rf[a] = total.astype(BF16)
    peers(a, lambda p: a3_send(p).start())
    peers(a, lambda p: a3_from(p).wait_recv())

    choose = pick[...][:, 0:ROWS]
    choose_b = choose.astype(BF16)
    squares = jnp.zeros((ROWS, 128), F32)
    largest = jnp.zeros((ROWS, 128), F32)
    for p in range(SIDE):
        block = rf[p].astype(F32)
        parts_r = [block[ROWS * t : ROWS * (t + 1)] for t in range(tiles)]
        gains = [v[half : half + 1] for v in parts_r]
        for v, gv in zip(parts_r, gains):
            squares = squares + v * v
            largest = jnp.maximum(largest, jnp.abs(v * gv))
        rows = jnp.concatenate(parts_r, axis=1).astype(BF16)
        chosen = jnp.dot(choose_b, rows, preferred_element_type=F32)
        y[p] = chosen * jnp.concatenate(gains, axis=1)
    inverse = lax.rsqrt(jnp.sum(squares, axis=1, keepdims=True) / cols + small_eps)
    peak = inverse * jnp.max(largest, axis=1, keepdims=True) + small_eps
    spread = jnp.concatenate(
        [jnp.broadcast_to(inverse / peak, (ROWS, 128)), jnp.broadcast_to(peak, (ROWS, 128))], axis=1
    )
    slots = jnp.dot(choose, spread, preferred_element_type=F32, precision=lax.Precision.HIGHEST)
    code = jnp.concatenate([slots[:, 0:128]] * tiles, axis=1)
    peaks = slots[:, 128:256]
    xs[...] = peaks[8:16]
    for k in range(SIDE // 2):
        fs[k] = jnp.concatenate(
            [y[2 * k + d, 8:16, :] * code[8:16] for d in range(2)], axis=0
        ).astype(BF16)
    x_partner = dcopy(xs, xr, D_X, partner)
    f_partner = dcopy(fs, fr, D_F, partner)
    x_partner.start()
    f_partner.start()
    x_partner.wait_recv()
    peaks = peaks[0:8] + xr[...]
    scale_slots = jnp.zeros((2, CAP), F32)
    for j in range(2):
        for k in range(CAP):
            here = (sublanes((2, CAP)) == j) & (lanes((2, CAP)) == k)
            r = CAP * j + k
            scale_slots = jnp.where(here, peaks[r : r + 1, 0:1], scale_slots)
    scale_out[...] = scale_slots
    f_partner.wait_recv()
    for k in range(SIDE // 2):
        there = fr[k].astype(F32)
        for d in range(2):
            p = 2 * k + d
            rows = (y[p, 0:8, :] * code[0:8] + there[8 * d : 8 * d + 8]).astype(BF16)
            disp_out[:, pl.ds(p * width, width)] = rows[0:4]

    peers(a, lambda p: q1(p).wait_send())
    peers(b, lambda p: q2(p).wait_send())
    loop(SIDE, lambda p: qd(p).wait_send())
    peers(a, lambda p: mlsend(p).wait_send())
    peers(a, lambda p: osend(p).wait_send())
    peers(b, lambda p: ml2_send(p).wait_send())
    peers(b, lambda p: o2_send(p).wait_send())
    peers(a, lambda p: a1_send(p).wait_send())
    peers(b, lambda p: a2_send(p).wait_send())
    peers(a, lambda p: a3_send(p).wait_send())
    for copy in to_partner + [o_partner, ml_partner, swap, x_partner, f_partner]:
        copy.wait_send()


def per_device(
    queries, latent_cache, context_lengths, value_up, out_proj, residual, norm_gain, expert_ids,
    gate_weights,
):
    seqs, ctx_dev, entry = latent_cache.shape
    half = seqs // 2
    columns = out_proj.shape[1]
    width = columns // SIDE
    piece = residual.shape[1]
    experts = 2
    rows = (width // 128) * ROWS + 8
    rest = jnp.zeros((7, piece), residual.dtype)
    rg = jnp.concatenate([residual, norm_gain[None, :], rest], axis=0)
    any_space = pl.BlockSpec(memory_space=pl.ANY)
    vmem = pl.BlockSpec(memory_space=pltpu.VMEM)
    smem = pl.BlockSpec(memory_space=pltpu.SMEM)
    V = pltpu.VMEM
    chunk = (SIDE, half, 16, 128)
    eights = (SIDE, 8, 128)
    scratch = [
        V(queries.shape, BF16),
        V((seqs, 128), F32),
        V((2, SIDE, SIDE, seqs + 8, 128), BF16),
        V((H * 5 * seqs, 128), F32),
        V(latent_cache.shape, BF16),
        V(chunk, BF16),
        V(chunk, BF16),
        V(eights, F32),
        V(eights, F32),
        V(chunk, F32),
        V(eights, F32),
        V(chunk, BF16),
        V(chunk, BF16),
        V(eights, F32),
        V(eights, F32),
        V((8, 128), F32),
        V(eights, F32),
        V(eights, F32),
        V(chunk[1:], F32),
        V((384, 128), F32),
        V((SIDE, 2 * ROWS, 128), BF16),
        V((SIDE, 2 * ROWS, 128), BF16),
        V((2, 128, VD), BF16),
        V((ROWS, VD), F32),
        V((ROWS, VD), F32),
        V((2, seqs + 8, piece), BF16),
        V((seqs + 8, 128), F32),
        V((seqs + 8, 128), F32),
        V((ROWS, 128), F32),
        V((SIDE, 256, width), BF16),
        V((SIDE, rows, 128), BF16),
        V((SIDE, rows, 128), BF16),
        V((rows, 128), BF16),
        V((SIDE, rows, 128), BF16),
        V((SIDE, rows, 128), BF16),
        V(expert_ids.shape, jnp.int32),
        V(gate_weights.shape, F32),
        V((seqs + 8, 128), F32),
        V((16, 128), F32),
        V((SIDE, 16, width), F32),
        V((SIDE // 2, 16, width), BF16),
        V((SIDE // 2, 16, width), BF16),
        V((8, 128), F32),
        V((8, 128), F32),
        pltpu.SemaphoreType.DMA((24,)),
        pltpu.SemaphoreType.DMA((10, SIDE)),
        pltpu.SemaphoreType.DMA((10, SIDE)),
        pltpu.SemaphoreType.DMA((8,)),
        pltpu.SemaphoreType.DMA((8,)),
    ]
    dispatched, slot_scale, slot_gate = pl.pallas_call(
        kernel,
        out_shape=(
            jax.ShapeDtypeStruct((experts * CAP, columns), BF16),
            jax.ShapeDtypeStruct((experts, CAP), F32),
            jax.ShapeDtypeStruct((experts, CAP), F32),
        ),
        in_specs=[any_space, any_space, smem] + [any_space] * 5,
        out_specs=(vmem, vmem, vmem),
        scratch_shapes=scratch,
        compiler_params=pltpu.CompilerParams(collective_id=0, has_side_effects=True),
    )(queries, latent_cache, context_lengths, value_up, out_proj, rg, expert_ids, gate_weights)
    return dispatched.reshape(experts, CAP, columns), slot_scale, slot_gate


def solution(mesh):
    split = Mesh(
        mesh.devices.reshape(mesh.shape["groups"], SIDE, SIDE, 2),
        ("groups", "kv_0", "kv_1", "kv_2"),
    )
    in_specs = (
        P("groups", KV),
        P("groups", KV, None),
        P("groups"),
        P(KV, None),
        P(KV, None),
        P("groups", KV),
        P(KV),
        P("groups", None),
        P("groups", None),
    )
    out_specs = (P(GROUPS_KV, None, None), P(GROUPS_KV, None), P(GROUPS_KV, None))
    return jax.shard_map(
        per_device, mesh=split, in_specs=in_specs, out_specs=out_specs, check_vma=False
    )
```

```python
import functools

import jax
import jax.numpy as jnp
from jax import lax
from jax.experimental import pallas as pl
from jax.experimental.pallas import tpu as pltpu
from jax.sharding import Mesh
from jax.sharding import PartitionSpec as P

H = 32
LAT = 512
ROPE = 64
VD = 128
TOPK = 8
CAP = 2
SIDE = 8
QUARTERS = 4
ROWS = 24
KV = ("kv_0", "kv_1", "kv_2")
GROUPS_KV = ("groups", "kv_0", "kv_1", "kv_2")
MESH = pl.DeviceIdType.MESH
F32 = jnp.float32
BF16 = jnp.bfloat16

score_scale = 192.0 ** (-0.5)
masked_score = -1e30
small_eps = 1e-06

Q1, Q2, QD, O1, ML1, ML2, O2, A1, A2, A3 = range(10)
D_VU, D_RES, D_GAIN, D_W, D_O, D_ML, D_F, D_X, D_V = range(9)


def lanes(shape):
    return lax.broadcasted_iota(jnp.int32, shape, len(shape) - 1)


def sublanes(shape):
    return lax.broadcasted_iota(jnp.int32, shape, len(shape) - 2)


def loop(count, body):
    def step(i, carry):
        body(i)
        return carry

    lax.fori_loop(0, count, step, 0)


def far_first(i):
    return SIDE // 2 + (1 - 2 * lax.rem(i, 2)) * lax.div(i + 1, 2)


def kernel(
    q_in, cache_in, ctx, vu_in, op_in, res_in, gain_in, ids_in, gate_in,
    disp_out, scale_out, gate_out,
    qraw, ext, qb, qa, cache, s0, r0, ml0, rml0, ow, mlw, s1, r1, ml1, rml1,
    ml2, rml2, fac, acc, ab, s2, r2, vu, vs, vr, res, gain, ta, tb, lhs, w,
    s3, r3, s4, r4, rf, ids, gate, pt, pick, y, fs, fr, xs, xr,
    loc, ssem, rsem, dsend, drecv,
):
    g = lax.axis_index("groups")
    yy = lax.axis_index("kv_0")
    xx = lax.axis_index("kv_1")
    c = lax.axis_index("kv_2")
    chip = yy * SIDE + xx
    dev = chip * 2 + c
    a = xx + c * (yy - xx)
    b = yy + c * (xx - yy)
    half_x = lax.rem(xx, 2)
    seqs, ctx_dev = cache.shape[0], cache.shape[2]
    half = seqs // 2
    width = w.shape[2]
    tiles = width // 128
    cols = SIDE * width

    def first(p):
        return (g, yy + c * (p - yy), xx + (1 - c) * (p - xx), c)

    def second(p):
        return (g, yy + (1 - c) * (p - yy), xx + c * (p - xx), c)

    partner = (g, yy, xx, 1 - c)
    neighbour = (g, yy, xx + 1 - 2 * half_x, c)

    def rcopy(src, dst, phase, to, frm, device):
        return pltpu.make_async_remote_copy(
            src_ref=src, dst_ref=dst, send_sem=ssem.at[phase, to], recv_sem=rsem.at[phase, frm],
            device_id=device, device_id_type=MESH,
        )

    def dcopy(src, dst, which, device):
        return pltpu.make_async_remote_copy(
            src_ref=src, dst_ref=dst, send_sem=dsend.at[which], recv_sem=drecv.at[which],
            device_id=device, device_id_type=MESH,
        )

    def peers(me, body):
        def one(i):
            body(lax.rem(me + far_first(i), SIDE))

        loop(SIDE - 1, one)

    def local(src, dst, k):
        return pltpu.make_async_copy(src, dst, loc.at[k])

    w_row = pl.multiple_of(half_x * 64 + c * 32, 32)
    q_load = local(q_in, qraw, 0)
    q_load.start()
    small = [
        local(vu_in, vu.at[c], 1),
        local(res_in, res.at[c], 2),
        local(gain_in, gain.at[c], 21),
        local(ids_in, ids, 3),
        local(gate_in, gate, 4),
    ]
    for copy in small:
        copy.start()
    w_loads = [
        local(op_in.at[:, pl.ds(p * width, width)], w.at[p, pl.ds(w_row, 32), :], 5 + p)
        for p in range(SIDE)
    ]
    for copy in w_loads:
        copy.start()
    parts = 8
    each = seqs // parts
    k_loads = [
        local(cache_in.at[pl.ds(each * p, each)], cache.at[pl.ds(each * p, each)], 13 + p)
        for p in range(parts)
    ]
    for copy in k_loads:
        copy.start()

    barrier = pltpu.get_barrier_semaphore()
    pl.semaphore_signal(barrier, inc=1, device_id=partner, device_id_type=MESH)

    def greet(p):
        pl.semaphore_signal(barrier, inc=1, device_id=first(p), device_id_type=MESH)

    def greet_second(p):
        pl.semaphore_signal(barrier, inc=1, device_id=second(p), device_id_type=MESH)

    peers(a, greet)
    peers(b, greet_second)

    ext[...] = jnp.zeros(ext.shape, F32)
    q_load.wait()
    quarter = half_x * 2 + c
    ext[:, 0:16] = qraw[:, 128:144].astype(F32)
    main = pltpu.roll(qraw[:, 0:128].astype(F32), quarter * 16, 1)
    extra = jnp.zeros((8, 128), F32)
    for k in range(seqs // 8):
        extra = extra + pltpu.roll(ext[8 * k : 8 * k + 8, :], lax.rem(quarter + k, 8) * 16, 1)
    qb[c, b, a] = jnp.concatenate([main, extra], axis=0).astype(BF16)

    pl.semaphore_wait(barrier, 2 * (SIDE - 1) + 1)

    def q1(p):
        return rcopy(qb.at[c, b, a], qb.at[c, b, a], Q1, p, a, first(p))

    def q1_from(p):
        return rcopy(qb.at[c, b, p], qb.at[c, b, p], Q1, p, p, first(p))

    def q2(p):
        return rcopy(qb.at[c, b], qb.at[c, b], Q2, p, b, second(p))

    def q2_from(p):
        return rcopy(qb.at[c, p], qb.at[c, p], Q2, p, p, second(p))

    def qd(p):
        return rcopy(qb.at[c, p], qb.at[c, p], QD, p, p, partner)

    def qd_from(p):
        return rcopy(qb.at[1 - c, p], qb.at[1 - c, p], QD, p, p, partner)

    peers(a, lambda p: q1(p).start())

    for copy in small:
        copy.wait()
    for copy in w_loads:
        copy.wait()
    w_rows = w.at[:, pl.ds(w_row, 32), :]
    to_partner = [
        dcopy(vu.at[c], vu.at[c], D_VU, partner),
        dcopy(res.at[c], res.at[c], D_RES, partner),
        dcopy(gain.at[c], gain.at[c], D_GAIN, partner),
        dcopy(w_rows, w_rows, D_W, partner),
    ]
    for copy in to_partner:
        copy.start()

    peers(a, lambda p: q1_from(p).wait_recv())
    peers(b, lambda p: q2(p).start())
    qd(b).start()

    for ref in (ml0, mlw, ab, ta, tb, pt):
        ref[...] = jnp.zeros(ref.shape, F32)
    idle_row = pl.multiple_of((1 - half_x) * 64, 64)

    def fill(p):
        w[p, pl.ds(idle_row, 64), :] = jnp.zeros((64, width), BF16)

        def block(k):
            start = pl.multiple_of(k * 16, 16)
            row = start + sublanes((16, width))
            column = p * width + lanes((16, width))
            target = chip * 112 + lax.rem(row, 64) + 56 * lax.div(row, 64)
            hit = jnp.where((column == target) & (lax.rem(row, 64) < 56), 1.0, 0.0)
            w[p, pl.ds(pl.multiple_of(128 + start, 16), 16), :] = hit.astype(BF16)

        loop(8, block)

    loop(SIDE, fill)

    idv = ids[...]
    gatev = gate[...]
    hits = jnp.zeros((8, seqs), F32)
    hit_rows = []
    gates = []
    for j in range(4):
        expert = (dev if j < 2 else chip * 2 + 1 - c) * 2 + j % 2
        same = idv == expert
        hit = jnp.sum(jnp.where(same, 1.0, 0.0), axis=0, keepdims=True)
        hit_rows.append(hit)
        gates.append(jnp.sum(jnp.where(same, gatev, 0.0), axis=0, keepdims=True))
        hits = jnp.where(sublanes((8, seqs)) == j, hit, hits)
    earlier = jnp.where(sublanes((seqs, seqs)) < lanes((seqs, seqs)), 1.0, 0.0)
    rank = jnp.dot(hits.astype(BF16), earlier.astype(BF16), preferred_element_type=F32)
    table = jnp.zeros((16, seqs), F32)
    gate_slots = jnp.zeros((2, CAP), F32)
    for j in range(4):
        for k in range(CAP):
            chosen = jnp.where(rank[j : j + 1] == float(k), hit_rows[j], 0.0)
            r = (j // 2) * 8 + (j % 2) * CAP + k
            table = jnp.where(sublanes((16, seqs)) == r, chosen, table)
            if j < 2:
                total = jnp.sum(chosen * gates[j], axis=1, keepdims=True)
                here = (sublanes((2, CAP)) == j) & (lanes((2, CAP)) == k)
                gate_slots = jnp.where(here, total, gate_slots)
    gate_out[...] = gate_slots
    pt[:, 0:seqs] = table
    own = jnp.where(c == 0, pt[...], pltpu.roll(pt[...], 128 - half, 1))
    pick[...] = jnp.where(lanes((16, 128)) < half, own, 0.0)

    for copy in to_partner[:3]:
        copy.wait_recv()
    ta[0:seqs, 0:56] = res[0].astype(F32)
    tb[0:seqs, 0:56] = res[1].astype(F32)
    ta[seqs : seqs + 1, 0:56] = gain[0].astype(F32)
    tb[seqs : seqs + 1, 0:56] = gain[1].astype(F32)
    both = ta[...] + pltpu.roll(tb[...], 64, 1)
    ta[...] = both
    row = sublanes((ROWS, 128))
    mine = jnp.where(c == 0, ta[0:ROWS, :], ta[half : half + ROWS, :])
    gain_row = jnp.broadcast_to(ta[seqs : seqs + 1, :], (ROWS, 128))
    lhs[...] = jnp.where(row < half, mine, jnp.where(row == half, gain_row, 0.0))

    def pass_on(p):
        q2_from(p).wait_recv()
        qd(p).start()

    peers(b, pass_on)
    loop(SIDE, lambda p: qd_from(p).wait_recv())

    lane = lanes((seqs, 128))

    def assemble(h):
        hy = lax.div(h, 4)
        hg = lax.rem(h, 4)
        m = [
            qb[0, hy, 2 * hg].astype(F32),
            qb[1, 2 * hg, hy].astype(F32),
            qb[0, hy, 2 * hg + 1].astype(F32),
            qb[1, 2 * hg + 1, hy].astype(F32),
        ]
        lane8 = lanes((8, 128))
        extras = []
        for k in range(seqs // 8):
            picked = m[0][seqs:]
            for i in range(1, QUARTERS):
                picked = jnp.where(lax.div(lane8, 16) == (k + i) % 8, m[i][seqs:], picked)
            extras.append(pltpu.roll(picked, (128 - 16 * k) % 128, 1))
        e = jnp.concatenate(extras, axis=0)
        m = [v[:seqs] for v in m]
        whole = [
            m[0],
            jnp.where(lane < 16, e, m[1]),
            jnp.where(lane < 16, m[1], jnp.where(lane < 32, e, m[2])),
            jnp.where(lane < 32, m[2], jnp.where(lane < 48, e, m[3])),
            jnp.where(lane < 48, m[3], e),
        ]
        for t in range(5):
            qa[pl.ds(pl.multiple_of((h * 5 + t) * seqs, 8), seqs), :] = whole[t]

    loop(H, assemble)

    for copy in k_loads:
        copy.wait()
    position = dev * ctx_dev + lanes((1, ctx_dev))
    pitch = 5 * seqs

    def attend(s, by_column):
        pieces = []
        for t in range(5):
            groups = []
            for k in range(4):
                if by_column:
                    start, stride = k * pitch, 4 * pitch
                else:
                    start, stride = 8 * k * pitch, pitch
                groups.append(qa[pl.ds(start + t * seqs + s, 8, stride=stride), :])
            pieces.append(jnp.concatenate(groups, axis=0).astype(BF16))
        q = jnp.concatenate(pieces, axis=1)[:, : LAT + ROPE]
        scores = jnp.dot(q, cache[s], preferred_element_type=F32)
        valid = position < ctx[s]
        scores = jnp.where(valid, scores * score_scale, masked_score)
        top = jnp.max(scores, axis=1, keepdims=True)
        weights = jnp.where(valid, jnp.exp(scores - top), 0.0)
        total = jnp.sum(weights, axis=1, keepdims=True)
        out = lax.dot_general(
            weights.astype(BF16), cache[s, 0:LAT, :], (((1,), (1,)), ((), ())),
            preferred_element_type=F32,
        )
        return top, total, out

    lane8 = lanes((8, 128))

    def note(ml, p, k, top, total):
        ml[p] = jnp.where(lane8 == k, top, jnp.where(lane8 == 64 + k, total, ml[p]))

    def by_column(dst, ml):
        def body(i):
            for u in range(4):
                s = i * 4 + u
                top, total, out = attend(s, True)
                for k in range(4):
                    rows = slice(8 * k, 8 * k + 8)
                    for d in range(2):
                        lo = out[rows, 256 * d : 256 * d + 128]
                        hi = out[rows, 256 * d + 128 : 256 * d + 256]
                        dst[2 * k + d, s] = jnp.concatenate([lo, hi], axis=0).astype(dst.dtype)
                        note(ml, 2 * k + d, s, top[rows], total[rows])

        loop(half // 4, body)

    def by_row(dst, ml):
        low = sublanes((8, 128)) < 4

        def merge(u, v, top_half):
            if top_half:
                return jnp.where(low, u, pltpu.roll(v, 4, 0))
            return jnp.where(low, pltpu.roll(u, 4, 0), v)

        def body(i):
            for u in range(2):
                pair = i * 2 + u
                t0, l0, o0 = attend(half + 2 * pair, False)
                t1, l1, o1 = attend(half + 2 * pair + 1, False)
                for k in range(4):
                    rows = slice(8 * k, 8 * k + 8)
                    wide = (8, 128)
                    for d in range(2):
                        top = merge(
                            jnp.broadcast_to(t0[rows], wide), jnp.broadcast_to(t1[rows], wide), d == 0
                        )
                        total = merge(
                            jnp.broadcast_to(l0[rows], wide), jnp.broadcast_to(l1[rows], wide), d == 0
                        )
                        p = 2 * k + d
                        for e in range(2):
                            blocks = [
                                merge(
                                    o0[rows, 128 * t : 128 * t + 128],
                                    o1[rows, 128 * t : 128 * t + 128],
                                    d == 0,
                                )
                                for t in (2 * e, 2 * e + 1)
                            ]
                            index = 2 * pair + e
                            dst[p, index] = jnp.concatenate(blocks, axis=0).astype(dst.dtype)
                            note(ml, p, index, top, total)

        loop(half // 4, body)

    o_partner = dcopy(s0, r0, D_O, partner)
    ml_partner = dcopy(ml0, rml0, D_ML, partner)

    @pl.when(c == 0)
    def _():
        by_row(s0, ml0)

    @pl.when(c == 1)
    def _():
        by_column(s0, ml0)

    ml_partner.start()
    o_partner.start()

    @pl.when(c == 0)
    def _():
        by_column(ow, mlw)

    @pl.when(c == 1)
    def _():
        by_row(ow, mlw)

    ml_partner.wait_recv()

    def mlsend(p):
        return rcopy(ml1.at[p], rml1.at[a], ML1, p, a, first(p))

    def ml_from(p):
        return rcopy(ml1.at[p], rml1.at[p], ML1, p, p, first(p))

    def osend(p):
        return rcopy(s1.at[p], r1.at[a], O1, p, a, first(p))

    def o_from(p):
        return rcopy(s1.at[p], r1.at[p], O1, p, p, first(p))

    def chip_max(p):
        here, there = mlw[p], rml0[p]
        top = jnp.maximum(here, there)
        total = jnp.exp(here - top) * pltpu.roll(here, 64, 1)
        total = total + jnp.exp(there - top) * pltpu.roll(there, 64, 1)
        ml1[p] = jnp.where(lane8 < 64, top, pltpu.roll(total, 64, 1))

    loop(SIDE, chip_max)
    peers(a, lambda p: mlsend(p).start())
    o_partner.wait_recv()

    def chip_sum(p):
        top = ml1[p]
        f_here = jnp.exp(mlw[p] - top)
        f_there = jnp.exp(rml0[p] - top)
        for k in range(half):
            fh = jnp.broadcast_to(f_here[:, k : k + 1], (8, 128))
            ft = jnp.broadcast_to(f_there[:, k : k + 1], (8, 128))
            fh = jnp.concatenate([fh, fh], axis=0)
            ft = jnp.concatenate([ft, ft], axis=0)
            s1[p, k] = (fh * ow[p, k] + ft * r0[p, k].astype(F32)).astype(BF16)

    def chip_send(p):
        chip_sum(p)
        osend(p).start()

    peers(a, chip_send)
    chip_sum(a)

    peers(a, lambda p: ml_from(p).wait_recv())
    rml1[a] = ml1[a]
    top = rml1[0]
    for p in range(1, SIDE):
        top = jnp.maximum(top, rml1[p])
    total = jnp.zeros((8, 128), F32)
    for p in range(SIDE):
        total = total + jnp.exp(rml1[p] - top) * pltpu.roll(rml1[p], 64, 1)
    packed = jnp.where(lane8 < 64, top, pltpu.roll(total, 64, 1))
    ml2[...] = packed

    def ml2_send(p):
        return rcopy(ml2, rml2.at[b], ML2, p, b, second(p))

    def ml2_from(p):
        return rcopy(ml2, rml2.at[p], ML2, p, p, second(p))

    peers(b, lambda p: ml2_send(p).start())
    peers(b, lambda p: ml2_from(p).wait_recv())
    rml2[b] = packed
    top = rml2[0]
    for p in range(1, SIDE):
        top = jnp.maximum(top, rml2[p])
    total = jnp.zeros((8, 128), F32)
    for p in range(SIDE):
        total = total + jnp.exp(rml2[p] - top) * pltpu.roll(rml2[p], 64, 1)
    for p in range(SIDE):
        fac[p] = jnp.exp(rml1[p] - top) / total

    def add(block, p, fresh):
        f = fac[p]
        for k in range(half):
            fk = jnp.broadcast_to(f[:, k : k + 1], (8, 128))
            term = jnp.concatenate([fk, fk], axis=0) * block[k].astype(F32)
            acc[k] = term if fresh else acc[k] + term

    add(s1.at[a], a, True)

    def take(p):
        o_from(p).wait_recv()
        add(r1.at[p], p, False)

    peers(a, take)

    @pl.when(c == 0)
    def _():
        for k in range(half):
            for d in range(2):
                ab[d * 192 + k * 8 : d * 192 + k * 8 + 8, :] = acc[k, 8 * d : 8 * d + 8, :]
        for j in range(SIDE):
            s2[j] = jnp.concatenate(
                [ab[pl.ds(d * 192 + j, ROWS, stride=8), :] for d in range(2)], axis=0
            ).astype(BF16)

    @pl.when(c == 1)
    def _():
        for k in range(half):
            for d in range(2):
                base = ((k % 2) * 2 + d) * 96 + (k // 2) * 8
                ab[base : base + 8, :] = acc[k, 8 * d : 8 * d + 8, :]
        for j in range(SIDE):
            s2[j] = jnp.concatenate(
                [ab[pl.ds(((j % 2) * 2 + d) * 96 + j // 2, ROWS, stride=4), :] for d in range(2)],
                axis=0,
            ).astype(BF16)

    def o2_send(p):
        return rcopy(s2.at[p], r2.at[b], O2, p, b, second(p))

    def o2_from(p):
        return rcopy(s2.at[p], r2.at[p], O2, p, p, second(p))

    peers(b, lambda p: o2_send(p).start())
    peers(b, lambda p: o2_from(p).wait_recv())
    r2[b] = s2[b]
    merged = r2[0].astype(F32)
    for p in range(1, SIDE):
        merged = merged + r2[p].astype(F32)

    part = jnp.zeros((ROWS, VD), F32)
    for k in range(2):
        block = merged[ROWS * k : ROWS * (k + 1)]
        high = block.astype(BF16)
        low = (block - high.astype(F32)).astype(BF16)
        part = part + jnp.dot(high, vu[k], preferred_element_type=F32)
        part = part + jnp.dot(low, vu[k], preferred_element_type=F32)
    vs[...] = part
    swap = dcopy(vs, vr, D_V, neighbour)
    swap.start()
    to_partner[3].wait_recv()
    swap.wait_recv()
    left = jnp.concatenate([(part + vr[...]).astype(BF16), lhs[...].astype(BF16)], axis=1)

    def a1_send(p):
        return rcopy(s3.at[p], r3.at[a], A1, p, a, first(p))

    def a1_from(p):
        return rcopy(s3.at[p], r3.at[p], A1, p, p, first(p))

    def a2_send(p):
        return rcopy(s4, r4.at[b], A2, p, b, second(p))

    def a2_from(p):
        return rcopy(s4, r4.at[p], A2, p, p, second(p))

    def a3_send(p):
        return rcopy(rf.at[a], rf.at[a], A3, p, a, first(p))

    def a3_from(p):
        return rcopy(rf.at[p], rf.at[p], A3, p, p, first(p))

    def project(p):
        out = jnp.dot(left, w[p], preferred_element_type=F32)
        blocks = [out[:, 128 * t : 128 * t + 128] for t in range(tiles)]
        blocks.append(jnp.zeros((8, 128), F32))
        s3[p] = jnp.concatenate(blocks, axis=0).astype(BF16)

    def project_send(p):
        project(p)
        a1_send(p).start()

    peers(a, project_send)
    project(a)
    peers(a, lambda p: a1_from(p).wait_recv())
    r3[a] = s3[a]
    total = r3[0].astype(F32)
    for p in range(1, SIDE):
        total = total + r3[p].astype(F32)
    s4[...] = total.astype(BF16)
    peers(b, lambda p: a2_send(p).start())
    peers(b, lambda p: a2_from(p).wait_recv())
    r4[b] = s4[...]
    total = r4[0].astype(F32)
    for p in range(1, SIDE):
        total = total + r4[p].astype(F32)
    rf[a] = total.astype(BF16)
    peers(a, lambda p: a3_send(p).start())
    peers(a, lambda p: a3_from(p).wait_recv())

    choose = pick[...][:, 0:ROWS]
    choose_b = choose.astype(BF16)
    squares = jnp.zeros((ROWS, 128), F32)
    largest = jnp.zeros((ROWS, 128), F32)
    for p in range(SIDE):
        block = rf[p].astype(F32)
        parts_r = [block[ROWS * t : ROWS * (t + 1)] for t in range(tiles)]
        gains = [v[half : half + 1] for v in parts_r]
        for v, gv in zip(parts_r, gains):
            squares = squares + v * v
            largest = jnp.maximum(largest, jnp.abs(v * gv))
        rows = jnp.concatenate(parts_r, axis=1).astype(BF16)
        chosen = jnp.dot(choose_b, rows, preferred_element_type=F32)
        y[p] = chosen * jnp.concatenate(gains, axis=1)
    inverse = lax.rsqrt(jnp.sum(squares, axis=1, keepdims=True) / cols + small_eps)
    peak = inverse * jnp.max(largest, axis=1, keepdims=True) + small_eps
    spread = jnp.concatenate(
        [jnp.broadcast_to(inverse / peak, (ROWS, 128)), jnp.broadcast_to(peak, (ROWS, 128))], axis=1
    )
    slots = jnp.dot(choose, spread, preferred_element_type=F32, precision=lax.Precision.HIGHEST)
    code = jnp.concatenate([slots[:, 0:128]] * tiles, axis=1)
    peaks = slots[:, 128:256]
    xs[...] = peaks[8:16]
    for k in range(SIDE // 2):
        fs[k] = jnp.concatenate(
            [y[2 * k + d, 8:16, :] * code[8:16] for d in range(2)], axis=0
        ).astype(BF16)
    x_partner = dcopy(xs, xr, D_X, partner)
    f_partner = dcopy(fs, fr, D_F, partner)
    x_partner.start()
    f_partner.start()
    x_partner.wait_recv()
    peaks = peaks[0:8] + xr[...]
    scale_slots = jnp.zeros((2, CAP), F32)
    for j in range(2):
        for k in range(CAP):
            here = (sublanes((2, CAP)) == j) & (lanes((2, CAP)) == k)
            r = CAP * j + k
            scale_slots = jnp.where(here, peaks[r : r + 1, 0:1], scale_slots)
    scale_out[...] = scale_slots
    f_partner.wait_recv()
    for k in range(SIDE // 2):
        there = fr[k].astype(F32)
        for d in range(2):
            p = 2 * k + d
            rows = (y[p, 0:8, :] * code[0:8] + there[8 * d : 8 * d + 8]).astype(BF16)
            for e in range(2):
                disp_out[e, :, pl.ds(p * width, width)] = rows[CAP * e : CAP * e + CAP]

    peers(a, lambda p: q1(p).wait_send())
    peers(b, lambda p: q2(p).wait_send())
    loop(SIDE, lambda p: qd(p).wait_send())
    peers(a, lambda p: mlsend(p).wait_send())
    peers(a, lambda p: osend(p).wait_send())
    peers(b, lambda p: ml2_send(p).wait_send())
    peers(b, lambda p: o2_send(p).wait_send())
    peers(a, lambda p: a1_send(p).wait_send())
    peers(b, lambda p: a2_send(p).wait_send())
    peers(a, lambda p: a3_send(p).wait_send())
    for copy in to_partner + [o_partner, ml_partner, swap, x_partner, f_partner]:
        copy.wait_send()


def per_device(
    queries, latent_cache, context_lengths, value_up, out_proj, residual, norm_gain, expert_ids,
    gate_weights,
):
    seqs, ctx_dev, entry = latent_cache.shape
    half = seqs // 2
    columns = out_proj.shape[1]
    width = columns // SIDE
    piece = residual.shape[1]
    experts = 2
    rows = (width // 128) * ROWS + 8
    any_space = pl.BlockSpec(memory_space=pl.ANY)
    vmem = pl.BlockSpec(memory_space=pltpu.VMEM)
    smem = pl.BlockSpec(memory_space=pltpu.SMEM)
    V = pltpu.VMEM
    chunk = (SIDE, half, 16, 128)
    eights = (SIDE, 8, 128)
    scratch = [
        V(queries.shape, BF16),
        V((seqs, 128), F32),
        V((2, SIDE, SIDE, seqs + 8, 128), BF16),
        V((H * 5 * seqs, 128), F32),
        V((seqs, entry, ctx_dev), BF16),
        V(chunk, BF16),
        V(chunk, BF16),
        V(eights, F32),
        V(eights, F32),
        V(chunk, F32),
        V(eights, F32),
        V(chunk, BF16),
        V(chunk, BF16),
        V(eights, F32),
        V(eights, F32),
        V((8, 128), F32),
        V(eights, F32),
        V(eights, F32),
        V(chunk[1:], F32),
        V((384, 128), F32),
        V((SIDE, 2 * ROWS, 128), BF16),
        V((SIDE, 2 * ROWS, 128), BF16),
        V((2, 128, VD), BF16),
        V((ROWS, VD), F32),
        V((ROWS, VD), F32),
        V((2, seqs, piece), BF16),
        V((2, 1, piece), BF16),
        V((seqs + 8, 128), F32),
        V((seqs + 8, 128), F32),
        V((ROWS, 128), F32),
        V((SIDE, 256, width), BF16),
        V((SIDE, rows, 128), BF16),
        V((SIDE, rows, 128), BF16),
        V((rows, 128), BF16),
        V((SIDE, rows, 128), BF16),
        V((SIDE, rows, 128), BF16),
        V(expert_ids.shape[::-1], jnp.int32),
        V(gate_weights.shape[::-1], F32),
        V((16, 128), F32),
        V((16, 128), F32),
        V((SIDE, 16, width), F32),
        V((SIDE // 2, 16, width), BF16),
        V((SIDE // 2, 16, width), BF16),
        V((8, 128), F32),
        V((8, 128), F32),
        pltpu.SemaphoreType.DMA((24,)),
        pltpu.SemaphoreType.DMA((10, SIDE)),
        pltpu.SemaphoreType.DMA((10, SIDE)),
        pltpu.SemaphoreType.DMA((9,)),
        pltpu.SemaphoreType.DMA((9,)),
    ]
    dispatched, slot_scale, slot_gate = pl.pallas_call(
        kernel,
        out_shape=(
            jax.ShapeDtypeStruct((experts, CAP, columns), BF16),
            jax.ShapeDtypeStruct((experts, CAP), F32),
            jax.ShapeDtypeStruct((experts, CAP), F32),
        ),
        in_specs=[any_space, any_space, smem] + [any_space] * 6,
        out_specs=(vmem, vmem, vmem),
        scratch_shapes=scratch,
        compiler_params=pltpu.CompilerParams(collective_id=0, has_side_effects=True),
    )(
        queries, latent_cache.transpose(0, 2, 1), context_lengths, value_up, out_proj, residual,
        norm_gain[None, :], expert_ids.T, gate_weights.T,
    )
    return dispatched, slot_scale, slot_gate


def solution(mesh):
    split = Mesh(
        mesh.devices.reshape(mesh.shape["groups"], SIDE, SIDE, 2),
        ("groups", "kv_0", "kv_1", "kv_2"),
    )
    in_specs = (
        P("groups", KV),
        P("groups", KV, None),
        P("groups"),
        P(KV, None),
        P(KV, None),
        P("groups", KV),
        P(KV),
        P("groups", None),
        P("groups", None),
    )
    out_specs = (P(GROUPS_KV, None, None), P(GROUPS_KV, None), P(GROUPS_KV, None))
    return jax.shard_map(
        per_device, mesh=split, in_specs=in_specs, out_specs=out_specs, check_vma=False
    )
```

```python
import functools

import jax
import jax.numpy as jnp
from jax import lax
from jax.experimental import pallas as pl
from jax.experimental.pallas import tpu as pltpu
from jax.sharding import Mesh
from jax.sharding import PartitionSpec as P

H = 32
LAT = 512
ROPE = 64
VD = 128
TOPK = 8
CAP = 2
SIDE = 8
QUARTERS = 4
ROWS = 24
PITCH = 5 * ROWS
A_GROUP = QUARTERS * PITCH + 8
KV = ("kv_0", "kv_1", "kv_2")
GROUPS_KV = ("groups", "kv_0", "kv_1", "kv_2")
MESH = pl.DeviceIdType.MESH
F32 = jnp.float32
BF16 = jnp.bfloat16

score_scale = 192.0 ** (-0.5)
masked_score = -1e30
small_eps = 1e-06

Q1, QD, O1, O1B, ML1, ML2, O2, A1, A2, A3 = range(10)
D_VU, D_RES, D_GAIN, D_W, D_O, D_OB, D_ML, D_F, D_X, D_V = range(10)


def lanes(shape):
    return lax.broadcasted_iota(jnp.int32, shape, len(shape) - 1)


def sublanes(shape):
    return lax.broadcasted_iota(jnp.int32, shape, len(shape) - 2)


def loop(count, body):
    def step(i, carry):
        body(i)
        return carry

    lax.fori_loop(0, count, step, 0)


def far_first(i):
    return SIDE // 2 + (1 - 2 * lax.rem(i, 2)) * lax.div(i + 1, 2)


def kernel(
    q_in, cache_in, ctx, vu_in, op_in, res_in, gain_in, ids_in, gate_in,
    disp_out, scale_out, gate_out,
    qraw, ext, qb, qa, qc, cache, wb, s0, r0, rml0, ow, mlo, s1, r1, ml1, rml1,
    ml2, rml2, fown, fpar, wown, wpar, acc, ab, s2, r2, vu, vs, vr, res, gain, ta, tb, lhs, w,
    s3, r3, s4, r4, rf, ids, gate, pt, pick, y, fs, fr, xs, xr,
    loc, ssem, rsem, qsend, qrecv, dsend, drecv, steps,
):
    g = lax.axis_index("groups")
    yy = lax.axis_index("kv_0")
    xx = lax.axis_index("kv_1")
    c = lax.axis_index("kv_2")
    chip = yy * SIDE + xx
    dev = chip * 2 + c
    a = xx + c * (yy - xx)
    b = yy + c * (xx - yy)
    half_x = lax.rem(xx, 2)
    seqs, ctx_dev = cache.shape[0], cache.shape[2]
    half = seqs // 2
    width = w.shape[2]
    tiles = width // 128
    cols = SIDE * width

    def first(p):
        return (g, yy + c * (p - yy), xx + (1 - c) * (p - xx), c)

    def second(p):
        return (g, yy + (1 - c) * (p - yy), xx + c * (p - xx), c)

    partner = (g, yy, xx, 1 - c)
    neighbour = (g, yy, xx + 1 - 2 * half_x, c)

    def rcopy(src, dst, phase, to, frm, device):
        return pltpu.make_async_remote_copy(
            src_ref=src, dst_ref=dst, send_sem=ssem.at[phase, to], recv_sem=rsem.at[phase, frm],
            device_id=device, device_id_type=MESH,
        )

    def dcopy(src, dst, which, device):
        return pltpu.make_async_remote_copy(
            src_ref=src, dst_ref=dst, send_sem=dsend.at[which], recv_sem=drecv.at[which],
            device_id=device, device_id_type=MESH,
        )

    def peers(me, body):
        def one(i):
            body(lax.rem(me + far_first(i), SIDE))

        loop(SIDE - 1, one)

    def local(src, dst, k):
        return pltpu.make_async_copy(src, dst, loc.at[k])

    w_row = pl.multiple_of(half_x * 64 + c * 32, 32)
    q_load = local(q_in, qraw, 0)
    q_load.start()
    small = [
        local(vu_in, vu.at[c], 1),
        local(res_in, res.at[c], 2),
        local(gain_in, gain.at[c], 21),
        local(ids_in, ids, 3),
        local(gate_in, gate, 4),
    ]
    for copy in small:
        copy.start()
    w_loads = [
        local(op_in.at[:, pl.ds(p * width, width)], w.at[p, pl.ds(w_row, 32), :], 5 + p)
        for p in range(SIDE)
    ]
    for copy in w_loads:
        copy.start()
    parts = 8
    each = seqs // parts
    k_loads = [
        local(cache_in.at[pl.ds(each * p, each)], cache.at[pl.ds(each * p, each)], 13 + p)
        for p in range(parts)
    ]
    for copy in k_loads:
        copy.start()

    barrier = pltpu.get_barrier_semaphore()
    pl.semaphore_signal(barrier, inc=1, device_id=partner, device_id_type=MESH)

    def greet(p):
        pl.semaphore_signal(barrier, inc=1, device_id=first(p), device_id_type=MESH)

    def greet_second(p):
        pl.semaphore_signal(barrier, inc=1, device_id=second(p), device_id_type=MESH)

    peers(a, greet)
    peers(b, greet_second)

    ext[...] = jnp.zeros(ext.shape, F32)
    q_load.wait()
    quarter = half_x * 2 + c
    ext[:, 0:16] = qraw[:, 128:144].astype(F32)
    main = pltpu.roll(qraw[:, 0:128].astype(F32), quarter * 16, 1)
    extra = jnp.zeros((8, 128), F32)
    for k in range(seqs // 8):
        extra = extra + pltpu.roll(ext[8 * k : 8 * k + 8, :], lax.rem(quarter + k, 8) * 16, 1)
    qb[c, b, a] = jnp.concatenate([main, extra], axis=0).astype(BF16)

    pl.semaphore_wait(barrier, 2 * (SIDE - 1) + 1)

    def q1(p):
        return rcopy(qb.at[c, b, a], qb.at[c, b, a], Q1, p, a, first(p))

    def q1_from(p):
        return rcopy(qb.at[c, b, p], qb.at[c, b, p], Q1, p, p, first(p))

    def q2(slot, source, chunk, to):
        block = qb.at[c, source, chunk]
        return pltpu.make_async_remote_copy(
            src_ref=block, dst_ref=block, send_sem=qsend.at[slot, chunk],
            recv_sem=qrecv.at[source, chunk], device_id=second(to), device_id_type=MESH,
        )

    def at(me, distance):
        return lax.rem(me + distance, SIDE)

    def qd(p):
        return rcopy(qb.at[c, p], qb.at[c, p], QD, p, p, partner)

    def qd_from(p):
        return rcopy(qb.at[1 - c, p], qb.at[1 - c, p], QD, p, p, partner)

    peers(a, lambda p: q1(p).start())

    def spread(distances):
        for d in distances:
            chunk = at(a, d)
            if d:
                q1_from(chunk).wait_recv()
            for e in (2, 6, 1, 7):
                q2(e, b, chunk, at(b, e)).start()

    def relay(distances):
        for d in distances:
            chunk = at(a, d)
            source = at(b, 6)
            q2(1, source, chunk, source).wait_recv()
            q2(3, source, chunk, at(b, 1)).start()
            if d % 2 == 0:
                q2(4, source, chunk, at(b, 2)).start()
            source = at(b, 2)
            q2(1, source, chunk, source).wait_recv()
            q2(5, source, chunk, at(b, 7)).start()
            if d % 2 == 1:
                q2(0, source, chunk, at(b, 6)).start()

    spread((0,))
    spread((1, 7))
    spread((2, 6))
    relay((0,))
    spread((3, 5))
    spread((4,))
    relay((1, 7))
    qd(b).start()
    relay((2, 6))
    relay((3, 5))
    relay((4,))
    qd(at(b, 2)).start()
    qd(at(b, 6)).start()

    for copy in small:
        copy.wait()
    for copy in w_loads:
        copy.wait()
    w_rows = w.at[:, pl.ds(w_row, 32), :]
    to_partner = [
        dcopy(vu.at[c], vu.at[c], D_VU, partner),
        dcopy(res.at[c], res.at[c], D_RES, partner),
        dcopy(gain.at[c], gain.at[c], D_GAIN, partner),
        dcopy(w_rows, w_rows, D_W, partner),
    ]
    for copy in to_partner[:3]:
        copy.start()

    for ref in (mlo, ab, ta, tb, pt):
        ref[...] = jnp.zeros(ref.shape, F32)
    for e in (1, 7, 3, 5, 4):
        source = at(b, e)
        loop(SIDE, lambda k: q2(1, source, k, source).wait_recv())
        qd(source).start()
    to_partner[3].start()
    loop(SIDE, lambda p: qd_from(p).wait_recv())

    lane = lanes((seqs, 128))

    lane8 = lanes((8, 128))

    def assemble(hy):
        for hg in range(QUARTERS):
            m = [
                qb[0, hy, 2 * hg].astype(F32),
                qb[1, 2 * hg, hy].astype(F32),
                qb[0, hy, 2 * hg + 1].astype(F32),
                qb[1, 2 * hg + 1, hy].astype(F32),
            ]
            extras = []
            for k in range(seqs // 8):
                picked = m[0][seqs:]
                for i in range(1, QUARTERS):
                    picked = jnp.where(lax.div(lane8, 16) == (k + i) % 8, m[i][seqs:], picked)
                extras.append(pltpu.roll(picked, (128 - 16 * k) % 128, 1))
            e = jnp.concatenate(extras, axis=0)
            m = [v[:seqs] for v in m]
            whole = [
                m[0],
                jnp.where(lane < 16, e, m[1]),
                jnp.where(lane < 16, m[1], jnp.where(lane < 32, e, m[2])),
                jnp.where(lane < 32, m[2], jnp.where(lane < 48, e, m[3])),
                jnp.where(lane < 48, m[3], e),
            ]
            for t in range(5):
                rows = pl.multiple_of(hy * A_GROUP + hg * PITCH + t * ROWS, 8)
                qa[pl.ds(rows, ROWS), :] = whole[t][:ROWS]
                rows = pl.multiple_of((hy * QUARTERS + hg) * PITCH + t * ROWS, 8)
                qc[pl.ds(rows, ROWS), :] = whole[t][seqs - ROWS :]

    loop(SIDE, assemble)

    for copy in k_loads:
        copy.wait()
    position = dev * ctx_dev + lanes((1, ctx_dev))
    part_k = half // 2

    def weigh(s, by_column):
        pieces = []
        for t in range(5):
            groups = []
            for k in range(4):
                if by_column:
                    rows = pl.ds(k * PITCH + t * ROWS + s, 8, stride=A_GROUP)
                    groups.append(qa[rows, :])
                else:
                    rows = pl.ds(8 * k * PITCH + t * ROWS + s - (seqs - ROWS), 8, stride=PITCH)
                    groups.append(qc[rows, :])
            pieces.append(jnp.concatenate(groups, axis=0).astype(BF16))
        q = jnp.concatenate(pieces, axis=1)[:, : LAT + ROPE]
        scores = jnp.dot(q, cache[s], preferred_element_type=F32)
        valid = position < ctx[s]
        scores = jnp.where(valid, scores * score_scale, masked_score)
        top = jnp.max(scores, axis=1, keepdims=True)
        weights = jnp.where(valid, jnp.exp(scores - top), 0.0)
        total = jnp.sum(weights, axis=1, keepdims=True)
        wb[s] = weights.astype(BF16)
        return top, total

    low = sublanes((8, 128)) < 4

    def merge(u, v, first_rows):
        if first_rows:
            return jnp.where(low, u, pltpu.roll(v, 4, 0))
        return jnp.where(low, pltpu.roll(u, 4, 0), v)

    def put(tile, k, top, total):
        return jnp.where(lane8 == k, top, jnp.where(lane8 == 64 + k, total, tile))

    def weigh_columns(i):
        tiles_m = [jnp.zeros((8, 128), F32) for _ in range(4)]
        for u in range(part_k):
            s = i * part_k + u
            top, total = weigh(s, True)
            for k in range(4):
                rows = slice(8 * k, 8 * k + 8)
                tiles_m[k] = put(tiles_m[k], s, top[rows], total[rows])
        for k in range(4):
            for d in range(2):
                mlo[0, 2 * k + d] += tiles_m[k]

    def weigh_rows(i):
        tiles_m = [jnp.zeros((8, 128), F32) for _ in range(SIDE)]
        for u in range(part_k // 2):
            pair = i * (part_k // 2) + u
            t0, l0 = weigh(half + 2 * pair, False)
            t1, l1 = weigh(half + 2 * pair + 1, False)
            for k in range(4):
                rows = slice(8 * k, 8 * k + 8)
                wide = [jnp.broadcast_to(v[rows], (8, 128)) for v in (t0, t1, l0, l1)]
                for d in range(2):
                    top = merge(wide[0], wide[1], d == 0)
                    total = merge(wide[2], wide[3], d == 0)
                    for e in range(2):
                        tile = tiles_m[2 * k + d]
                        tiles_m[2 * k + d] = put(tile, 2 * pair + e, top, total)
        for p in range(SIDE):
            mlo[1, p] += tiles_m[p]

    loop(2, weigh_columns)
    loop(2, weigh_rows)
    ml_partner = dcopy(mlo.at[1 - c], rml0, D_ML, partner)
    ml_partner.start()

    def attend(s):
        return lax.dot_general(
            wb[s], cache[s, 0:LAT, :], (((1,), (1,)), ((), ())), preferred_element_type=F32
        )

    def by_column(dst, i):
        for u in range(part_k):
            out = attend(i * part_k + u)
            for k in range(4):
                rows = slice(8 * k, 8 * k + 8)
                for d in range(2):
                    lo = out[rows, 256 * d : 256 * d + 128]
                    hi = out[rows, 256 * d + 128 : 256 * d + 256]
                    dst[i, 2 * k + d, u] = jnp.concatenate([lo, hi], axis=0).astype(dst.dtype)

    def by_row(dst, i):
        for u in range(part_k // 2):
            s = half + i * part_k + 2 * u
            o0 = attend(s)
            o1 = attend(s + 1)
            for k in range(4):
                rows = slice(8 * k, 8 * k + 8)
                for d in range(2):
                    for e in range(2):
                        blocks = [
                            merge(
                                o0[rows, 128 * t : 128 * t + 128],
                                o1[rows, 128 * t : 128 * t + 128],
                                d == 0,
                            )
                            for t in (2 * e, 2 * e + 1)
                        ]
                        dst[i, 2 * k + d, 2 * u + e] = jnp.concatenate(blocks, axis=0).astype(
                            dst.dtype
                        )

    def o_partner(i):
        return dcopy(s0.at[i], r0.at[i], D_O + i, partner)

    def for_partner(i):
        @pl.when(c == 0)
        def _():
            by_row(s0, i)

        @pl.when(c == 1)
        def _():
            by_column(s0, i)

        o_partner(i).start()

    loop(2, for_partner)

    ml_partner.wait_recv()

    def mlsend(p):
        return rcopy(ml1.at[p], rml1.at[a], ML1, p, a, first(p))

    def ml_from(p):
        return rcopy(ml1.at[p], rml1.at[p], ML1, p, p, first(p))

    def osend(i, p):
        return rcopy(s1.at[i, p], r1.at[i, a], O1 + i, p, a, first(p))

    def o_from(i, p):
        return rcopy(s1.at[i, p], r1.at[i, p], O1 + i, p, p, first(p))

    for p in range(SIDE):
        here, there = mlo[c, p], rml0[p]
        top = jnp.maximum(here, there)
        f_here = jnp.exp(here - top)
        f_there = jnp.exp(there - top)
        total = f_here * pltpu.roll(here, 64, 1) + f_there * pltpu.roll(there, 64, 1)
        ml1[p] = jnp.where(lane8 < 64, top, pltpu.roll(total, 64, 1))
        fown[p] = f_here
        fpar[p] = f_there
    peers(a, lambda p: mlsend(p).start())

    def widen(wide, p, f):
        for k in range(half):
            wide[p, k] = jnp.broadcast_to(f[:, k : k + 1], (8, 128))

    def twice(f):
        return jnp.concatenate([f, f], axis=0)

    def widen_both(i):
        for d in range(2):
            widen(wown, 2 * i + d, fown[2 * i + d])
            widen(wpar, 2 * i + d, fpar[2 * i + d])

    loop(SIDE // 2, widen_both)

    def chip_sum(i, p):
        for k in range(part_k):
            fh = twice(wown[p, i * part_k + k])
            ft = twice(wpar[p, i * part_k + k])
            s1[i, p, k] = (fh * ow[i, p, k] + ft * r0[i, p, k].astype(F32)).astype(BF16)

    def for_self(i):
        @pl.when(c == 0)
        def _():
            by_column(ow, i)

        @pl.when(c == 1)
        def _():
            by_row(ow, i)

        o_partner(i).wait_recv()

        def chip_send(p):
            chip_sum(i, p)
            osend(i, p).start()

        peers(a, chip_send)
        chip_sum(i, a)

    loop(2, for_self)

    peers(a, lambda p: ml_from(p).wait_recv())
    rml1[a] = ml1[a]
    row_top = rml1[0]
    for p in range(1, SIDE):
        row_top = jnp.maximum(row_top, rml1[p])
    total = jnp.zeros((8, 128), F32)
    for p in range(SIDE):
        factor = jnp.exp(rml1[p] - row_top)
        total = total + factor * pltpu.roll(rml1[p], 64, 1)
        fown[p] = factor
    packed = jnp.where(lane8 < 64, row_top, pltpu.roll(total, 64, 1))
    ml2[...] = packed

    def ml2_send(p):
        return rcopy(ml2, rml2.at[b], ML2, p, b, second(p))

    def ml2_from(p):
        return rcopy(ml2, rml2.at[p], ML2, p, p, second(p))

    peers(b, lambda p: ml2_send(p).start())

    def widen_row(i):
        for d in range(2):
            widen(wown, 2 * i + d, fown[2 * i + d])

    loop(SIDE // 2, widen_row)

    idle_row = pl.multiple_of((1 - half_x) * 64, 64)

    def fill(p):
        w[p, pl.ds(idle_row, 64), :] = jnp.zeros((64, width), BF16)

        def block(k):
            start = pl.multiple_of(k * 16, 16)
            row = start + sublanes((16, width))
            column = p * width + lanes((16, width))
            target = chip * 112 + lax.rem(row, 64) + 56 * lax.div(row, 64)
            hit = jnp.where((column == target) & (lax.rem(row, 64) < 56), 1.0, 0.0)
            w[p, pl.ds(pl.multiple_of(128 + start, 16), 16), :] = hit.astype(BF16)

        loop(8, block)

    loop(SIDE, fill)

    idv = ids[...]
    gatev = gate[...]
    hits = jnp.zeros((8, seqs), F32)
    hit_rows = []
    gates = []
    for j in range(4):
        expert = (dev if j < 2 else chip * 2 + 1 - c) * 2 + j % 2
        same = idv == expert
        hit = jnp.sum(jnp.where(same, 1.0, 0.0), axis=0, keepdims=True)
        hit_rows.append(hit)
        gates.append(jnp.sum(jnp.where(same, gatev, 0.0), axis=0, keepdims=True))
        hits = jnp.where(sublanes((8, seqs)) == j, hit, hits)
    earlier = jnp.where(sublanes((seqs, seqs)) < lanes((seqs, seqs)), 1.0, 0.0)
    rank = jnp.dot(hits.astype(BF16), earlier.astype(BF16), preferred_element_type=F32)
    table = jnp.zeros((16, seqs), F32)
    gate_slots = jnp.zeros((2, CAP), F32)
    for j in range(4):
        for k in range(CAP):
            chosen = jnp.where(rank[j : j + 1] == float(k), hit_rows[j], 0.0)
            r = (j // 2) * 8 + (j % 2) * CAP + k
            table = jnp.where(sublanes((16, seqs)) == r, chosen, table)
            if j < 2:
                total = jnp.sum(chosen * gates[j], axis=1, keepdims=True)
                here = (sublanes((2, CAP)) == j) & (lanes((2, CAP)) == k)
                gate_slots = jnp.where(here, total, gate_slots)
    gate_out[...] = gate_slots
    pt[:, 0:seqs] = table
    own = jnp.where(c == 0, pt[...], pltpu.roll(pt[...], 128 - half, 1))
    pick[...] = jnp.where(lanes((16, 128)) < half, own, 0.0)

    for copy in to_partner[:3]:
        copy.wait_recv()
    ta[0:seqs, 0:56] = res[0].astype(F32)
    tb[0:seqs, 0:56] = res[1].astype(F32)
    ta[seqs : seqs + 1, 0:56] = gain[0].astype(F32)
    tb[seqs : seqs + 1, 0:56] = gain[1].astype(F32)
    both = ta[...] + pltpu.roll(tb[...], 64, 1)
    ta[...] = both
    row = sublanes((ROWS, 128))
    mine = jnp.where(c == 0, ta[0:ROWS, :], ta[half : half + ROWS, :])
    gain_row = jnp.broadcast_to(ta[seqs : seqs + 1, :], (ROWS, 128))
    lhs[...] = jnp.where(row < half, mine, jnp.where(row == half, gain_row, 0.0))

    def add(block, i, p, fresh):
        for k in range(part_k):
            index = i * part_k + k
            term = twice(wown[p, index]) * block[k].astype(F32)
            acc[index] = term if fresh else acc[index] + term

    def gather(i):
        add(s1.at[i, a], i, a, True)

        def take(p):
            o_from(i, p).wait_recv()
            add(r1.at[i, p], i, p, False)

        peers(a, take)

    loop(2, gather)
    peers(b, lambda p: ml2_from(p).wait_recv())
    rml2[b] = packed
    top = rml2[0]
    for p in range(1, SIDE):
        top = jnp.maximum(top, rml2[p])
    total = jnp.zeros((8, 128), F32)
    for p in range(SIDE):
        total = total + jnp.exp(rml2[p] - top) * pltpu.roll(rml2[p], 64, 1)
    final = jnp.exp(row_top - top) / total
    for k in range(half):
        acc[k] = acc[k] * twice(jnp.broadcast_to(final[:, k : k + 1], (8, 128)))

    @pl.when(c == 0)
    def _():
        for k in range(half):
            for d in range(2):
                ab[d * 192 + k * 8 : d * 192 + k * 8 + 8, :] = acc[k, 8 * d : 8 * d + 8, :]
        for j in range(SIDE):
            s2[j] = jnp.concatenate(
                [ab[pl.ds(d * 192 + j, ROWS, stride=8), :] for d in range(2)], axis=0
            ).astype(BF16)

    @pl.when(c == 1)
    def _():
        for k in range(half):
            for d in range(2):
                base = ((k % 2) * 2 + d) * 96 + (k // 2) * 8
                ab[base : base + 8, :] = acc[k, 8 * d : 8 * d + 8, :]
        for j in range(SIDE):
            s2[j] = jnp.concatenate(
                [ab[pl.ds(((j % 2) * 2 + d) * 96 + j // 2, ROWS, stride=4), :] for d in range(2)],
                axis=0,
            ).astype(BF16)

    def o2_send(p):
        return rcopy(s2.at[p], r2.at[b], O2, p, b, second(p))

    def o2_from(p):
        return rcopy(s2.at[p], r2.at[p], O2, p, p, second(p))

    peers(b, lambda p: o2_send(p).start())
    peers(b, lambda p: o2_from(p).wait_recv())
    r2[b] = s2[b]
    merged = r2[0].astype(F32)
    for p in range(1, SIDE):
        merged = merged + r2[p].astype(F32)

    part = jnp.zeros((ROWS, VD), F32)
    for k in range(2):
        block = merged[ROWS * k : ROWS * (k + 1)]
        high = block.astype(BF16)
        low = (block - high.astype(F32)).astype(BF16)
        part = part + jnp.dot(high, vu[k], preferred_element_type=F32)
        part = part + jnp.dot(low, vu[k], preferred_element_type=F32)
    vs[...] = part
    swap = dcopy(vs, vr, D_V, neighbour)
    swap.start()
    to_partner[3].wait_recv()
    swap.wait_recv()
    left = jnp.concatenate([(part + vr[...]).astype(BF16), lhs[...].astype(BF16)], axis=1)

    def a1_send(p):
        return rcopy(s3.at[p], r3.at[a], A1, p, a, first(p))

    def a1_from(p):
        return rcopy(s3.at[p], r3.at[p], A1, p, p, first(p))

    def a2_send(p):
        return rcopy(s4, r4.at[b], A2, p, b, second(p))

    def a2_from(p):
        return rcopy(s4, r4.at[p], A2, p, p, second(p))

    def a3_send(p):
        return rcopy(rf.at[a], rf.at[a], A3, p, a, first(p))

    def a3_from(p):
        return rcopy(rf.at[p], rf.at[p], A3, p, p, first(p))

    def in_step(k):
        pl.semaphore_signal(steps.at[k], inc=1, device_id=partner, device_id_type=MESH)
        pl.semaphore_wait(steps.at[k], 1)

    def project(p):
        out = jnp.dot(left, w[p], preferred_element_type=F32)
        blocks = [out[:half, 128 * t : 128 * t + 128] for t in range(tiles)]
        blocks += [out[half : half + 1, 128 * t : 128 * t + 128] for t in range(tiles)]
        blocks.append(jnp.zeros((rf.shape[1] - tiles * (half + 1), 128), F32))
        s3[p] = jnp.concatenate(blocks, axis=0).astype(BF16)

    def project_send(p):
        project(p)
        a1_send(p).start()

    in_step(0)
    peers(a, project_send)
    project(a)
    peers(a, lambda p: a1_from(p).wait_recv())
    r3[a] = s3[a]
    total = r3[0].astype(F32)
    for p in range(1, SIDE):
        total = total + r3[p].astype(F32)
    s4[...] = total.astype(BF16)
    in_step(1)
    peers(b, lambda p: a2_send(p).start())
    peers(a, lambda p: q1(p).wait_send())
    for d in range(SIDE):
        chunk = at(a, d)
        for slot in (1, 2, 3, 5, 6, 7, 4 if d % 2 == 0 else 0):
            q2(slot, b, chunk, at(b, 1)).wait_send()
    loop(SIDE, lambda p: qd(p).wait_send())
    peers(a, lambda p: mlsend(p).wait_send())
    for i in range(2):
        peers(a, lambda p: osend(i, p).wait_send())
        o_partner(i).wait_send()
    peers(b, lambda p: ml2_send(p).wait_send())
    peers(b, lambda p: o2_send(p).wait_send())
    for copy in to_partner + [ml_partner, swap]:
        copy.wait_send()
    peers(b, lambda p: a2_from(p).wait_recv())
    r4[b] = s4[...]
    total = r4[0].astype(F32)
    for p in range(1, SIDE):
        total = total + r4[p].astype(F32)
    rf[a] = total.astype(BF16)
    in_step(2)
    peers(a, lambda p: a3_send(p).start())
    peers(a, lambda p: a1_send(p).wait_send())
    peers(b, lambda p: a2_send(p).wait_send())
    peers(a, lambda p: a3_from(p).wait_recv())

    choose = pick[...][:, 0:half]
    choose_b = choose.astype(BF16)
    squares = jnp.zeros((half, 128), F32)
    largest = jnp.zeros((half, 128), F32)
    for p in range(SIDE):
        block = rf[p].astype(F32)
        parts_r = [block[half * t : half * (t + 1)] for t in range(tiles)]
        gains = [block[half * tiles + t : half * tiles + t + 1] for t in range(tiles)]
        for v, gv in zip(parts_r, gains):
            squares = squares + v * v
            largest = jnp.maximum(largest, jnp.abs(v * gv))
        rows = jnp.concatenate(parts_r, axis=1).astype(BF16)
        chosen = jnp.dot(choose_b, rows, preferred_element_type=F32)
        y[p] = chosen * jnp.concatenate(gains, axis=1)
    inverse = lax.rsqrt(jnp.sum(squares, axis=1, keepdims=True) / cols + small_eps)
    peak = inverse * jnp.max(largest, axis=1, keepdims=True) + small_eps
    spread = jnp.concatenate(
        [jnp.broadcast_to(inverse / peak, (half, 128)), jnp.broadcast_to(peak, (half, 128))], axis=1
    )
    slots = jnp.dot(choose, spread, preferred_element_type=F32, precision=lax.Precision.HIGHEST)
    code = jnp.concatenate([slots[:, 0:128]] * tiles, axis=1)
    peaks = slots[:, 128:256]
    xs[...] = peaks[8:16]
    for k in range(SIDE // 2):
        fs[k] = jnp.concatenate(
            [y[2 * k + d, 8:16, :] * code[8:16] for d in range(2)], axis=0
        ).astype(BF16)
    x_partner = dcopy(xs, xr, D_X, partner)
    f_partner = dcopy(fs, fr, D_F, partner)
    x_partner.start()
    f_partner.start()
    x_partner.wait_recv()
    peaks = peaks[0:8] + xr[...]
    scale_slots = jnp.zeros((2, CAP), F32)
    for j in range(2):
        for k in range(CAP):
            here = (sublanes((2, CAP)) == j) & (lanes((2, CAP)) == k)
            r = CAP * j + k
            scale_slots = jnp.where(here, peaks[r : r + 1, 0:1], scale_slots)
    scale_out[...] = scale_slots
    f_partner.wait_recv()
    for k in range(SIDE // 2):
        there = fr[k].astype(F32)
        for d in range(2):
            p = 2 * k + d
            rows = (y[p, 0:8, :] * code[0:8] + there[8 * d : 8 * d + 8]).astype(BF16)
            for e in range(2):
                disp_out[e, :, pl.ds(p * width, width)] = rows[CAP * e : CAP * e + CAP]

    peers(a, lambda p: a3_send(p).wait_send())
    x_partner.wait_send()
    f_partner.wait_send()


def per_device(
    queries, latent_cache, context_lengths, value_up, out_proj, residual, norm_gain, expert_ids,
    gate_weights,
):
    seqs, ctx_dev, entry = latent_cache.shape
    half = seqs // 2
    columns = out_proj.shape[1]
    width = columns // SIDE
    piece = residual.shape[1]
    experts = 2
    rows = -(-(width // 128) * (half + 1) // 8) * 8
    any_space = pl.BlockSpec(memory_space=pl.ANY)
    vmem = pl.BlockSpec(memory_space=pltpu.VMEM)
    smem = pl.BlockSpec(memory_space=pltpu.SMEM)
    V = pltpu.VMEM
    chunk = (2, SIDE, half // 2, 16, 128)
    eights = (SIDE, 8, 128)
    scratch = [
        V(queries.shape, BF16),
        V((seqs, 128), F32),
        V((2, SIDE, SIDE, seqs + 8, 128), BF16),
        V((SIDE * A_GROUP, 128), F32),
        V((H * PITCH, 128), F32),
        V((seqs, entry, ctx_dev), BF16),
        V((seqs, H, ctx_dev), BF16),
        V(chunk, BF16),
        V(chunk, BF16),
        V(eights, F32),
        V(chunk, F32),
        V((2,) + eights, F32),
        V(chunk, BF16),
        V(chunk, BF16),
        V(eights, F32),
        V(eights, F32),
        V((8, 128), F32),
        V(eights, F32),
        V(eights, F32),
        V(eights, F32),
        V((SIDE, half, 8, 128), F32),
        V((SIDE, half, 8, 128), F32),
        V((half, 16, 128), F32),
        V((384, 128), F32),
        V((SIDE, 2 * ROWS, 128), BF16),
        V((SIDE, 2 * ROWS, 128), BF16),
        V((2, 128, VD), BF16),
        V((ROWS, VD), F32),
        V((ROWS, VD), F32),
        V((2, seqs, piece), BF16),
        V((2, 1, piece), BF16),
        V((seqs + 8, 128), F32),
        V((seqs + 8, 128), F32),
        V((ROWS, 128), F32),
        V((SIDE, 256, width), BF16),
        V((SIDE, rows, 128), BF16),
        V((SIDE, rows, 128), BF16),
        V((rows, 128), BF16),
        V((SIDE, rows, 128), BF16),
        V((SIDE, rows, 128), BF16),
        V(expert_ids.shape[::-1], jnp.int32),
        V(gate_weights.shape[::-1], F32),
        V((16, 128), F32),
        V((16, 128), F32),
        V((SIDE, 16, width), F32),
        V((SIDE // 2, 16, width), BF16),
        V((SIDE // 2, 16, width), BF16),
        V((8, 128), F32),
        V((8, 128), F32),
        pltpu.SemaphoreType.DMA((24,)),
        pltpu.SemaphoreType.DMA((10, SIDE)),
        pltpu.SemaphoreType.DMA((10, SIDE)),
        pltpu.SemaphoreType.DMA((SIDE, SIDE)),
        pltpu.SemaphoreType.DMA((SIDE, SIDE)),
        pltpu.SemaphoreType.DMA((10,)),
        pltpu.SemaphoreType.DMA((10,)),
        pltpu.SemaphoreType.REGULAR((3,)),
    ]
    dispatched, slot_scale, slot_gate = pl.pallas_call(
        kernel,
        out_shape=(
            jax.ShapeDtypeStruct((experts, CAP, columns), BF16),
            jax.ShapeDtypeStruct((experts, CAP), F32),
            jax.ShapeDtypeStruct((experts, CAP), F32),
        ),
        in_specs=[any_space, any_space, smem] + [any_space] * 6,
        out_specs=(vmem, vmem, vmem),
        scratch_shapes=scratch,
        compiler_params=pltpu.CompilerParams(collective_id=0, has_side_effects=True),
    )(
        queries, latent_cache.transpose(0, 2, 1), context_lengths, value_up, out_proj, residual,
        norm_gain[None, :], expert_ids.T, gate_weights.T,
    )
    return dispatched, slot_scale, slot_gate


def solution(mesh):
    split = Mesh(
        mesh.devices.reshape(mesh.shape["groups"], SIDE, SIDE, 2),
        ("groups", "kv_0", "kv_1", "kv_2"),
    )
    in_specs = (
        P("groups", KV),
        P("groups", KV, None),
        P("groups"),
        P(KV, None),
        P(KV, None),
        P("groups", KV),
        P(KV),
        P("groups", None),
        P("groups", None),
    )
    out_specs = (P(GROUPS_KV, None, None), P(GROUPS_KV, None), P(GROUPS_KV, None))
    return jax.shard_map(
        per_device, mesh=split, in_specs=in_specs, out_specs=out_specs, check_vma=False
    )
```

```python
import functools

import jax
import jax.numpy as jnp
from jax import lax
from jax.experimental import pallas as pl
from jax.experimental.pallas import tpu as pltpu
from jax.sharding import Mesh
from jax.sharding import PartitionSpec as P

H = 32
LAT = 512
ROPE = 64
VD = 128
TOPK = 8
CAP = 2
SIDE = 8
QUARTERS = 4
ROWS = 24
PITCH = 5 * ROWS
A_GROUP = QUARTERS * PITCH + 8
KV = ("kv_0", "kv_1", "kv_2")
GROUPS_KV = ("groups", "kv_0", "kv_1", "kv_2")
MESH = pl.DeviceIdType.MESH
F32 = jnp.float32
BF16 = jnp.bfloat16

score_scale = 192.0 ** (-0.5)
masked_score = -1e30
small_eps = 1e-06

Q1, Q1B, O1, O1B, ML1, ML2, O2, A1, A2, A3 = range(10)
D_VU, D_RES, D_GAIN, D_W, D_F, D_X, D_V = range(7)


def lanes(shape):
    return lax.broadcasted_iota(jnp.int32, shape, len(shape) - 1)


def sublanes(shape):
    return lax.broadcasted_iota(jnp.int32, shape, len(shape) - 2)


def loop(count, body):
    def step(i, carry):
        body(i)
        return carry

    lax.fori_loop(0, count, step, 0)


def far_first(i):
    return SIDE // 2 + (1 - 2 * lax.rem(i, 2)) * lax.div(i + 1, 2)


def kernel(
    q_in, cache_in, ctx, vu_in, op_in, res_in, gain_in, ids_in, gate_in,
    disp_out, scale_out, gate_out,
    qraw, ext, main, qs, qb, qa, cache, wb, s1, r1, ml1, rml1,
    ml2, rml2, fown, wown, acc, ab, s2, r2, vu, vs, vr, res, gain, ta, tb, lhs, w,
    s3, r3, s4, r4, rf, ids, gate, pt, pick, y, fs, fr, xs, xr,
    loc, ssem, rsem, qsend, qrecv, ksend, krecv, dsend, drecv, steps,
):
    g = lax.axis_index("groups")
    yy = lax.axis_index("kv_0")
    xx = lax.axis_index("kv_1")
    c = lax.axis_index("kv_2")
    chip = yy * SIDE + xx
    dev = chip * 2 + c
    a = xx + c * (yy - xx)
    b = yy + c * (xx - yy)
    half_x = lax.rem(xx, 2)
    half, ctx_dev = cache.shape[1], cache.shape[3]
    seqs = 2 * half
    width = w.shape[2]
    tiles = width // 128
    cols = SIDE * width

    def first(p):
        return (g, yy + c * (p - yy), xx + (1 - c) * (p - xx), c)

    def second(p):
        return (g, yy + (1 - c) * (p - yy), xx + c * (p - xx), c)

    def across(p):
        return (g, yy + (1 - c) * (p - yy), xx + c * (p - xx), 1 - c)

    partner = (g, yy, xx, 1 - c)
    neighbour = (g, yy, xx + 1 - 2 * half_x, c)

    def rcopy(src, dst, phase, to, frm, device, recv_phase=None, recv_from=None):
        recv = (phase, frm) if recv_phase is None else (recv_phase, recv_from)
        return pltpu.make_async_remote_copy(
            src_ref=src, dst_ref=dst, send_sem=ssem.at[phase, to], recv_sem=rsem.at[recv],
            device_id=device, device_id_type=MESH,
        )

    def dcopy(src, dst, which, device):
        return pltpu.make_async_remote_copy(
            src_ref=src, dst_ref=dst, send_sem=dsend.at[which], recv_sem=drecv.at[which],
            device_id=device, device_id_type=MESH,
        )

    def peers(me, body):
        def one(i):
            body(lax.rem(me + far_first(i), SIDE))

        loop(SIDE - 1, one)

    def local(src, dst, k):
        return pltpu.make_async_copy(src, dst, loc.at[k])

    w_row = pl.multiple_of(half_x * 64 + c * 32, 32)
    q_load = local(q_in, qraw, 0)
    q_load.start()
    small = [
        local(vu_in, vu.at[c], 1),
        local(res_in, res.at[c], 2),
        local(gain_in, gain.at[c], 23),
        local(ids_in, ids, 3),
        local(gate_in, gate, 4),
    ]
    for copy in small:
        copy.start()
    w_loads = [
        local(op_in.at[:, pl.ds(p * width, width)], w.at[p, pl.ds(w_row, 32), :], 5 + p)
        for p in range(SIDE)
    ]
    for copy in w_loads:
        copy.start()
    parts = ksend.shape[0]
    each = half // parts
    k_loads = [
        local(
            cache_in.at[pl.ds(c * half + each * p, each)], cache.at[c, pl.ds(each * p, each)], 13 + p
        )
        for p in range(parts)
    ]

    def k_copy(p):
        return pltpu.make_async_remote_copy(
            src_ref=cache_in.at[pl.ds((1 - c) * half + each * p, each)],
            dst_ref=cache.at[c, pl.ds(each * p, each)],
            send_sem=ksend.at[p], recv_sem=krecv.at[p], device_id=partner, device_id_type=MESH,
        )

    def k_from(p):
        return pltpu.make_async_remote_copy(
            src_ref=cache_in.at[pl.ds(each * p, each)],
            dst_ref=cache.at[1 - c, pl.ds(each * p, each)],
            send_sem=ksend.at[p], recv_sem=krecv.at[p], device_id=partner, device_id_type=MESH,
        )

    for copy in k_loads:
        copy.start()

    barrier = pltpu.get_barrier_semaphore()
    pl.semaphore_signal(barrier, inc=1, device_id=partner, device_id_type=MESH)

    def greet(p):
        pl.semaphore_signal(barrier, inc=1, device_id=first(p), device_id_type=MESH)
        y, x = first(p)[1:3]
        pl.semaphore_signal(barrier, inc=1, device_id=(g, y, x, 1 - c), device_id_type=MESH)

    def greet_second(p):
        pl.semaphore_signal(barrier, inc=1, device_id=second(p), device_id_type=MESH)
        pl.semaphore_signal(barrier, inc=1, device_id=across(p), device_id_type=MESH)

    peers(a, greet)
    peers(b, greet_second)

    ext[...] = jnp.zeros(ext.shape, F32)
    q_load.wait()
    quarter = half_x * 2 + c
    ext[:, 0:16] = qraw[:, 128:144].astype(F32)
    main[...] = pltpu.roll(qraw[:, 0:128].astype(F32), quarter * 16, 1)

    def chunk_of(base):
        extra = jnp.zeros((4, 128), F32)
        for k in range(half // 4):
            row = base + 4 * k
            extra = extra + pltpu.roll(ext[row : row + 4, :], lax.rem(quarter + k, 8) * 16, 1)
        return jnp.concatenate([main[base : base + half, :], extra], axis=0)

    halves = [chunk_of(0), chunk_of(half)]
    qb[b, a, c] = jnp.where(c == 0, halves[0], halves[1]).astype(BF16)
    qs[...] = jnp.where(c == 0, halves[1], halves[0]).astype(BF16)

    pl.semaphore_wait(barrier, 4 * (SIDE - 1) + 1)

    def q1(p):
        return rcopy(qb.at[b, a, c], qb.at[b, a, c], Q1, p, 0, first(p), Q1 + c, a)

    def q1_across(p):
        return rcopy(qs, qb.at[a, b, c], Q1B, p, 0, across(p), Q1 + c, b)

    def q1_from(p, core):
        return rcopy(qs, qb.at[b, p, core], Q1, p, 0, first(p), Q1 + core, p)

    q1_across(b).start()
    peers(a, lambda p: q1(p).start())
    peers(b, lambda p: q1_across(p).start())

    def q2(slot, source, chunk, to):
        block = qb.at[source, chunk]
        return pltpu.make_async_remote_copy(
            src_ref=block, dst_ref=block, send_sem=qsend.at[slot, chunk],
            recv_sem=qrecv.at[source, chunk], device_id=second(to), device_id_type=MESH,
        )

    def at(me, distance):
        return lax.rem(me + distance, SIDE)

    def spread(distances):
        for d in distances:
            chunk = at(a, d)
            if d:
                q1_from(chunk, c).wait_recv()
            q1_from(chunk, 1 - c).wait_recv()
            for e in (2, 6, 1, 7):
                q2(e, b, chunk, at(b, e)).start()

    def relay(distances):
        for d in distances:
            chunk = at(a, d)
            source = at(b, 6)
            q2(1, source, chunk, source).wait_recv()
            q2(3, source, chunk, at(b, 1)).start()
            if d % 2 == 0:
                q2(4, source, chunk, at(b, 2)).start()
            source = at(b, 2)
            q2(1, source, chunk, source).wait_recv()
            q2(5, source, chunk, at(b, 7)).start()
            if d % 2 == 1:
                q2(0, source, chunk, at(b, 6)).start()

    spread((0,))
    k_copy(0).start()
    spread((1, 7))
    k_copy(1).start()
    spread((2, 6))
    k_copy(2).start()
    relay((0,))
    k_copy(3).start()
    spread((3, 5))
    k_copy(4).start()
    spread((4,))
    k_copy(5).start()
    relay((1, 7))
    k_copy(6).start()
    relay((2, 6))
    k_copy(7).start()
    relay((3, 5))
    k_copy(8).start()
    relay((4,))
    k_copy(9).start()

    for copy in small:
        copy.wait()
    for copy in w_loads:
        copy.wait()
    w_rows = w.at[:, pl.ds(w_row, 32), :]
    to_partner = [
        dcopy(vu.at[c], vu.at[c], D_VU, partner),
        dcopy(res.at[c], res.at[c], D_RES, partner),
        dcopy(gain.at[c], gain.at[c], D_GAIN, partner),
        dcopy(w_rows, w_rows, D_W, partner),
    ]
    for copy in to_partner[:3]:
        copy.start()

    for ref in (ml1, ab, ta, tb, pt):
        ref[...] = jnp.zeros(ref.shape, F32)
    for e in (1, 7, 3, 5, 4):
        source = at(b, e)
        loop(SIDE, lambda k: q2(1, source, k, source).wait_recv())
    to_partner[3].start()

    lane = lanes((ROWS, 128))
    lane8 = lanes((8, 128))
    low = sublanes((8, 128)) < 4

    def assemble(hy):
        for hg in range(QUARTERS):
            m = []
            for e in range(2):
                x = 2 * hg + e
                for q in range(2):
                    m.append(qb[hy + c * (x - hy), x + c * (hy - x), q].astype(F32))
            turned = []
            for k in range(half // 4):
                picked = m[0][16:ROWS]
                for i in range(1, QUARTERS):
                    picked = jnp.where(lax.div(lane8, 16) == (k + i) % 8, m[i][16:ROWS], picked)
                picked = pltpu.roll(picked, (128 - 16 * k) % 128, 1)
                turned.append(picked if k % 2 else pltpu.roll(picked, 4, 0))
            e = jnp.concatenate(
                [
                    jnp.where(low, turned[0], turned[1]),
                    jnp.where(low, turned[2], turned[3]),
                    turned[4],
                ],
                axis=0,
            )
            whole = [
                m[0],
                jnp.where(lane < 16, e, m[1]),
                jnp.where(lane < 16, m[1], jnp.where(lane < 32, e, m[2])),
                jnp.where(lane < 32, m[2], jnp.where(lane < 48, e, m[3])),
                jnp.where(lane < 48, m[3], e),
            ]
            base = hy * (A_GROUP - 8 * c) + hg * PITCH
            for t in range(5):
                qa[pl.ds(pl.multiple_of(base + t * ROWS, 8), ROWS), :] = whole[t]

    loop(SIDE, assemble)

    for copy in k_loads:
        copy.wait()
    for p in range(parts):
        k_from(p).wait_recv()
    position = chip * 2 * ctx_dev + lanes((1, 2 * ctx_dev))
    part_k = half // 2

    def weigh(s, by_column):
        pieces = []
        for t in range(5):
            groups = []
            for k in range(4):
                if by_column:
                    rows = pl.ds(k * PITCH + t * ROWS + s, 8, stride=A_GROUP)
                else:
                    rows = pl.ds(8 * k * PITCH + t * ROWS + s, 8, stride=PITCH)
                groups.append(qa[rows, :])
            pieces.append(jnp.concatenate(groups, axis=0).astype(BF16))
        q = jnp.concatenate(pieces, axis=1)[:, : LAT + ROPE]
        keys = jnp.concatenate([cache[0, s], cache[1, s]], axis=1)
        scores = jnp.dot(q, keys, preferred_element_type=F32)
        valid = position < ctx[c * half + s]
        scores = jnp.where(valid, scores * score_scale, masked_score)
        top = jnp.max(scores, axis=1, keepdims=True)
        weights = jnp.where(valid, jnp.exp(scores - top), 0.0)
        total = jnp.sum(weights, axis=1, keepdims=True)
        wb[s] = weights.astype(BF16)
        return top, total

    def merge(u, v, first_rows):
        if first_rows:
            return jnp.where(low, u, pltpu.roll(v, 4, 0))
        return jnp.where(low, pltpu.roll(u, 4, 0), v)

    def put(tile, k, top, total):
        return jnp.where(lane8 == k, top, jnp.where(lane8 == 64 + k, total, tile))

    def weigh_columns(i):
        tiles_m = [jnp.zeros((8, 128), F32) for _ in range(4)]
        for u in range(part_k):
            s = i * part_k + u
            top, total = weigh(s, True)
            for k in range(4):
                rows = slice(8 * k, 8 * k + 8)
                tiles_m[k] = put(tiles_m[k], s, top[rows], total[rows])
        for k in range(4):
            for d in range(2):
                ml1[2 * k + d] += tiles_m[k]

    def weigh_rows(i):
        tiles_m = [jnp.zeros((8, 128), F32) for _ in range(SIDE)]
        for u in range(part_k // 2):
            pair = i * (part_k // 2) + u
            t0, l0 = weigh(2 * pair, False)
            t1, l1 = weigh(2 * pair + 1, False)
            for k in range(4):
                rows = slice(8 * k, 8 * k + 8)
                wide = [jnp.broadcast_to(v[rows], (8, 128)) for v in (t0, t1, l0, l1)]
                for d in range(2):
                    top = merge(wide[0], wide[1], d == 0)
                    total = merge(wide[2], wide[3], d == 0)
                    for e in range(2):
                        tile = tiles_m[2 * k + d]
                        tiles_m[2 * k + d] = put(tile, 2 * pair + e, top, total)
        for p in range(SIDE):
            ml1[p] += tiles_m[p]

    @pl.when(c == 0)
    def _():
        loop(2, weigh_columns)

    @pl.when(c == 1)
    def _():
        loop(2, weigh_rows)

    def mlsend(p):
        return rcopy(ml1.at[p], rml1.at[a], ML1, p, a, first(p))

    def ml_from(p):
        return rcopy(ml1.at[p], rml1.at[p], ML1, p, p, first(p))

    peers(a, lambda p: mlsend(p).start())

    def attend(s):
        values = jnp.concatenate([cache[0, s, 0:LAT, :], cache[1, s, 0:LAT, :]], axis=1)
        return lax.dot_general(
            wb[s], values, (((1,), (1,)), ((), ())), preferred_element_type=F32
        )

    def by_column(dst, i):
        for u in range(part_k):
            out = attend(i * part_k + u)
            for k in range(4):
                rows = slice(8 * k, 8 * k + 8)
                for d in range(2):
                    lo = out[rows, 256 * d : 256 * d + 128]
                    hi = out[rows, 256 * d + 128 : 256 * d + 256]
                    dst[i, 2 * k + d, u] = jnp.concatenate([lo, hi], axis=0).astype(dst.dtype)

    def by_row(dst, i):
        for u in range(part_k // 2):
            s = i * part_k + 2 * u
            o0 = attend(s)
            o1 = attend(s + 1)
            for k in range(4):
                rows = slice(8 * k, 8 * k + 8)
                for d in range(2):
                    for e in range(2):
                        blocks = [
                            merge(
                                o0[rows, 128 * t : 128 * t + 128],
                                o1[rows, 128 * t : 128 * t + 128],
                                d == 0,
                            )
                            for t in (2 * e, 2 * e + 1)
                        ]
                        dst[i, 2 * k + d, 2 * u + e] = jnp.concatenate(blocks, axis=0).astype(
                            dst.dtype
                        )

    def osend(i, p):
        return rcopy(s1.at[i, p], r1.at[i, a], O1 + i, p, a, first(p))

    def o_from(i, p):
        return rcopy(s1.at[i, p], r1.at[i, p], O1 + i, p, p, first(p))

    def widen(wide, p, f):
        for k in range(half):
            wide[p, k] = jnp.broadcast_to(f[:, k : k + 1], (8, 128))

    def twice(f):
        return jnp.concatenate([f, f], axis=0)

    def for_self(i):
        @pl.when(c == 0)
        def _():
            by_column(s1, i)

        @pl.when(c == 1)
        def _():
            by_row(s1, i)

        peers(a, lambda p: osend(i, p).start())

    loop(2, for_self)

    peers(a, lambda p: ml_from(p).wait_recv())
    rml1[a] = ml1[a]
    row_top = rml1[0]
    for p in range(1, SIDE):
        row_top = jnp.maximum(row_top, rml1[p])
    total = jnp.zeros((8, 128), F32)
    for p in range(SIDE):
        factor = jnp.exp(rml1[p] - row_top)
        total = total + factor * pltpu.roll(rml1[p], 64, 1)
        fown[p] = factor
    packed = jnp.where(lane8 < 64, row_top, pltpu.roll(total, 64, 1))
    ml2[...] = packed

    def ml2_send(p):
        return rcopy(ml2, rml2.at[b], ML2, p, b, second(p))

    def ml2_from(p):
        return rcopy(ml2, rml2.at[p], ML2, p, p, second(p))

    peers(b, lambda p: ml2_send(p).start())

    def widen_row(i):
        for d in range(2):
            widen(wown, 2 * i + d, fown[2 * i + d])

    loop(SIDE // 2, widen_row)

    idle_row = pl.multiple_of((1 - half_x) * 64, 64)

    def fill(p):
        w[p, pl.ds(idle_row, 64), :] = jnp.zeros((64, width), BF16)

        def block(k):
            start = pl.multiple_of(k * 16, 16)
            row = start + sublanes((16, width))
            column = p * width + lanes((16, width))
            target = chip * 112 + lax.rem(row, 64) + 56 * lax.div(row, 64)
            hit = jnp.where((column == target) & (lax.rem(row, 64) < 56), 1.0, 0.0)
            w[p, pl.ds(pl.multiple_of(128 + start, 16), 16), :] = hit.astype(BF16)

        loop(8, block)

    loop(SIDE, fill)

    idv = ids[...]
    gatev = gate[...]
    hits = jnp.zeros((8, seqs), F32)
    hit_rows = []
    gates = []
    for j in range(4):
        expert = (dev if j < 2 else chip * 2 + 1 - c) * 2 + j % 2
        same = idv == expert
        hit = jnp.sum(jnp.where(same, 1.0, 0.0), axis=0, keepdims=True)
        hit_rows.append(hit)
        gates.append(jnp.sum(jnp.where(same, gatev, 0.0), axis=0, keepdims=True))
        hits = jnp.where(sublanes((8, seqs)) == j, hit, hits)
    earlier = jnp.where(sublanes((seqs, seqs)) < lanes((seqs, seqs)), 1.0, 0.0)
    rank = jnp.dot(hits.astype(BF16), earlier.astype(BF16), preferred_element_type=F32)
    table = jnp.zeros((16, seqs), F32)
    gate_slots = jnp.zeros((2, CAP), F32)
    for j in range(4):
        for k in range(CAP):
            chosen = jnp.where(rank[j : j + 1] == float(k), hit_rows[j], 0.0)
            r = (j // 2) * 8 + (j % 2) * CAP + k
            table = jnp.where(sublanes((16, seqs)) == r, chosen, table)
            if j < 2:
                total = jnp.sum(chosen * gates[j], axis=1, keepdims=True)
                here = (sublanes((2, CAP)) == j) & (lanes((2, CAP)) == k)
                gate_slots = jnp.where(here, total, gate_slots)
    gate_out[...] = gate_slots
    pt[:, 0:seqs] = table
    own = jnp.where(c == 0, pt[...], pltpu.roll(pt[...], 128 - half, 1))
    pick[...] = jnp.where(lanes((16, 128)) < half, own, 0.0)

    for copy in to_partner[:3]:
        copy.wait_recv()
    ta[0:seqs, 0:56] = res[0].astype(F32)
    tb[0:seqs, 0:56] = res[1].astype(F32)
    ta[seqs : seqs + 1, 0:56] = gain[0].astype(F32)
    tb[seqs : seqs + 1, 0:56] = gain[1].astype(F32)
    both = ta[...] + pltpu.roll(tb[...], 64, 1)
    ta[...] = both
    row = sublanes((ROWS, 128))
    mine = jnp.where(c == 0, ta[0:ROWS, :], ta[half : half + ROWS, :])
    gain_row = jnp.broadcast_to(ta[seqs : seqs + 1, :], (ROWS, 128))
    lhs[...] = jnp.where(row < half, mine, jnp.where(row == half, gain_row, 0.0))

    def add(block, i, p, fresh):
        for k in range(part_k):
            index = i * part_k + k
            term = twice(wown[p, index]) * block[k].astype(F32)
            acc[index] = term if fresh else acc[index] + term

    def gather(i):
        add(s1.at[i, a], i, a, True)

        def take(p):
            o_from(i, p).wait_recv()
            add(r1.at[i, p], i, p, False)

        peers(a, take)

    loop(2, gather)
    peers(b, lambda p: ml2_from(p).wait_recv())
    rml2[b] = packed
    top = rml2[0]
    for p in range(1, SIDE):
        top = jnp.maximum(top, rml2[p])
    total = jnp.zeros((8, 128), F32)
    for p in range(SIDE):
        total = total + jnp.exp(rml2[p] - top) * pltpu.roll(rml2[p], 64, 1)
    final = jnp.exp(row_top - top) / total
    for k in range(half):
        acc[k] = acc[k] * twice(jnp.broadcast_to(final[:, k : k + 1], (8, 128)))

    @pl.when(c == 0)
    def _():
        for k in range(half):
            for d in range(2):
                ab[d * 192 + k * 8 : d * 192 + k * 8 + 8, :] = acc[k, 8 * d : 8 * d + 8, :]
        for j in range(SIDE):
            s2[j] = jnp.concatenate(
                [ab[pl.ds(d * 192 + j, ROWS, stride=8), :] for d in range(2)], axis=0
            ).astype(BF16)

    @pl.when(c == 1)
    def _():
        for k in range(half):
            for d in range(2):
                base = ((k % 2) * 2 + d) * 96 + (k // 2) * 8
                ab[base : base + 8, :] = acc[k, 8 * d : 8 * d + 8, :]
        for j in range(SIDE):
            s2[j] = jnp.concatenate(
                [ab[pl.ds(((j % 2) * 2 + d) * 96 + j // 2, ROWS, stride=4), :] for d in range(2)],
                axis=0,
            ).astype(BF16)

    def o2_send(p):
        return rcopy(s2.at[p], r2.at[b], O2, p, b, second(p))

    def o2_from(p):
        return rcopy(s2.at[p], r2.at[p], O2, p, p, second(p))

    peers(b, lambda p: o2_send(p).start())
    peers(b, lambda p: o2_from(p).wait_recv())
    r2[b] = s2[b]
    merged = r2[0].astype(F32)
    for p in range(1, SIDE):
        merged = merged + r2[p].astype(F32)

    part = jnp.zeros((ROWS, VD), F32)
    for k in range(2):
        block = merged[ROWS * k : ROWS * (k + 1)]
        high = block.astype(BF16)
        low = (block - high.astype(F32)).astype(BF16)
        part = part + jnp.dot(high, vu[k], preferred_element_type=F32)
        part = part + jnp.dot(low, vu[k], preferred_element_type=F32)
    vs[...] = part
    swap = dcopy(vs, vr, D_V, neighbour)
    swap.start()
    to_partner[3].wait_recv()
    swap.wait_recv()
    left = jnp.concatenate([(part + vr[...]).astype(BF16), lhs[...].astype(BF16)], axis=1)

    def a1_send(p):
        return rcopy(s3.at[p], r3.at[a], A1, p, a, first(p))

    def a1_from(p):
        return rcopy(s3.at[p], r3.at[p], A1, p, p, first(p))

    def a2_send(p):
        return rcopy(s4, r4.at[b], A2, p, b, second(p))

    def a2_from(p):
        return rcopy(s4, r4.at[p], A2, p, p, second(p))

    def a3_send(p):
        return rcopy(rf.at[a], rf.at[a], A3, p, a, first(p))

    def a3_from(p):
        return rcopy(rf.at[p], rf.at[p], A3, p, p, first(p))

    def in_step(k):
        pl.semaphore_signal(steps.at[k], inc=1, device_id=partner, device_id_type=MESH)
        pl.semaphore_wait(steps.at[k], 1)

    def project(p):
        out = jnp.dot(left, w[p], preferred_element_type=F32)
        blocks = [out[:half, 128 * t : 128 * t + 128] for t in range(tiles)]
        blocks += [out[half : half + 1, 128 * t : 128 * t + 128] for t in range(tiles)]
        blocks.append(jnp.zeros((rf.shape[1] - tiles * (half + 1), 128), F32))
        s3[p] = jnp.concatenate(blocks, axis=0).astype(BF16)

    def project_send(p):
        project(p)
        a1_send(p).start()

    in_step(0)
    peers(a, project_send)
    project(a)
    peers(a, lambda p: a1_from(p).wait_recv())
    r3[a] = s3[a]
    total = r3[0].astype(F32)
    for p in range(1, SIDE):
        total = total + r3[p].astype(F32)
    s4[...] = total.astype(BF16)
    in_step(1)
    peers(b, lambda p: a2_send(p).start())
    peers(a, lambda p: q1(p).wait_send())
    loop(SIDE, lambda p: q1_across(p).wait_send())
    for p in range(parts):
        k_copy(p).wait_send()
    for d in range(SIDE):
        chunk = at(a, d)
        for slot in (1, 2, 3, 5, 6, 7, 4 if d % 2 == 0 else 0):
            q2(slot, b, chunk, at(b, 1)).wait_send()
    peers(a, lambda p: mlsend(p).wait_send())
    for i in range(2):
        peers(a, lambda p: osend(i, p).wait_send())
    peers(b, lambda p: ml2_send(p).wait_send())
    peers(b, lambda p: o2_send(p).wait_send())
    for copy in to_partner + [swap]:
        copy.wait_send()
    peers(b, lambda p: a2_from(p).wait_recv())
    r4[b] = s4[...]
    total = r4[0].astype(F32)
    for p in range(1, SIDE):
        total = total + r4[p].astype(F32)
    rf[a] = total.astype(BF16)
    in_step(2)
    peers(a, lambda p: a3_send(p).start())
    peers(a, lambda p: a1_send(p).wait_send())
    peers(b, lambda p: a2_send(p).wait_send())
    peers(a, lambda p: a3_from(p).wait_recv())

    choose = pick[...][:, 0:half]
    choose_b = choose.astype(BF16)
    squares = jnp.zeros((half, 128), F32)
    largest = jnp.zeros((half, 128), F32)
    for p in range(SIDE):
        block = rf[p].astype(F32)
        parts_r = [block[half * t : half * (t + 1)] for t in range(tiles)]
        gains = [block[half * tiles + t : half * tiles + t + 1] for t in range(tiles)]
        for v, gv in zip(parts_r, gains):
            squares = squares + v * v
            largest = jnp.maximum(largest, jnp.abs(v * gv))
        rows = jnp.concatenate(parts_r, axis=1).astype(BF16)
        chosen = jnp.dot(choose_b, rows, preferred_element_type=F32)
        y[p] = chosen * jnp.concatenate(gains, axis=1)
    inverse = lax.rsqrt(jnp.sum(squares, axis=1, keepdims=True) / cols + small_eps)
    peak = inverse * jnp.max(largest, axis=1, keepdims=True) + small_eps
    spread = jnp.concatenate(
        [jnp.broadcast_to(inverse / peak, (half, 128)), jnp.broadcast_to(peak, (half, 128))], axis=1
    )
    slots = jnp.dot(choose, spread, preferred_element_type=F32, precision=lax.Precision.HIGHEST)
    code = jnp.concatenate([slots[:, 0:128]] * tiles, axis=1)
    peaks = slots[:, 128:256]
    xs[...] = peaks[8:16]
    for k in range(SIDE // 2):
        fs[k] = jnp.concatenate(
            [y[2 * k + d, 8:16, :] * code[8:16] for d in range(2)], axis=0
        ).astype(BF16)
    x_partner = dcopy(xs, xr, D_X, partner)
    f_partner = dcopy(fs, fr, D_F, partner)
    x_partner.start()
    f_partner.start()
    x_partner.wait_recv()
    peaks = peaks[0:8] + xr[...]
    scale_slots = jnp.zeros((2, CAP), F32)
    for j in range(2):
        for k in range(CAP):
            here = (sublanes((2, CAP)) == j) & (lanes((2, CAP)) == k)
            r = CAP * j + k
            scale_slots = jnp.where(here, peaks[r : r + 1, 0:1], scale_slots)
    scale_out[...] = scale_slots
    f_partner.wait_recv()
    for k in range(SIDE // 2):
        there = fr[k].astype(F32)
        for d in range(2):
            p = 2 * k + d
            rows = (y[p, 0:8, :] * code[0:8] + there[8 * d : 8 * d + 8]).astype(BF16)
            for e in range(2):
                disp_out[e, :, pl.ds(p * width, width)] = rows[CAP * e : CAP * e + CAP]

    peers(a, lambda p: a3_send(p).wait_send())
    x_partner.wait_send()
    f_partner.wait_send()


def per_device(
    queries, latent_cache, context_lengths, value_up, out_proj, residual, norm_gain, expert_ids,
    gate_weights,
):
    seqs, ctx_dev, entry = latent_cache.shape
    half = seqs // 2
    columns = out_proj.shape[1]
    width = columns // SIDE
    piece = residual.shape[1]
    experts = 2
    rows = -(-(width // 128) * (half + 1) // 8) * 8
    any_space = pl.BlockSpec(memory_space=pl.ANY)
    vmem = pl.BlockSpec(memory_space=pltpu.VMEM)
    smem = pl.BlockSpec(memory_space=pltpu.SMEM)
    V = pltpu.VMEM
    chunk = (2, SIDE, half // 2, 16, 128)
    eights = (SIDE, 8, 128)
    scratch = [
        V(queries.shape, BF16),
        V((seqs, 128), F32),
        V((seqs, 128), F32),
        V((ROWS, 128), BF16),
        V((SIDE, SIDE, 2, ROWS, 128), BF16),
        V((SIDE * A_GROUP, 128), F32),
        V((2, half, entry, ctx_dev), BF16),
        V((half, H, 2 * ctx_dev), BF16),
        V(chunk, BF16),
        V(chunk, BF16),
        V(eights, F32),
        V(eights, F32),
        V((8, 128), F32),
        V(eights, F32),
        V(eights, F32),
        V((SIDE, half, 8, 128), F32),
        V((half, 16, 128), F32),
        V((384, 128), F32),
        V((SIDE, 2 * ROWS, 128), BF16),
        V((SIDE, 2 * ROWS, 128), BF16),
        V((2, 128, VD), BF16),
        V((ROWS, VD), F32),
        V((ROWS, VD), F32),
        V((2, seqs, piece), BF16),
        V((2, 1, piece), BF16),
        V((seqs + 8, 128), F32),
        V((seqs + 8, 128), F32),
        V((ROWS, 128), F32),
        V((SIDE, 256, width), BF16),
        V((SIDE, rows, 128), BF16),
        V((SIDE, rows, 128), BF16),
        V((rows, 128), BF16),
        V((SIDE, rows, 128), BF16),
        V((SIDE, rows, 128), BF16),
        V(expert_ids.shape[::-1], jnp.int32),
        V(gate_weights.shape[::-1], F32),
        V((16, 128), F32),
        V((16, 128), F32),
        V((SIDE, 16, width), F32),
        V((SIDE // 2, 16, width), BF16),
        V((SIDE // 2, 16, width), BF16),
        V((8, 128), F32),
        V((8, 128), F32),
        pltpu.SemaphoreType.DMA((24,)),
        pltpu.SemaphoreType.DMA((10, SIDE)),
        pltpu.SemaphoreType.DMA((10, SIDE)),
        pltpu.SemaphoreType.DMA((SIDE, SIDE)),
        pltpu.SemaphoreType.DMA((SIDE, SIDE)),
        pltpu.SemaphoreType.DMA((half // 2,)),
        pltpu.SemaphoreType.DMA((half // 2,)),
        pltpu.SemaphoreType.DMA((7,)),
        pltpu.SemaphoreType.DMA((7,)),
        pltpu.SemaphoreType.REGULAR((3,)),
    ]
    dispatched, slot_scale, slot_gate = pl.pallas_call(
        kernel,
        out_shape=(
            jax.ShapeDtypeStruct((experts, CAP, columns), BF16),
            jax.ShapeDtypeStruct((experts, CAP), F32),
            jax.ShapeDtypeStruct((experts, CAP), F32),
        ),
        in_specs=[any_space, any_space, smem] + [any_space] * 6,
        out_specs=(vmem, vmem, vmem),
        scratch_shapes=scratch,
        compiler_params=pltpu.CompilerParams(collective_id=0, has_side_effects=True),
    )(
        queries, latent_cache.transpose(0, 2, 1), context_lengths, value_up, out_proj, residual,
        norm_gain[None, :], expert_ids.T, gate_weights.T,
    )
    return dispatched, slot_scale, slot_gate


def solution(mesh):
    split = Mesh(
        mesh.devices.reshape(mesh.shape["groups"], SIDE, SIDE, 2),
        ("groups", "kv_0", "kv_1", "kv_2"),
    )
    in_specs = (
        P("groups", KV),
        P("groups", KV, None),
        P("groups"),
        P(KV, None),
        P(KV, None),
        P("groups", KV),
        P(KV),
        P("groups", None),
        P("groups", None),
    )
    out_specs = (P(GROUPS_KV, None, None), P(GROUPS_KV, None), P(GROUPS_KV, None))
    return jax.shard_map(
        per_device, mesh=split, in_specs=in_specs, out_specs=out_specs, check_vma=False
    )
```

```python
import functools

import jax
import jax.numpy as jnp
from jax import lax
from jax.experimental import pallas as pl
from jax.experimental.pallas import tpu as pltpu
from jax.sharding import Mesh
from jax.sharding import PartitionSpec as P

H = 32
LAT = 512
ROPE = 64
VD = 128
TOPK = 8
CAP = 2
SIDE = 8
QUARTERS = 4
ROWS = 24
PITCH = 5 * ROWS
A_GROUP = QUARTERS * PITCH + 8
KV = ("kv_0", "kv_1", "kv_2")
GROUPS_KV = ("groups", "kv_0", "kv_1", "kv_2")
FAR_FIRST = (4, 3, 5, 2, 6, 1, 7)
DIRECT = (3, 4, 5)
PARTS = 2
CUTS = (0, 4, 7)
MESH = pl.DeviceIdType.MESH
F32 = jnp.float32
BF16 = jnp.bfloat16

score_scale = 192.0 ** (-0.5)
masked_score = -1e30
small_eps = 1e-06

Q1, Q1B, ML1, ML2, O2, A1, A2, A3, O1 = 0, 1, 2, 3, 4, 5, 7, 9, 11
PHASES = O1 + PARTS
D_VU, D_RES, D_GAIN, D_W, D_F, D_X, D_N, D_NW = range(8)


def lanes(shape):
    return lax.broadcasted_iota(jnp.int32, shape, len(shape) - 1)


def sublanes(shape):
    return lax.broadcasted_iota(jnp.int32, shape, len(shape) - 2)


def loop(count, body):
    def step(i, carry):
        body(i)
        return carry

    lax.fori_loop(0, count, step, 0)


def padded(tiles, half):
    return -(-tiles * (half + 1) // 8) * 8


def far_first(i):
    return SIDE // 2 + (1 - 2 * lax.rem(i, 2)) * lax.div(i + 1, 2)


def kernel(
    q_in, cache_in, ctx_in, vu_in, op_in, res_in, gain_in, ids_in, gate_in,
    disp_out, scale_out, gate_out,
    qraw, ext, main, qs, qb, qa, cache, wb, s1, r1, ml1, rml1,
    ml2, rml2, fown, wown, acc, ab, s2, r2, vu, res, gain, ta, tb, lhs, w,
    s3, r3, s4, r4, rf, ids, gate, pt, pick, y, fs, fr, xs, xr,
    ctx, loc, ssem, rsem, qsend, qrecv, ksend, krecv, dsend, drecv, steps,
):
    g = lax.axis_index("groups")
    yy = lax.axis_index("kv_0")
    xx = lax.axis_index("kv_1")
    c = lax.axis_index("kv_2")
    chip = yy * SIDE + xx
    dev = chip * 2 + c
    a = xx + c * (yy - xx)
    b = yy + c * (xx - yy)
    half_x = lax.rem(xx, 2)
    half, ctx_dev = cache.shape[1], cache.shape[3]
    seqs = 2 * half
    width = w.shape[2]
    tiles = width // 128
    cols = SIDE * width

    def first(p):
        return (g, yy + c * (p - yy), xx + (1 - c) * (p - xx), c)

    def second(p):
        return (g, yy + (1 - c) * (p - yy), xx + c * (p - xx), c)

    def across(p):
        return (g, yy + (1 - c) * (p - yy), xx + c * (p - xx), 1 - c)

    partner = (g, yy, xx, 1 - c)
    neighbour = (g, yy, xx + 1 - 2 * half_x, c)

    def rcopy(src, dst, phase, to, frm, device, recv_phase=None, recv_from=None):
        recv = (phase, frm) if recv_phase is None else (recv_phase, recv_from)
        return pltpu.make_async_remote_copy(
            src_ref=src, dst_ref=dst, send_sem=ssem.at[phase, to], recv_sem=rsem.at[recv],
            device_id=device, device_id_type=MESH,
        )

    def dcopy(src, dst, which, device):
        return pltpu.make_async_remote_copy(
            src_ref=src, dst_ref=dst, send_sem=dsend.at[which], recv_sem=drecv.at[which],
            device_id=device, device_id_type=MESH,
        )

    def peers(me, body):
        for d in FAR_FIRST:
            body(lax.rem(me + d, SIDE))

    def peers_loop(me, body):
        def one(i):
            body(lax.rem(me + far_first(i), SIDE))

        loop(SIDE - 1, one)

    def local(src, dst, k):
        return pltpu.make_async_copy(src, dst, loc.at[k])

    w_row = pl.multiple_of(half_x * 64 + c * 32, 32)
    q_load = local(q_in, qraw, 0)
    q_load.start()
    small = [
        local(vu_in, vu.at[c], 1),
        local(res_in, res.at[c], 2),
        local(gain_in, gain.at[c], 23),
        local(ids_in, ids, 3),
        local(ctx_in, ctx, 24),
        local(gate_in, gate, 4),
    ]
    for copy in small:
        copy.start()
    w_loads = [
        local(op_in.at[:, pl.ds(p * width, width)], w.at[p, pl.ds(w_row, 32), :], 5 + p)
        for p in range(SIDE)
    ]
    for copy in w_loads:
        copy.start()
    parts = ksend.shape[0]
    each = half // parts
    k_loads = [
        local(
            cache_in.at[pl.ds(c * half + each * p, each)], cache.at[c, pl.ds(each * p, each)], 13 + p
        )
        for p in range(parts)
    ]

    def k_copy(p):
        return pltpu.make_async_remote_copy(
            src_ref=cache_in.at[pl.ds((1 - c) * half + each * p, each)],
            dst_ref=cache.at[c, pl.ds(each * p, each)],
            send_sem=ksend.at[p], recv_sem=krecv.at[p], device_id=partner, device_id_type=MESH,
        )

    def k_from(p):
        return pltpu.make_async_remote_copy(
            src_ref=cache_in.at[pl.ds(each * p, each)],
            dst_ref=cache.at[1 - c, pl.ds(each * p, each)],
            send_sem=ksend.at[p], recv_sem=krecv.at[p], device_id=partner, device_id_type=MESH,
        )

    for copy in k_loads:
        copy.start()

    barrier = pltpu.get_barrier_semaphore()
    pl.semaphore_signal(barrier, inc=1, device_id=partner, device_id_type=MESH)

    def greet(p):
        pl.semaphore_signal(barrier, inc=1, device_id=first(p), device_id_type=MESH)
        y, x = first(p)[1:3]
        pl.semaphore_signal(barrier, inc=1, device_id=(g, y, x, 1 - c), device_id_type=MESH)

    def greet_second(p):
        pl.semaphore_signal(barrier, inc=1, device_id=second(p), device_id_type=MESH)
        pl.semaphore_signal(barrier, inc=1, device_id=across(p), device_id_type=MESH)

    peers(a, greet)
    peers(b, greet_second)

    ext[...] = jnp.zeros(ext.shape, F32)
    q_load.wait()
    quarter = half_x * 2 + c
    ext[:, 0:16] = qraw[:, 128:144].astype(F32)
    main[...] = pltpu.roll(qraw[:, 0:128].astype(F32), quarter * 16, 1)

    def chunk_of(base):
        extra = jnp.zeros((4, 128), F32)
        for k in range(half // 4):
            row = base + 4 * k
            extra = extra + pltpu.roll(ext[row : row + 4, :], lax.rem(quarter + k, 8) * 16, 1)
        return jnp.concatenate([main[base : base + half, :], extra], axis=0)

    halves = [chunk_of(0), chunk_of(half)]
    qb[b, a, c] = jnp.where(c == 0, halves[0], halves[1]).astype(BF16)
    qs[...] = jnp.where(c == 0, halves[1], halves[0]).astype(BF16)

    pl.semaphore_wait(barrier, 4 * (SIDE - 1) + 1)

    def q1(p):
        return rcopy(qb.at[b, a, c], qb.at[b, a, c], Q1, p, 0, first(p), Q1 + c, a)

    def q1_across(p):
        return rcopy(qs, qb.at[a, b, c], Q1B, p, 0, across(p), Q1 + c, b)

    def q1_from(p, core):
        return rcopy(qs, qb.at[b, p, core], Q1, p, 0, first(p), Q1 + core, p)

    q1_across(b).start()
    peers(a, lambda p: q1(p).start())
    peers(b, lambda p: q1_across(p).start())

    def q2(slot, source, chunk, to):
        block = qb.at[source, chunk]
        return pltpu.make_async_remote_copy(
            src_ref=block, dst_ref=block, send_sem=qsend.at[slot, chunk],
            recv_sem=qrecv.at[source, chunk], device_id=second(to), device_id_type=MESH,
        )

    def at(me, distance):
        return lax.rem(me + distance, SIDE)

    def spread(distances):
        for d in distances:
            chunk = at(a, d)
            if d:
                q1_from(chunk, c).wait_recv()
            q1_from(chunk, 1 - c).wait_recv()
            for e in FAR_FIRST if d in DIRECT else (2, 6, 1, 7):
                q2(e, b, chunk, at(b, e)).start()

    def relay(distances):
        for d in distances:
            chunk = at(a, d)
            source = at(b, 6)
            q2(1, source, chunk, source).wait_recv()
            q2(3, source, chunk, at(b, 1)).start()
            if d % 2 == 0:
                q2(4, source, chunk, at(b, 2)).start()
            source = at(b, 2)
            q2(1, source, chunk, source).wait_recv()
            q2(5, source, chunk, at(b, 7)).start()
            if d % 2 == 1:
                q2(0, source, chunk, at(b, 6)).start()

    for copy in w_loads:
        copy.wait()
    w_rows = w.at[:, pl.ds(w_row, 32), :]
    beside = pl.multiple_of((1 - half_x) * 64 + c * 32, 32)
    w_beside = w.at[:, pl.ds(beside, 32), :]
    w_out = dcopy(w_rows, w_rows, D_N, neighbour)
    w_in = dcopy(w_beside, w_beside, D_N, neighbour)
    w_across = dcopy(w_beside, w_beside, D_NW, partner)

    @pl.when(c == 0)
    def _():
        w_out.start()

    spread((0,))
    k_copy(0).start()
    spread((1, 7))
    k_copy(1).start()
    spread((2, 6))
    k_copy(2).start()
    relay((0,))
    k_copy(3).start()
    spread((3, 5))
    k_copy(4).start()
    spread((4,))
    k_copy(5).start()
    relay((1, 7))
    k_copy(6).start()
    relay((2, 6))
    k_copy(7).start()
    relay([d for d in (3, 5, 4) if d not in DIRECT])
    k_copy(8).start()
    k_copy(9).start()

    @pl.when(c == 1)
    def _():
        w_out.start()

    for copy in small:
        copy.wait()
    to_partner = [
        dcopy(vu.at[c], vu.at[c], D_VU, partner),
        dcopy(res.at[c], res.at[c], D_RES, partner),
        dcopy(gain.at[c], gain.at[c], D_GAIN, partner),
        dcopy(w_rows, w_rows, D_W, partner),
    ]
    for copy in to_partner[:3]:
        copy.start()

    for ref in (ml1, ab, ta, tb, pt):
        ref[...] = jnp.zeros(ref.shape, F32)
    for d in range(SIDE):
        chunk = at(a, d)
        for e in range(1, SIDE):
            if d in DIRECT or e not in (2, 6):
                source = at(b, e)
                q2(1, source, chunk, source).wait_recv()
    to_partner[3].start()

    lane = lanes((ROWS, 128))
    lane8 = lanes((8, 128))
    low = sublanes((8, 128)) < 4

    def assemble(hy):
        for hg in range(QUARTERS):
            m = []
            for e in range(2):
                x = 2 * hg + e
                for q in range(2):
                    m.append(qb[hy + c * (x - hy), x + c * (hy - x), q].astype(F32))
            turned = []
            for k in range(half // 4):
                picked = m[0][16:ROWS]
                for i in range(1, QUARTERS):
                    picked = jnp.where(lax.div(lane8, 16) == (k + i) % 8, m[i][16:ROWS], picked)
                picked = pltpu.roll(picked, (128 - 16 * k) % 128, 1)
                turned.append(picked if k % 2 else pltpu.roll(picked, 4, 0))
            e = jnp.concatenate(
                [
                    jnp.where(low, turned[0], turned[1]),
                    jnp.where(low, turned[2], turned[3]),
                    turned[4],
                ],
                axis=0,
            )
            whole = [
                m[0],
                jnp.where(lane < 16, e, m[1]),
                jnp.where(lane < 16, m[1], jnp.where(lane < 32, e, m[2])),
                jnp.where(lane < 32, m[2], jnp.where(lane < 48, e, m[3])),
                jnp.where(lane < 48, m[3], e),
            ]
            base = hy * (A_GROUP - 8 * c) + hg * PITCH
            for t in range(5):
                qa[pl.ds(pl.multiple_of(base + t * ROWS, 8), ROWS), :] = whole[t]

    loop(SIDE, assemble)

    for copy in k_loads:
        copy.wait()
    for p in range(parts):
        k_from(p).wait_recv()
    position = chip * 2 * ctx_dev + lanes((1, 2 * ctx_dev))
    part_k = half // PARTS
    many = half // 2

    def weigh(s, by_column):
        pieces = []
        for t in range(5):
            groups = []
            for k in range(4):
                if by_column:
                    rows = pl.ds(k * PITCH + t * ROWS + s, 8, stride=A_GROUP)
                else:
                    rows = pl.ds(8 * k * PITCH + t * ROWS + s, 8, stride=PITCH)
                groups.append(qa[rows, :])
            pieces.append(jnp.concatenate(groups, axis=0).astype(BF16))
        q = jnp.concatenate(pieces, axis=1)[:, : LAT + ROPE]
        keys = jnp.concatenate([cache[0, s], cache[1, s]], axis=1)
        scores = jnp.dot(q, keys, preferred_element_type=F32)
        valid = position < ctx[c * half + s]
        scores = jnp.where(valid, scores * score_scale, masked_score)
        top = jnp.max(scores, axis=1, keepdims=True)
        weights = jnp.where(valid, jnp.exp(scores - top), 0.0)
        total = jnp.sum(weights, axis=1, keepdims=True)
        wb[s] = weights.astype(BF16)
        return top, total

    def merge(u, v, first_rows):
        if first_rows:
            return jnp.where(low, u, pltpu.roll(v, 4, 0))
        return jnp.where(low, pltpu.roll(u, 4, 0), v)

    def put(tile, k, top, total):
        return jnp.where(lane8 == k, top, jnp.where(lane8 == 64 + k, total, tile))

    def weigh_columns(i):
        tiles_m = [jnp.zeros((8, 128), F32) for _ in range(4)]
        for u in range(many):
            s = i * many + u
            top, total = weigh(s, True)
            for k in range(4):
                rows = slice(8 * k, 8 * k + 8)
                tiles_m[k] = put(tiles_m[k], s, top[rows], total[rows])
        for k in range(4):
            for d in range(2):
                ml1[2 * k + d] += tiles_m[k]

    def weigh_rows(i):
        tiles_m = [jnp.zeros((8, 128), F32) for _ in range(SIDE)]
        for u in range(many // 2):
            pair = i * (many // 2) + u
            t0, l0 = weigh(2 * pair, False)
            t1, l1 = weigh(2 * pair + 1, False)
            for k in range(4):
                rows = slice(8 * k, 8 * k + 8)
                wide = [jnp.broadcast_to(v[rows], (8, 128)) for v in (t0, t1, l0, l1)]
                for d in range(2):
                    top = merge(wide[0], wide[1], d == 0)
                    total = merge(wide[2], wide[3], d == 0)
                    for e in range(2):
                        tile = tiles_m[2 * k + d]
                        tiles_m[2 * k + d] = put(tile, 2 * pair + e, top, total)
        for p in range(SIDE):
            ml1[p] += tiles_m[p]

    @pl.when(c == 0)
    def _():
        loop(2, weigh_columns)

    @pl.when(c == 1)
    def _():
        loop(2, weigh_rows)

    def mlsend(p):
        return rcopy(ml1.at[p], rml1.at[a], ML1, p, a, first(p))

    def ml_from(p):
        return rcopy(ml1.at[p], rml1.at[p], ML1, p, p, first(p))

    peers(a, lambda p: mlsend(p).start())

    def attend(s):
        values = jnp.concatenate([cache[0, s, 0:LAT, :], cache[1, s, 0:LAT, :]], axis=1)
        return lax.dot_general(
            wb[s], values, (((1,), (1,)), ((), ())), preferred_element_type=F32
        )

    def by_column(dst, i):
        for u in range(part_k):
            out = attend(i * part_k + u)
            for k in range(4):
                rows = slice(8 * k, 8 * k + 8)
                for d in range(2):
                    lo = out[rows, 256 * d : 256 * d + 128]
                    hi = out[rows, 256 * d + 128 : 256 * d + 256]
                    dst[i, 2 * k + d, u] = jnp.concatenate([lo, hi], axis=0).astype(dst.dtype)

    def by_row(dst, i):
        for u in range(part_k // 2):
            s = i * part_k + 2 * u
            o0 = attend(s)
            o1 = attend(s + 1)
            for k in range(4):
                rows = slice(8 * k, 8 * k + 8)
                for d in range(2):
                    for e in range(2):
                        blocks = [
                            merge(
                                o0[rows, 128 * t : 128 * t + 128],
                                o1[rows, 128 * t : 128 * t + 128],
                                d == 0,
                            )
                            for t in (2 * e, 2 * e + 1)
                        ]
                        dst[i, 2 * k + d, 2 * u + e] = jnp.concatenate(blocks, axis=0).astype(
                            dst.dtype
                        )

    def osend(i, p):
        return rcopy(s1.at[i, p], r1.at[i, a], O1 + i, p, a, first(p))

    def o_from(i, p):
        return rcopy(s1.at[i, p], r1.at[i, p], O1 + i, p, p, first(p))

    def widen(wide, p, f):
        for k in range(half):
            wide[p, k] = jnp.broadcast_to(f[:, k : k + 1], (8, 128))

    def twice(f):
        return jnp.concatenate([f, f], axis=0)

    def for_self(i):
        @pl.when(c == 0)
        def _():
            by_column(s1, i)

        @pl.when(c == 1)
        def _():
            by_row(s1, i)

        peers(a, lambda p: osend(i, p).start())

    loop(PARTS, for_self)

    peers(a, lambda p: ml_from(p).wait_recv())
    rml1[a] = ml1[a]
    row_top = rml1[0]
    for p in range(1, SIDE):
        row_top = jnp.maximum(row_top, rml1[p])
    total = jnp.zeros((8, 128), F32)
    for p in range(SIDE):
        factor = jnp.exp(rml1[p] - row_top)
        total = total + factor * pltpu.roll(rml1[p], 64, 1)
        fown[p] = factor
    packed = jnp.where(lane8 < 64, row_top, pltpu.roll(total, 64, 1))
    ml2[...] = packed

    def ml2_send(p):
        return rcopy(ml2, rml2.at[b], ML2, p, b, second(p))

    def ml2_from(p):
        return rcopy(ml2, rml2.at[p], ML2, p, p, second(p))

    peers(b, lambda p: ml2_send(p).start())

    def widen_row(i):
        for d in range(2):
            widen(wown, 2 * i + d, fown[2 * i + d])

    loop(SIDE // 2, widen_row)


    def fill(p):
        def block(k):
            start = pl.multiple_of(k * 16, 16)
            row = start + sublanes((16, width))
            column = p * width + lanes((16, width))
            target = chip * 112 + lax.rem(row, 64) + 56 * lax.div(row, 64)
            hit = jnp.where((column == target) & (lax.rem(row, 64) < 56), 1.0, 0.0)
            w[p, pl.ds(pl.multiple_of(128 + start, 16), 16), :] = hit.astype(BF16)

        loop(8, block)

    loop(SIDE, fill)

    idv = ids[...]
    gatev = gate[...]
    hits = jnp.zeros((8, seqs), F32)
    hit_rows = []
    gates = []
    for j in range(4):
        expert = (dev if j < 2 else chip * 2 + 1 - c) * 2 + j % 2
        same = idv == expert
        hit = jnp.sum(jnp.where(same, 1.0, 0.0), axis=0, keepdims=True)
        hit_rows.append(hit)
        gates.append(jnp.sum(jnp.where(same, gatev, 0.0), axis=0, keepdims=True))
        hits = jnp.where(sublanes((8, seqs)) == j, hit, hits)
    earlier = jnp.where(sublanes((seqs, seqs)) < lanes((seqs, seqs)), 1.0, 0.0)
    rank = jnp.dot(hits.astype(BF16), earlier.astype(BF16), preferred_element_type=F32)
    table = jnp.zeros((16, seqs), F32)
    gate_slots = jnp.zeros((2, CAP), F32)
    for j in range(4):
        for k in range(CAP):
            chosen = jnp.where(rank[j : j + 1] == float(k), hit_rows[j], 0.0)
            r = (j // 2) * 8 + (j % 2) * CAP + k
            table = jnp.where(sublanes((16, seqs)) == r, chosen, table)
            if j < 2:
                total = jnp.sum(chosen * gates[j], axis=1, keepdims=True)
                here = (sublanes((2, CAP)) == j) & (lanes((2, CAP)) == k)
                gate_slots = jnp.where(here, total, gate_slots)
    gate_out[...] = gate_slots
    pt[:, 0:seqs] = table
    own = jnp.where(c == 0, pt[...], pltpu.roll(pt[...], 128 - half, 1))
    pick[...] = jnp.where(lanes((16, 128)) < half, own, 0.0)

    w_in.wait_recv()
    w_across.start()

    for copy in to_partner[:3]:
        copy.wait_recv()
    ta[0:seqs, 0:56] = res[0].astype(F32)
    tb[0:seqs, 0:56] = res[1].astype(F32)
    ta[seqs : seqs + 1, 0:56] = gain[0].astype(F32)
    tb[seqs : seqs + 1, 0:56] = gain[1].astype(F32)
    both = ta[...] + pltpu.roll(tb[...], 64, 1)
    ta[...] = both
    row = sublanes((ROWS, 128))
    mine = jnp.where(c == 0, ta[0:ROWS, :], ta[half : half + ROWS, :])
    gain_row = jnp.broadcast_to(ta[seqs : seqs + 1, :], (ROWS, 128))
    lhs[...] = jnp.where(row < half, mine, jnp.where(row == half, gain_row, 0.0))

    def add(block, i, p, fresh):
        for k in range(part_k):
            index = i * part_k + k
            term = twice(wown[p, index]) * block[k].astype(F32)
            acc[index] = term if fresh else acc[index] + term

    def gather(i):
        add(s1.at[i, a], i, a, True)

        def take(p):
            o_from(i, p).wait_recv()
            add(r1.at[i, p], i, p, False)

        peers_loop(a, take)

    loop(PARTS, gather)
    peers(b, lambda p: ml2_from(p).wait_recv())
    rml2[b] = packed
    top = rml2[0]
    for p in range(1, SIDE):
        top = jnp.maximum(top, rml2[p])
    total = jnp.zeros((8, 128), F32)
    for p in range(SIDE):
        total = total + jnp.exp(rml2[p] - top) * pltpu.roll(rml2[p], 64, 1)
    final = jnp.exp(row_top - top) / total
    for k in range(half):
        acc[k] = acc[k] * twice(jnp.broadcast_to(final[:, k : k + 1], (8, 128)))

    @pl.when(c == 0)
    def _():
        for k in range(half):
            for d in range(2):
                ab[d * 192 + k * 8 : d * 192 + k * 8 + 8, :] = acc[k, 8 * d : 8 * d + 8, :]
        for j in range(SIDE):
            s2[j] = jnp.concatenate(
                [ab[pl.ds(d * 192 + j, ROWS, stride=8), :] for d in range(2)], axis=0
            ).astype(BF16)

    @pl.when(c == 1)
    def _():
        for k in range(half):
            for d in range(2):
                base = ((k % 2) * 2 + d) * 96 + (k // 2) * 8
                ab[base : base + 8, :] = acc[k, 8 * d : 8 * d + 8, :]
        for j in range(SIDE):
            s2[j] = jnp.concatenate(
                [ab[pl.ds(((j % 2) * 2 + d) * 96 + j // 2, ROWS, stride=4), :] for d in range(2)],
                axis=0,
            ).astype(BF16)

    def o2_send(p):
        return rcopy(s2.at[p], r2.at[b], O2, p, b, second(p))

    def o2_from(p):
        return rcopy(s2.at[p], r2.at[p], O2, p, p, second(p))

    peers(b, lambda p: o2_send(p).start())
    peers(b, lambda p: o2_from(p).wait_recv())
    r2[b] = s2[b]
    merged = r2[0].astype(F32)
    for p in range(1, SIDE):
        merged = merged + r2[p].astype(F32)

    part = jnp.zeros((ROWS, VD), F32)
    for k in range(2):
        block = merged[ROWS * k : ROWS * (k + 1)]
        high = block.astype(BF16)
        low = (block - high.astype(F32)).astype(BF16)
        part = part + jnp.dot(high, vu[k], preferred_element_type=F32)
        part = part + jnp.dot(low, vu[k], preferred_element_type=F32)
    to_partner[3].wait_recv()
    w_across.wait_recv()
    left = jnp.concatenate([part.astype(BF16), lhs[...].astype(BF16)], axis=1)

    def part_rows(j):
        sizes = [padded(CUTS[k + 1] - CUTS[k], half) for k in range(2)]
        return pl.ds(sum(sizes[:j]), sizes[j])

    def a1_send(j, p):
        rows = part_rows(j)
        return rcopy(s3.at[p, rows], r3.at[a, rows], A1 + j, p, a, first(p))

    def a1_from(j, p):
        rows = part_rows(j)
        return rcopy(s3.at[p, rows], r3.at[p, rows], A1 + j, p, p, first(p))

    def a2_send(j, p):
        rows = part_rows(j)
        return rcopy(s4.at[rows], r4.at[b, rows], A2 + j, p, b, second(p))

    def a2_from(j, p):
        rows = part_rows(j)
        return rcopy(s4.at[rows], r4.at[p, rows], A2 + j, p, p, second(p))

    def a3_send(j, p):
        rows = part_rows(j)
        return rcopy(rf.at[a, rows], rf.at[a, rows], A3 + j, p, a, first(p))

    def a3_from(j, p):
        rows = part_rows(j)
        return rcopy(rf.at[p, rows], rf.at[p, rows], A3 + j, p, p, first(p))

    def in_step(k):
        pl.semaphore_signal(steps.at[k], inc=1, device_id=partner, device_id_type=MESH)
        pl.semaphore_wait(steps.at[k], 1)

    def project(j, p):
        out = jnp.dot(left, w[p, :, 128 * CUTS[j] : 128 * CUTS[j + 1]], preferred_element_type=F32)
        count = CUTS[j + 1] - CUTS[j]
        blocks = [out[:half, 128 * t : 128 * t + 128] for t in range(count)]
        blocks += [out[half : half + 1, 128 * t : 128 * t + 128] for t in range(count)]
        blocks.append(jnp.zeros((padded(count, half) - count * (half + 1), 128), F32))
        s3[p, part_rows(j), :] = jnp.concatenate(blocks, axis=0).astype(BF16)

    def total_of(ref, j):
        total = ref[0, part_rows(j), :].astype(F32)
        for p in range(1, SIDE):
            total = total + ref[p, part_rows(j), :].astype(F32)
        return total.astype(BF16)

    in_step(0)
    for j in range(2):

        def project_send(p):
            project(j, p)
            a1_send(j, p).start()

        peers_loop(a, project_send)
        project(j, a)
    for j in range(2):
        peers(a, lambda p: a1_from(j, p).wait_recv())
        r3[a, part_rows(j), :] = s3[a, part_rows(j), :]
        s4[part_rows(j), :] = total_of(r3, j)
        if j == 0:
            in_step(1)
        peers(b, lambda p: a2_send(j, p).start())
    peers(a, lambda p: q1(p).wait_send())
    loop(SIDE, lambda p: q1_across(p).wait_send())
    for p in range(parts):
        k_copy(p).wait_send()
    for d in range(SIDE):
        chunk = at(a, d)
        for slot in range(1, SIDE) if d in DIRECT else (1, 2, 3, 5, 6, 7, 4 if d % 2 == 0 else 0):
            q2(slot, b, chunk, at(b, 1)).wait_send()
    peers(a, lambda p: mlsend(p).wait_send())
    for i in range(PARTS):
        peers(a, lambda p: osend(i, p).wait_send())
    peers(b, lambda p: ml2_send(p).wait_send())
    peers(b, lambda p: o2_send(p).wait_send())
    for copy in to_partner + [w_out, w_across]:
        copy.wait_send()
    for j in range(2):
        peers(b, lambda p: a2_from(j, p).wait_recv())
        r4[b, part_rows(j), :] = s4[part_rows(j), :]
        rf[a, part_rows(j), :] = total_of(r4, j)
        if j == 0:
            in_step(2)
        peers(a, lambda p: a3_send(j, p).start())
    for j in range(2):
        peers(a, lambda p: a1_send(j, p).wait_send())
        peers(b, lambda p: a2_send(j, p).wait_send())
    for j in range(2):
        peers(a, lambda p: a3_from(j, p).wait_recv())

    choose = pick[...][:, 0:half]
    choose_b = choose.astype(BF16)
    squares = jnp.zeros((half, 128), F32)
    largest = jnp.zeros((half, 128), F32)
    for p in range(SIDE):
        parts_r = []
        gains = []
        for j in range(2):
            block = rf[p, part_rows(j), :].astype(F32)
            count = CUTS[j + 1] - CUTS[j]
            parts_r += [block[half * t : half * (t + 1)] for t in range(count)]
            gains += [block[half * count + t : half * count + t + 1] for t in range(count)]
        for v, gv in zip(parts_r, gains):
            squares = squares + v * v
            largest = jnp.maximum(largest, jnp.abs(v * gv))
        rows = jnp.concatenate(parts_r, axis=1).astype(BF16)
        chosen = jnp.dot(choose_b, rows, preferred_element_type=F32)
        y[p] = chosen * jnp.concatenate(gains, axis=1)
    inverse = lax.rsqrt(jnp.sum(squares, axis=1, keepdims=True) / cols + small_eps)
    peak = inverse * jnp.max(largest, axis=1, keepdims=True) + small_eps
    spread = jnp.concatenate(
        [jnp.broadcast_to(inverse / peak, (half, 128)), jnp.broadcast_to(peak, (half, 128))], axis=1
    )
    slots = jnp.dot(choose, spread, preferred_element_type=F32, precision=lax.Precision.HIGHEST)
    code = jnp.concatenate([slots[:, 0:128]] * tiles, axis=1)
    peaks = slots[:, 128:256]
    xs[...] = peaks[8:16]
    for k in range(SIDE // 2):
        fs[k] = jnp.concatenate(
            [y[2 * k + d, 8:16, :] * code[8:16] for d in range(2)], axis=0
        ).astype(BF16)
    x_partner = dcopy(xs, xr, D_X, partner)
    f_partner = dcopy(fs, fr, D_F, partner)
    x_partner.start()
    f_partner.start()
    x_partner.wait_recv()
    peaks = peaks[0:8] + xr[...]
    scale_slots = jnp.zeros((2, CAP), F32)
    for j in range(2):
        for k in range(CAP):
            here = (sublanes((2, CAP)) == j) & (lanes((2, CAP)) == k)
            r = CAP * j + k
            scale_slots = jnp.where(here, peaks[r : r + 1, 0:1], scale_slots)
    scale_out[...] = scale_slots
    f_partner.wait_recv()
    for k in range(SIDE // 2):
        there = fr[k].astype(F32)
        for d in range(2):
            p = 2 * k + d
            rows = (y[p, 0:8, :] * code[0:8] + there[8 * d : 8 * d + 8]).astype(BF16)
            for e in range(2):
                disp_out[e, :, pl.ds(p * width, width)] = rows[CAP * e : CAP * e + CAP]

    for j in range(2):
        peers(a, lambda p: a3_send(j, p).wait_send())
    x_partner.wait_send()
    f_partner.wait_send()


def per_device(
    queries, latent_cache, context_lengths, value_up, out_proj, residual, norm_gain, expert_ids,
    gate_weights,
):
    seqs, ctx_dev, entry = latent_cache.shape
    half = seqs // 2
    columns = out_proj.shape[1]
    width = columns // SIDE
    piece = residual.shape[1]
    experts = 2
    rows = sum(padded(CUTS[k + 1] - CUTS[k], half) for k in range(2))
    any_space = pl.BlockSpec(memory_space=pl.ANY)
    vmem = pl.BlockSpec(memory_space=pltpu.VMEM)
    V = pltpu.VMEM
    chunk = (PARTS, SIDE, half // PARTS, 16, 128)
    eights = (SIDE, 8, 128)
    scratch = [
        V(queries.shape, BF16),
        V((seqs, 128), F32),
        V((seqs, 128), F32),
        V((ROWS, 128), BF16),
        V((SIDE, SIDE, 2, ROWS, 128), BF16),
        V((SIDE * A_GROUP, 128), F32),
        V((2, half, entry, ctx_dev), BF16),
        V((half, H, 2 * ctx_dev), BF16),
        V(chunk, BF16),
        V(chunk, BF16),
        V(eights, F32),
        V(eights, F32),
        V((8, 128), F32),
        V(eights, F32),
        V(eights, F32),
        V((SIDE, half, 8, 128), F32),
        V((half, 16, 128), F32),
        V((384, 128), F32),
        V((SIDE, 2 * ROWS, 128), BF16),
        V((SIDE, 2 * ROWS, 128), BF16),
        V((2, 128, VD), BF16),
        V((2, seqs, piece), BF16),
        V((2, 1, piece), BF16),
        V((seqs + 8, 128), F32),
        V((seqs + 8, 128), F32),
        V((ROWS, 128), F32),
        V((SIDE, 256, width), BF16),
        V((SIDE, rows, 128), BF16),
        V((SIDE, rows, 128), BF16),
        V((rows, 128), BF16),
        V((SIDE, rows, 128), BF16),
        V((SIDE, rows, 128), BF16),
        V(expert_ids.shape[::-1], jnp.int32),
        V(gate_weights.shape[::-1], F32),
        V((16, 128), F32),
        V((16, 128), F32),
        V((SIDE, 16, width), F32),
        V((SIDE // 2, 16, width), BF16),
        V((SIDE // 2, 16, width), BF16),
        V((8, 128), F32),
        V((8, 128), F32),
        pltpu.SMEM(context_lengths.shape, jnp.int32),
        pltpu.SemaphoreType.DMA((25,)),
        pltpu.SemaphoreType.DMA((PHASES, SIDE)),
        pltpu.SemaphoreType.DMA((PHASES, SIDE)),
        pltpu.SemaphoreType.DMA((SIDE, SIDE)),
        pltpu.SemaphoreType.DMA((SIDE, SIDE)),
        pltpu.SemaphoreType.DMA((half // 2,)),
        pltpu.SemaphoreType.DMA((half // 2,)),
        pltpu.SemaphoreType.DMA((8,)),
        pltpu.SemaphoreType.DMA((8,)),
        pltpu.SemaphoreType.REGULAR((3,)),
    ]
    dispatched, slot_scale, slot_gate = pl.pallas_call(
        kernel,
        out_shape=(
            jax.ShapeDtypeStruct((experts, CAP, columns), BF16),
            jax.ShapeDtypeStruct((experts, CAP), F32),
            jax.ShapeDtypeStruct((experts, CAP), F32),
        ),
        in_specs=[any_space] * 9,
        out_specs=(vmem, vmem, vmem),
        scratch_shapes=scratch,
        compiler_params=pltpu.CompilerParams(collective_id=0, has_side_effects=True),
    )(
        queries, latent_cache.transpose(0, 2, 1), context_lengths, value_up, out_proj, residual,
        norm_gain[None, :], expert_ids.T, gate_weights.T,
    )
    def hand_over(*refs):
        for source, target in zip(refs[:3], refs[3:]):
            target[...] = source[...]

    results = (dispatched, slot_scale, slot_gate)
    return pl.pallas_call(
        hand_over,
        out_shape=tuple(jax.ShapeDtypeStruct(r.shape, r.dtype) for r in results),
        in_specs=[vmem] * 3,
        out_specs=(vmem,) * 3,
    )(*results)


def solution(mesh):
    split = Mesh(
        mesh.devices.reshape(mesh.shape["groups"], SIDE, SIDE, 2),
        ("groups", "kv_0", "kv_1", "kv_2"),
    )
    in_specs = (
        P("groups", KV),
        P("groups", KV, None),
        P("groups"),
        P(KV, None),
        P(KV, None),
        P("groups", KV),
        P(KV),
        P("groups", None),
        P("groups", None),
    )
    out_specs = (P(GROUPS_KV, None, None), P(GROUPS_KV, None), P(GROUPS_KV, None))
    return jax.shard_map(
        per_device, mesh=split, in_specs=in_specs, out_specs=out_specs, check_vma=False
    )
```

```python
import functools

import jax
import jax.numpy as jnp
from jax import lax
from jax.experimental import pallas as pl
from jax.experimental.pallas import tpu as pltpu
from jax.sharding import Mesh
from jax.sharding import PartitionSpec as P

H = 32
LAT = 512
ROPE = 64
VD = 128
TOPK = 8
CAP = 2
SIDE = 8
QUARTERS = 4
ROWS = 24
PITCH = 5 * ROWS
A_GROUP = QUARTERS * PITCH + 8
KV = ("kv_0", "kv_1", "kv_2")
GROUPS_KV = ("groups", "kv_0", "kv_1", "kv_2")
FAR_FIRST = (4, 3, 5, 2, 6, 1, 7)
DIRECT = (3, 4, 5)
PARTS = 2
CUTS = (0, 4, 7)
MESH = pl.DeviceIdType.MESH
F32 = jnp.float32
BF16 = jnp.bfloat16

score_scale = 192.0 ** (-0.5)
masked_score = -1e30
small_eps = 1e-06

Q1, Q1B, ML2, O2, A1, A2, A3, O1 = 0, 1, 2, 3, 4, 6, 8, 10
ML1 = O1 + PARTS
PHASES = ML1 + PARTS
D_VU, D_RES, D_GAIN, D_W, D_F, D_X, D_NW, D_N = range(8)


def lanes(shape):
    return lax.broadcasted_iota(jnp.int32, shape, len(shape) - 1)


def sublanes(shape):
    return lax.broadcasted_iota(jnp.int32, shape, len(shape) - 2)


def loop(count, body):
    def step(i, carry):
        body(i)
        return carry

    lax.fori_loop(0, count, step, 0)


def padded(tiles, half):
    return -(-tiles * (half + 1) // 8) * 8


def far_first(i):
    return SIDE // 2 + (1 - 2 * lax.rem(i, 2)) * lax.div(i + 1, 2)


def kernel(
    q_in, cache_in, ctx_in, vu_in, op_in, res_in, gain_in, ids_in, gate_in,
    disp_out, scale_out, gate_out,
    qraw, ext, main, qs, qb, qa, cache, wb, s1, r1, ml1, rml1,
    ml2, rml2, fown, wown, acc, ab, s2, r2, vu, res, gain, ta, tb, lhs, w,
    s3, r3, s4, r4, rf, ids, gate, pt, pick, y, fs, fr, xs, xr,
    ctx, loc, ssem, rsem, qsend, qrecv, ksend, krecv, dsend, drecv, steps,
):
    g = lax.axis_index("groups")
    yy = lax.axis_index("kv_0")
    xx = lax.axis_index("kv_1")
    c = lax.axis_index("kv_2")
    chip = yy * SIDE + xx
    dev = chip * 2 + c
    a = xx + c * (yy - xx)
    b = yy + c * (xx - yy)
    half_x = lax.rem(xx, 2)
    half, ctx_dev = cache.shape[1], cache.shape[3]
    seqs = 2 * half
    width = w.shape[2]
    tiles = width // 128
    cols = SIDE * width

    def first(p):
        return (g, yy + c * (p - yy), xx + (1 - c) * (p - xx), c)

    def second(p):
        return (g, yy + (1 - c) * (p - yy), xx + c * (p - xx), c)

    def across(p):
        return (g, yy + (1 - c) * (p - yy), xx + c * (p - xx), 1 - c)

    partner = (g, yy, xx, 1 - c)
    neighbour = (g, yy, xx + 1 - 2 * half_x, c)

    def rcopy(src, dst, phase, to, frm, device, recv_phase=None, recv_from=None):
        recv = (phase, frm) if recv_phase is None else (recv_phase, recv_from)
        return pltpu.make_async_remote_copy(
            src_ref=src, dst_ref=dst, send_sem=ssem.at[phase, to], recv_sem=rsem.at[recv],
            device_id=device, device_id_type=MESH,
        )

    def dcopy(src, dst, which, device):
        return pltpu.make_async_remote_copy(
            src_ref=src, dst_ref=dst, send_sem=dsend.at[which], recv_sem=drecv.at[which],
            device_id=device, device_id_type=MESH,
        )

    def peers(me, body):
        for d in FAR_FIRST:
            body(lax.rem(me + d, SIDE))

    def peers_loop(me, body):
        def one(i):
            body(lax.rem(me + far_first(i), SIDE))

        loop(SIDE - 1, one)

    def local(src, dst, k):
        return pltpu.make_async_copy(src, dst, loc.at[k])

    w_row = pl.multiple_of(half_x * 64 + c * 32, 32)
    q_load = local(q_in, qraw, 0)
    q_load.start()
    small = [
        local(vu_in, vu.at[c], 1),
        local(res_in, res.at[c], 2),
        local(gain_in, gain.at[c], 23),
        local(ids_in, ids, 3),
        local(ctx_in, ctx, 24),
        local(gate_in, gate, 4),
    ]
    for copy in small:
        copy.start()
    w_loads = [
        local(op_in.at[:, pl.ds(p * width, width)], w.at[p, pl.ds(w_row, 32), :], 5 + p)
        for p in range(SIDE)
    ]
    for copy in w_loads:
        copy.start()
    parts = ksend.shape[0]
    each = half // parts
    k_loads = [
        local(
            cache_in.at[pl.ds(c * half + each * p, each)], cache.at[c, pl.ds(each * p, each)], 13 + p
        )
        for p in range(parts)
    ]

    def k_copy(p):
        return pltpu.make_async_remote_copy(
            src_ref=cache_in.at[pl.ds((1 - c) * half + each * p, each)],
            dst_ref=cache.at[c, pl.ds(each * p, each)],
            send_sem=ksend.at[p], recv_sem=krecv.at[p], device_id=partner, device_id_type=MESH,
        )

    def k_from(p):
        return pltpu.make_async_remote_copy(
            src_ref=cache_in.at[pl.ds(each * p, each)],
            dst_ref=cache.at[1 - c, pl.ds(each * p, each)],
            send_sem=ksend.at[p], recv_sem=krecv.at[p], device_id=partner, device_id_type=MESH,
        )

    for copy in k_loads:
        copy.start()

    barrier = pltpu.get_barrier_semaphore()
    pl.semaphore_signal(barrier, inc=1, device_id=partner, device_id_type=MESH)

    def greet(p):
        pl.semaphore_signal(barrier, inc=1, device_id=first(p), device_id_type=MESH)
        y, x = first(p)[1:3]
        pl.semaphore_signal(barrier, inc=1, device_id=(g, y, x, 1 - c), device_id_type=MESH)

    def greet_second(p):
        pl.semaphore_signal(barrier, inc=1, device_id=second(p), device_id_type=MESH)
        pl.semaphore_signal(barrier, inc=1, device_id=across(p), device_id_type=MESH)

    peers(a, greet)
    peers(b, greet_second)

    ext[...] = jnp.zeros(ext.shape, F32)
    q_load.wait()
    quarter = half_x * 2 + c
    ext[:, 0:16] = qraw[:, 128:144].astype(F32)
    main[...] = pltpu.roll(qraw[:, 0:128].astype(F32), quarter * 16, 1)

    def chunk_of(base):
        extra = jnp.zeros((4, 128), F32)
        for k in range(half // 4):
            row = base + 4 * k
            extra = extra + pltpu.roll(ext[row : row + 4, :], lax.rem(quarter + k, 8) * 16, 1)
        return jnp.concatenate([main[base : base + half, :], extra], axis=0)

    halves = [chunk_of(0), chunk_of(half)]
    qb[b, a, c] = jnp.where(c == 0, halves[0], halves[1]).astype(BF16)
    qs[...] = jnp.where(c == 0, halves[1], halves[0]).astype(BF16)

    pl.semaphore_wait(barrier, 4 * (SIDE - 1) + 1)

    def q1(p):
        return rcopy(qb.at[b, a, c], qb.at[b, a, c], Q1, p, 0, first(p), Q1 + c, a)

    def q1_across(p):
        return rcopy(qs, qb.at[a, b, c], Q1B, p, 0, across(p), Q1 + c, b)

    def q1_from(p, core):
        return rcopy(qs, qb.at[b, p, core], Q1, p, 0, first(p), Q1 + core, p)

    q1_across(b).start()
    peers(a, lambda p: q1(p).start())
    peers(b, lambda p: q1_across(p).start())

    def q2(slot, source, chunk, to):
        block = qb.at[source, chunk]
        return pltpu.make_async_remote_copy(
            src_ref=block, dst_ref=block, send_sem=qsend.at[slot, chunk],
            recv_sem=qrecv.at[source, chunk], device_id=second(to), device_id_type=MESH,
        )

    def at(me, distance):
        return lax.rem(me + distance, SIDE)

    def spread(distances):
        for d in distances:
            chunk = at(a, d)
            if d:
                q1_from(chunk, c).wait_recv()
            q1_from(chunk, 1 - c).wait_recv()
            for e in FAR_FIRST if d in DIRECT else (2, 6, 1, 7):
                q2(e, b, chunk, at(b, e)).start()

    def relay(distances):
        for d in [d for d in distances if d not in DIRECT]:
            chunk = at(a, d)
            source = at(b, 6)
            q2(1, source, chunk, source).wait_recv()
            q2(3, source, chunk, at(b, 1)).start()
            if d % 2 == 0:
                q2(4, source, chunk, at(b, 2)).start()
            source = at(b, 2)
            q2(1, source, chunk, source).wait_recv()
            q2(5, source, chunk, at(b, 7)).start()
            if d % 2 == 1:
                q2(0, source, chunk, at(b, 6)).start()

    for copy in w_loads:
        copy.wait()
    w_rows = w.at[:, pl.ds(w_row, 32), :]
    beside = pl.multiple_of((1 - half_x) * 64 + c * 32, 32)
    w_beside = w.at[:, pl.ds(beside, 32), :]
    w_out, w_in = [], []
    for k in range(2):
        some = pl.ds(k * (SIDE // 2), SIDE // 2)
        ours, theirs = w.at[some, pl.ds(w_row, 32), :], w.at[some, pl.ds(beside, 32), :]
        w_out.append(dcopy(ours, ours, D_N + k, neighbour))
        w_in.append(dcopy(theirs, theirs, D_N + k, neighbour))
    w_across = dcopy(w_beside, w_beside, D_NW, partner)

    @pl.when(c == 0)
    def _():
        w_out[0].start()
        w_out[1].start()

    spread((0,))
    k_copy(0).start()
    spread((1, 7))
    k_copy(1).start()
    spread((2, 6))
    k_copy(2).start()
    relay((0,))
    k_copy(3).start()
    spread((3, 5))
    k_copy(4).start()
    spread((4,))
    k_copy(5).start()
    relay((1, 7))
    k_copy(6).start()
    relay((2, 6))
    k_copy(7).start()
    relay((3, 5, 4))
    pl.when(c == 1)(w_out[0].start)
    k_copy(8).start()
    k_copy(9).start()


    for copy in small:
        copy.wait()
    to_partner = [
        dcopy(vu.at[c], vu.at[c], D_VU, partner),
        dcopy(res.at[c], res.at[c], D_RES, partner),
        dcopy(gain.at[c], gain.at[c], D_GAIN, partner),
        dcopy(w_rows, w_rows, D_W, partner),
    ]
    for copy in to_partner[:3]:
        copy.start()

    for ref in (ab, ta, tb, pt):
        ref[...] = jnp.zeros(ref.shape, F32)
    to_partner[3].start()

    lane = lanes((ROWS, 128))
    lane8 = lanes((8, 128))
    low = sublanes((8, 128)) < 4

    def assemble(hy):
        for hg in range(QUARTERS):
            m = []
            for e in range(2):
                x = 2 * hg + e
                for q in range(2):
                    m.append(qb[hy + c * (x - hy), x + c * (hy - x), q].astype(F32))
            turned = []
            for k in range(half // 4):
                picked = m[0][16:ROWS]
                for i in range(1, QUARTERS):
                    picked = jnp.where(lax.div(lane8, 16) == (k + i) % 8, m[i][16:ROWS], picked)
                picked = pltpu.roll(picked, (128 - 16 * k) % 128, 1)
                turned.append(picked if k % 2 else pltpu.roll(picked, 4, 0))
            e = jnp.concatenate(
                [
                    jnp.where(low, turned[0], turned[1]),
                    jnp.where(low, turned[2], turned[3]),
                    turned[4],
                ],
                axis=0,
            )
            whole = [
                m[0],
                jnp.where(lane < 16, e, m[1]),
                jnp.where(lane < 16, m[1], jnp.where(lane < 32, e, m[2])),
                jnp.where(lane < 32, m[2], jnp.where(lane < 48, e, m[3])),
                jnp.where(lane < 48, m[3], e),
            ]
            base = hy * (A_GROUP - 8 * c) + hg * PITCH
            for t in range(5):
                qa[pl.ds(pl.multiple_of(base + t * ROWS, 8), ROWS), :] = whole[t]

    def missing(d, e):
        if e and (d in DIRECT or e not in (2, 6)):
            chunk, source = at(a, d), at(b, e)
            q2(1, source, chunk, source).wait_recv()

    @pl.when(c == 0)
    def _():
        for e in (0, 2, 6, 1, 7, 3, 5, 4):
            for d in (0, 1, 7, 2, 6, 3, 5, 4):
                missing(d, e)
            assemble(at(b, e))

    @pl.when(c == 1)
    def _():
        for d in (0, 1, 7, 2, 6, 3, 5, 4):
            for e in (2, 6, 1, 7, 3, 5, 4):
                missing(d, e)
            assemble(at(a, d))


    for copy in k_loads:
        copy.wait()
    for p in range(parts):
        k_from(p).wait_recv()
    position = chip * 2 * ctx_dev + lanes((1, 2 * ctx_dev))
    part_k = half // PARTS
    many = half // PARTS

    def weigh(s, by_column):
        pieces = []
        for t in range(5):
            groups = []
            for k in range(4):
                if by_column:
                    rows = pl.ds(k * PITCH + t * ROWS + s, 8, stride=A_GROUP)
                else:
                    rows = pl.ds(8 * k * PITCH + t * ROWS + s, 8, stride=PITCH)
                groups.append(qa[rows, :])
            pieces.append(jnp.concatenate(groups, axis=0).astype(BF16))
        q = jnp.concatenate(pieces, axis=1)[:, : LAT + ROPE]
        keys = jnp.concatenate([cache[0, s], cache[1, s]], axis=1)
        scores = jnp.dot(q, keys, preferred_element_type=F32)
        valid = position < ctx[c * half + s]
        scores = jnp.where(valid, scores * score_scale, masked_score)
        top = jnp.max(scores, axis=1, keepdims=True)
        weights = jnp.where(valid, jnp.exp(scores - top), 0.0)
        total = jnp.sum(weights, axis=1, keepdims=True)
        wb[s] = weights.astype(BF16)
        return top, total

    def merge(u, v, first_rows):
        if first_rows:
            return jnp.where(low, u, pltpu.roll(v, 4, 0))
        return jnp.where(low, pltpu.roll(u, 4, 0), v)

    def put(tile, k, top, total):
        return jnp.where(lane8 == k, top, jnp.where(lane8 == 64 + k, total, tile))

    def weigh_columns(i):
        tiles_m = [jnp.zeros((8, 128), F32) for _ in range(4)]
        for u in range(many):
            s = i * many + u
            top, total = weigh(s, True)
            for k in range(4):
                rows = slice(8 * k, 8 * k + 8)
                tiles_m[k] = put(tiles_m[k], s, top[rows], total[rows])
        for k in range(4):
            for d in range(2):
                ml1[i, 2 * k + d] = tiles_m[k]

    def weigh_rows(i):
        tiles_m = [jnp.zeros((8, 128), F32) for _ in range(SIDE)]
        for u in range(many // 2):
            pair = i * (many // 2) + u
            t0, l0 = weigh(2 * pair, False)
            t1, l1 = weigh(2 * pair + 1, False)
            for k in range(4):
                rows = slice(8 * k, 8 * k + 8)
                wide = [jnp.broadcast_to(v[rows], (8, 128)) for v in (t0, t1, l0, l1)]
                for d in range(2):
                    top = merge(wide[0], wide[1], d == 0)
                    total = merge(wide[2], wide[3], d == 0)
                    for e in range(2):
                        tile = tiles_m[2 * k + d]
                        tiles_m[2 * k + d] = put(tile, 2 * pair + e, top, total)
        for p in range(SIDE):
            ml1[i, p] = tiles_m[p]

    def mlsend(i, p):
        return rcopy(ml1.at[i, p], rml1.at[i, a], ML1 + i, p, a, first(p))

    def ml_from(i, p):
        return rcopy(ml1.at[i, p], rml1.at[i, p], ML1 + i, p, p, first(p))

    def attend(s):
        values = jnp.concatenate([cache[0, s, 0:LAT, :], cache[1, s, 0:LAT, :]], axis=1)
        return lax.dot_general(
            wb[s], values, (((1,), (1,)), ((), ())), preferred_element_type=F32
        )

    def by_column(dst, i):
        for u in range(part_k):
            out = attend(i * part_k + u)
            for k in range(4):
                rows = slice(8 * k, 8 * k + 8)
                for d in range(2):
                    lo = out[rows, 256 * d : 256 * d + 128]
                    hi = out[rows, 256 * d + 128 : 256 * d + 256]
                    dst[i, 2 * k + d, u] = jnp.concatenate([lo, hi], axis=0).astype(dst.dtype)

    def by_row(dst, i):
        for u in range(part_k // 2):
            s = i * part_k + 2 * u
            o0 = attend(s)
            o1 = attend(s + 1)
            for k in range(4):
                rows = slice(8 * k, 8 * k + 8)
                for d in range(2):
                    for e in range(2):
                        blocks = [
                            merge(
                                o0[rows, 128 * t : 128 * t + 128],
                                o1[rows, 128 * t : 128 * t + 128],
                                d == 0,
                            )
                            for t in (2 * e, 2 * e + 1)
                        ]
                        dst[i, 2 * k + d, 2 * u + e] = jnp.concatenate(blocks, axis=0).astype(
                            dst.dtype
                        )

    def osend(i, p):
        return rcopy(s1.at[i, p], r1.at[i, a], O1 + i, p, a, first(p))

    def o_from(i, p):
        return rcopy(s1.at[i, p], r1.at[i, p], O1 + i, p, p, first(p))

    def twice(f):
        return jnp.concatenate([f, f], axis=0)

    def on_core(columns, rows):
        pl.when(c == 0)(columns)
        pl.when(c == 1)(rows)

    for i in range(PARTS):
        on_core(lambda: weigh_columns(i), lambda: weigh_rows(i))
        peers(a, lambda p: mlsend(i, p).start())
        on_core(lambda: by_column(s1, i), lambda: by_row(s1, i))
        peers(a, lambda p: osend(i, p).start())


    def fill(p):
        def block(k):
            start = pl.multiple_of(k * 16, 16)
            row = start + sublanes((16, width))
            column = p * width + lanes((16, width))
            target = chip * 112 + lax.rem(row, 64) + 56 * lax.div(row, 64)
            hit = jnp.where((column == target) & (lax.rem(row, 64) < 56), 1.0, 0.0)
            w[p, pl.ds(pl.multiple_of(128 + start, 16), 16), :] = hit.astype(BF16)

        loop(8, block)

    loop(SIDE, fill)

    idv = ids[...]
    gatev = gate[...]
    hits = jnp.zeros((8, seqs), F32)
    hit_rows = []
    gates = []
    for j in range(4):
        expert = (dev if j < 2 else chip * 2 + 1 - c) * 2 + j % 2
        same = idv == expert
        hit = jnp.sum(jnp.where(same, 1.0, 0.0), axis=0, keepdims=True)
        hit_rows.append(hit)
        gates.append(jnp.sum(jnp.where(same, gatev, 0.0), axis=0, keepdims=True))
        hits = jnp.where(sublanes((8, seqs)) == j, hit, hits)
    earlier = jnp.where(sublanes((seqs, seqs)) < lanes((seqs, seqs)), 1.0, 0.0)
    rank = jnp.dot(hits.astype(BF16), earlier.astype(BF16), preferred_element_type=F32)
    table = jnp.zeros((16, seqs), F32)
    gate_slots = jnp.zeros((2, CAP), F32)
    for j in range(4):
        for k in range(CAP):
            chosen = jnp.where(rank[j : j + 1] == float(k), hit_rows[j], 0.0)
            r = (j // 2) * 8 + (j % 2) * CAP + k
            table = jnp.where(sublanes((16, seqs)) == r, chosen, table)
            if j < 2:
                total = jnp.sum(chosen * gates[j], axis=1, keepdims=True)
                here = (sublanes((2, CAP)) == j) & (lanes((2, CAP)) == k)
                gate_slots = jnp.where(here, total, gate_slots)
    gate_out[...] = gate_slots
    pt[:, 0:seqs] = table
    own = jnp.where(c == 0, pt[...], pltpu.roll(pt[...], 128 - half, 1))
    pick[...] = jnp.where(lanes((16, 128)) < half, own, 0.0)

    for copy in to_partner[:3]:
        copy.wait_recv()
    ta[0:seqs, 0:56] = res[0].astype(F32)
    tb[0:seqs, 0:56] = res[1].astype(F32)
    ta[seqs : seqs + 1, 0:56] = gain[0].astype(F32)
    tb[seqs : seqs + 1, 0:56] = gain[1].astype(F32)
    both = ta[...] + pltpu.roll(tb[...], 64, 1)
    ta[...] = both
    row = sublanes((ROWS, 128))
    mine = jnp.where(c == 0, ta[0:ROWS, :], ta[half : half + ROWS, :])
    gain_row = jnp.broadcast_to(ta[seqs : seqs + 1, :], (ROWS, 128))
    lhs[...] = jnp.where(row < half, mine, jnp.where(row == half, gain_row, 0.0))

    def ml2_send(p):
        return rcopy(ml2, rml2.at[b], ML2, p, b, second(p))

    def ml2_from(p):
        return rcopy(ml2, rml2.at[p], ML2, p, p, second(p))

    def add(block, i, p, fresh):
        for k in range(part_k):
            term = twice(wown[p, k]) * block[k].astype(F32)
            index = i * part_k + k
            acc[index] = term if fresh else acc[index] + term

    packed = jnp.zeros((8, 128), F32)
    for i in range(PARTS):
        peers(a, lambda p: ml_from(i, p).wait_recv())
        rml1[i, a] = ml1[i, a]
        row_top = rml1[i, 0]
        for p in range(1, SIDE):
            row_top = jnp.maximum(row_top, rml1[i, p])
        total = jnp.zeros((8, 128), F32)
        for p in range(SIDE):
            factor = jnp.exp(rml1[i, p] - row_top)
            total = total + factor * pltpu.roll(rml1[i, p], 64, 1)
            fown[p] = factor
        both = jnp.where(lane8 < 64, row_top, pltpu.roll(total, 64, 1))
        group = lax.rem(lane8, 64)
        packed = jnp.where((group >= i * part_k) & (group < (i + 1) * part_k), both, packed)
        if i == PARTS - 1:
            ml2[...] = packed
            peers(b, lambda p: ml2_send(p).start())
            pl.when(c == 1)(w_out[1].start)
        for p in range(SIDE):
            f = fown[p]
            for k in range(part_k):
                lane_k = i * part_k + k
                wown[p, k] = jnp.broadcast_to(f[:, lane_k : lane_k + 1], (8, 128))
        add(s1.at[i, a], i, a, True)

        def take(p):
            o_from(i, p).wait_recv()
            add(r1.at[i, p], i, p, False)

        peers_loop(a, take)

    @pl.when(c == 0)
    def _():
        for k in range(half):
            for d in range(2):
                ab[d * 192 + k * 8 : d * 192 + k * 8 + 8, :] = acc[k, 8 * d : 8 * d + 8, :]
        for j in range(SIDE):
            s2[j] = jnp.concatenate(
                [ab[pl.ds(d * 192 + j, ROWS, stride=8), :] for d in range(2)], axis=0
            ).astype(BF16)

    @pl.when(c == 1)
    def _():
        for k in range(half):
            for d in range(2):
                base = ((k % 2) * 2 + d) * 96 + (k // 2) * 8
                ab[base : base + 8, :] = acc[k, 8 * d : 8 * d + 8, :]
        for j in range(SIDE):
            s2[j] = jnp.concatenate(
                [ab[pl.ds(((j % 2) * 2 + d) * 96 + j // 2, ROWS, stride=4), :] for d in range(2)],
                axis=0,
            ).astype(BF16)

    def o2_send(p):
        return rcopy(s2.at[p], r2.at[b], O2, p, b, second(p))

    def o2_from(p):
        return rcopy(s2.at[p], r2.at[p], O2, p, p, second(p))

    peers(b, lambda p: o2_send(p).start())
    peers(b, lambda p: ml2_from(p).wait_recv())
    rml2[b] = packed
    row_even = b - c * (b - lax.div(b, 2))
    row_odd = row_even + 4 * c
    even = lax.rem(lanes((1, 128)), 2) == 0
    each_ml = jnp.concatenate(
        [
            jnp.where(even, rml2[p, pl.ds(row_even, 1), :], rml2[p, pl.ds(row_odd, 1), :])
            for p in range(SIDE)
        ],
        axis=0,
    )
    factor = jnp.exp(each_ml - jnp.max(each_ml, axis=0, keepdims=True))
    total = jnp.sum(factor * pltpu.roll(each_ml, 64, 1), axis=0, keepdims=True)
    factor = jnp.where(lane8 < half, factor / total, 0.0)
    factor = jnp.concatenate([factor, jnp.zeros((120, 128), F32)], axis=0).T
    factors = [jnp.broadcast_to(factor[0:ROWS, p : p + 1], (ROWS, 128)) for p in range(SIDE)]
    for copy in w_in:
        copy.wait_recv()
    w_across.start()
    peers(b, lambda p: o2_from(p).wait_recv())
    r2[b] = s2[b]
    merged = twice(factors[0]) * r2[0].astype(F32)
    for p in range(1, SIDE):
        merged = merged + twice(factors[p]) * r2[p].astype(F32)

    part = jnp.zeros((ROWS, VD), F32)
    for k in range(2):
        block = merged[ROWS * k : ROWS * (k + 1)]
        high = block.astype(BF16)
        low = (block - high.astype(F32)).astype(BF16)
        part = part + jnp.dot(high, vu[k], preferred_element_type=F32)
        part = part + jnp.dot(low, vu[k], preferred_element_type=F32)
    to_partner[3].wait_recv()
    w_across.wait_recv()
    left = jnp.concatenate([part.astype(BF16), lhs[...].astype(BF16)], axis=1)

    def part_rows(j):
        sizes = [padded(CUTS[k + 1] - CUTS[k], half) for k in range(2)]
        return pl.ds(sum(sizes[:j]), sizes[j])

    def a1_send(j, p):
        rows = part_rows(j)
        return rcopy(s3.at[p, rows], r3.at[a, rows], A1 + j, p, a, first(p))

    def a1_from(j, p):
        rows = part_rows(j)
        return rcopy(s3.at[p, rows], r3.at[p, rows], A1 + j, p, p, first(p))

    def a2_send(j, p):
        rows = part_rows(j)
        return rcopy(s4.at[rows], r4.at[b, rows], A2 + j, p, b, second(p))

    def a2_from(j, p):
        rows = part_rows(j)
        return rcopy(s4.at[rows], r4.at[p, rows], A2 + j, p, p, second(p))

    def a3_send(j, p):
        rows = part_rows(j)
        return rcopy(rf.at[a, rows], rf.at[a, rows], A3 + j, p, a, first(p))

    def a3_from(j, p):
        rows = part_rows(j)
        return rcopy(rf.at[p, rows], rf.at[p, rows], A3 + j, p, p, first(p))

    def in_step(k):
        pl.semaphore_signal(steps.at[k], inc=1, device_id=partner, device_id_type=MESH)
        pl.semaphore_wait(steps.at[k], 1)

    def project(j, p):
        out = jnp.dot(left, w[p, :, 128 * CUTS[j] : 128 * CUTS[j + 1]], preferred_element_type=F32)
        count = CUTS[j + 1] - CUTS[j]
        blocks = [out[:half, 128 * t : 128 * t + 128] for t in range(count)]
        blocks += [out[half : half + 1, 128 * t : 128 * t + 128] for t in range(count)]
        blocks.append(jnp.zeros((padded(count, half) - count * (half + 1), 128), F32))
        s3[p, part_rows(j), :] = jnp.concatenate(blocks, axis=0).astype(BF16)

    def total_of(ref, j):
        total = ref[0, part_rows(j), :].astype(F32)
        for p in range(1, SIDE):
            total = total + ref[p, part_rows(j), :].astype(F32)
        return total.astype(BF16)

    in_step(0)
    for j in range(2):

        for batch in ((4, 3, 5), (2, 6, 1, 7)):
            for d in batch:
                project(j, at(a, d))
            for d in batch:
                a1_send(j, at(a, d)).start()
    for j in range(2):
        project(j, a)
    for j in range(2):
        peers(a, lambda p: a1_from(j, p).wait_recv())
        r3[a, part_rows(j), :] = s3[a, part_rows(j), :]
        s4[part_rows(j), :] = total_of(r3, j)
        if j == 0:
            in_step(1)
        peers(b, lambda p: a2_send(j, p).start())
    peers(a, lambda p: q1(p).wait_send())
    loop(SIDE, lambda p: q1_across(p).wait_send())
    for p in range(parts):
        k_copy(p).wait_send()
    for d in range(SIDE):
        chunk = at(a, d)
        for slot in range(1, SIDE) if d in DIRECT else (1, 2, 3, 5, 6, 7, 4 if d % 2 == 0 else 0):
            q2(slot, b, chunk, at(b, 1)).wait_send()
    for i in range(PARTS):
        peers(a, lambda p: mlsend(i, p).wait_send())
    for i in range(PARTS):
        peers(a, lambda p: osend(i, p).wait_send())
    peers(b, lambda p: ml2_send(p).wait_send())
    peers(b, lambda p: o2_send(p).wait_send())
    for copy in to_partner + w_out + [w_across]:
        copy.wait_send()
    for j in range(2):
        peers(b, lambda p: a2_from(j, p).wait_recv())
        r4[b, part_rows(j), :] = s4[part_rows(j), :]
        rf[a, part_rows(j), :] = total_of(r4, j)
        if j == 0:
            in_step(2)
        peers(a, lambda p: a3_send(j, p).start())
    for j in range(2):
        peers(a, lambda p: a1_send(j, p).wait_send())
        peers(b, lambda p: a2_send(j, p).wait_send())
    for j in range(2):
        peers(a, lambda p: a3_from(j, p).wait_recv())

    choose = pick[...][:, 0:half]
    choose_b = choose.astype(BF16)
    squares = jnp.zeros((half, 128), F32)
    largest = jnp.zeros((half, 128), F32)
    for p in range(SIDE):
        parts_r = []
        gains = []
        for j in range(2):
            block = rf[p, part_rows(j), :].astype(F32)
            count = CUTS[j + 1] - CUTS[j]
            parts_r += [block[half * t : half * (t + 1)] for t in range(count)]
            gains += [block[half * count + t : half * count + t + 1] for t in range(count)]
        for v, gv in zip(parts_r, gains):
            squares = squares + v * v
            largest = jnp.maximum(largest, jnp.abs(v * gv))
        rows = jnp.concatenate(parts_r, axis=1).astype(BF16)
        chosen = jnp.dot(choose_b, rows, preferred_element_type=F32)
        y[p] = chosen * jnp.concatenate(gains, axis=1)
    inverse = lax.rsqrt(jnp.sum(squares, axis=1, keepdims=True) / cols + small_eps)
    peak = inverse * jnp.max(largest, axis=1, keepdims=True) + small_eps
    spread = jnp.concatenate(
        [jnp.broadcast_to(inverse / peak, (half, 128)), jnp.broadcast_to(peak, (half, 128))], axis=1
    )
    slots = jnp.dot(choose, spread, preferred_element_type=F32, precision=lax.Precision.HIGHEST)
    code = jnp.concatenate([slots[:, 0:128]] * tiles, axis=1)
    peaks = slots[:, 128:256]
    xs[...] = peaks[8:16]
    for k in range(SIDE // 2):
        fs[k] = jnp.concatenate(
            [y[2 * k + d, 8:16, :] * code[8:16] for d in range(2)], axis=0
        ).astype(BF16)
    x_partner = dcopy(xs, xr, D_X, partner)
    f_partner = dcopy(fs, fr, D_F, partner)
    x_partner.start()
    f_partner.start()
    x_partner.wait_recv()
    peaks = peaks[0:8] + xr[...]
    scale_slots = jnp.zeros((2, CAP), F32)
    for j in range(2):
        for k in range(CAP):
            here = (sublanes((2, CAP)) == j) & (lanes((2, CAP)) == k)
            r = CAP * j + k
            scale_slots = jnp.where(here, peaks[r : r + 1, 0:1], scale_slots)
    scale_out[...] = scale_slots
    f_partner.wait_recv()
    for k in range(SIDE // 2):
        there = fr[k].astype(F32)
        for d in range(2):
            p = 2 * k + d
            rows = (y[p, 0:8, :] * code[0:8] + there[8 * d : 8 * d + 8]).astype(BF16)
            for e in range(2):
                disp_out[e, :, pl.ds(p * width, width)] = rows[CAP * e : CAP * e + CAP]

    for j in range(2):
        peers(a, lambda p: a3_send(j, p).wait_send())
    x_partner.wait_send()
    f_partner.wait_send()


def per_device(
    queries, latent_cache, context_lengths, value_up, out_proj, residual, norm_gain, expert_ids,
    gate_weights,
):
    seqs, ctx_dev, entry = latent_cache.shape
    half = seqs // 2
    columns = out_proj.shape[1]
    width = columns // SIDE
    piece = residual.shape[1]
    experts = 2
    rows = sum(padded(CUTS[k + 1] - CUTS[k], half) for k in range(2))
    any_space = pl.BlockSpec(memory_space=pl.ANY)
    vmem = pl.BlockSpec(memory_space=pltpu.VMEM)
    V = pltpu.VMEM
    chunk = (PARTS, SIDE, half // PARTS, 16, 128)
    eights = (SIDE, 8, 128)
    scratch = [
        V(queries.shape, BF16),
        V((seqs, 128), F32),
        V((seqs, 128), F32),
        V((ROWS, 128), BF16),
        V((SIDE, SIDE, 2, ROWS, 128), BF16),
        V((SIDE * A_GROUP, 128), F32),
        V((2, half, entry, ctx_dev), BF16),
        V((half, H, 2 * ctx_dev), BF16),
        V(chunk, BF16),
        V(chunk, BF16),
        V((PARTS,) + eights, F32),
        V((PARTS,) + eights, F32),
        V((8, 128), F32),
        V(eights, F32),
        V(eights, F32),
        V((SIDE, half // PARTS, 8, 128), F32),
        V((half, 16, 128), F32),
        V((384, 128), F32),
        V((SIDE, 2 * ROWS, 128), BF16),
        V((SIDE, 2 * ROWS, 128), BF16),
        V((2, 128, VD), BF16),
        V((2, seqs, piece), BF16),
        V((2, 1, piece), BF16),
        V((seqs + 8, 128), F32),
        V((seqs + 8, 128), F32),
        V((ROWS, 128), F32),
        V((SIDE, 256, width), BF16),
        V((SIDE, rows, 128), BF16),
        V((SIDE, rows, 128), BF16),
        V((rows, 128), BF16),
        V((SIDE, rows, 128), BF16),
        V((SIDE, rows, 128), BF16),
        V(expert_ids.shape[::-1], jnp.int32),
        V(gate_weights.shape[::-1], F32),
        V((16, 128), F32),
        V((16, 128), F32),
        V((SIDE, 16, width), F32),
        V((SIDE // 2, 16, width), BF16),
        V((SIDE // 2, 16, width), BF16),
        V((8, 128), F32),
        V((8, 128), F32),
        pltpu.SMEM(context_lengths.shape, jnp.int32),
        pltpu.SemaphoreType.DMA((25,)),
        pltpu.SemaphoreType.DMA((PHASES, SIDE)),
        pltpu.SemaphoreType.DMA((PHASES, SIDE)),
        pltpu.SemaphoreType.DMA((SIDE, SIDE)),
        pltpu.SemaphoreType.DMA((SIDE, SIDE)),
        pltpu.SemaphoreType.DMA((half // 2,)),
        pltpu.SemaphoreType.DMA((half // 2,)),
        pltpu.SemaphoreType.DMA((9,)),
        pltpu.SemaphoreType.DMA((9,)),
        pltpu.SemaphoreType.REGULAR((3,)),
    ]
    dispatched, slot_scale, slot_gate = pl.pallas_call(
        kernel,
        out_shape=(
            jax.ShapeDtypeStruct((experts, CAP, columns), BF16),
            jax.ShapeDtypeStruct((experts, CAP), F32),
            jax.ShapeDtypeStruct((experts, CAP), F32),
        ),
        in_specs=[any_space] * 9,
        out_specs=(vmem, vmem, vmem),
        scratch_shapes=scratch,
        compiler_params=pltpu.CompilerParams(collective_id=0, has_side_effects=True),
    )(
        queries, latent_cache.transpose(0, 2, 1), context_lengths, value_up, out_proj, residual,
        norm_gain[None, :], expert_ids.T, gate_weights.T,
    )
    def hand_over(*refs):
        for source, target in zip(refs[:3], refs[3:]):
            target[...] = source[...]

    results = (dispatched, slot_scale, slot_gate)
    return pl.pallas_call(
        hand_over,
        out_shape=tuple(jax.ShapeDtypeStruct(r.shape, r.dtype) for r in results),
        in_specs=[vmem] * 3,
        out_specs=(vmem,) * 3,
    )(*results)


def solution(mesh):
    split = Mesh(
        mesh.devices.reshape(mesh.shape["groups"], SIDE, SIDE, 2),
        ("groups", "kv_0", "kv_1", "kv_2"),
    )
    in_specs = (
        P("groups", KV),
        P("groups", KV, None),
        P("groups"),
        P(KV, None),
        P(KV, None),
        P("groups", KV),
        P(KV),
        P("groups", None),
        P("groups", None),
    )
    out_specs = (P(GROUPS_KV, None, None), P(GROUPS_KV, None), P(GROUPS_KV, None))
    return jax.shard_map(
        per_device, mesh=split, in_specs=in_specs, out_specs=out_specs, check_vma=False
    )
```

```python
import functools

import jax
import jax.numpy as jnp
from jax import lax
from jax.experimental import pallas as pl
from jax.experimental.pallas import tpu as pltpu
from jax.sharding import Mesh
from jax.sharding import PartitionSpec as P

H = 32
LAT = 512
ROPE = 64
VD = 128
TOPK = 8
CAP = 2
SIDE = 8
QUARTERS = 4
ROWS = 24
PITCH = 5 * ROWS
A_GROUP = QUARTERS * PITCH + 8
KV = ("kv_0", "kv_1", "kv_2")
GROUPS_KV = ("groups", "kv_0", "kv_1", "kv_2")
FAR_FIRST = (4, 3, 5, 2, 6, 1, 7)
DIRECT = (3, 4, 5)
PARTS = 2
CUTS = (0, 4, 7)
MESH = pl.DeviceIdType.MESH
F32 = jnp.float32
BF16 = jnp.bfloat16

score_scale = 192.0 ** (-0.5)
masked_score = -1e30
small_eps = 1e-06

Q1, Q1B, ML2, O2, A1, A2, A3, O1 = 0, 1, 2, 3, 4, 6, 8, 10
ML1 = O1 + PARTS
PHASES = ML1 + PARTS
D_VU, D_RES, D_GAIN, D_W, D_F, D_X, D_NW, D_N = range(8)


def lanes(shape):
    return lax.broadcasted_iota(jnp.int32, shape, len(shape) - 1)


def sublanes(shape):
    return lax.broadcasted_iota(jnp.int32, shape, len(shape) - 2)


def loop(count, body):
    def step(i, carry):
        body(i)
        return carry

    lax.fori_loop(0, count, step, 0)


def padded(tiles, half):
    return -(-tiles * (half + 1) // 8) * 8


def far_first(i):
    return SIDE // 2 + (1 - 2 * lax.rem(i, 2)) * lax.div(i + 1, 2)


def kernel(
    q_in, cache_in, ctx_in, vu_in, op_in, res_in, gain_in, ids_in, gate_in,
    disp_out, scale_out, gate_out,
    qraw, ext, main, qs, qb, qa, cache, wb, s1, r1, ml1, rml1,
    ml2, rml2, fown, wown, acc, ab, s2, r2, vu, res, gain, ta, tb, lhs, w,
    s3, r3, s4, r4, rf, ids, gate, pt, pick, y, fs, fr, xs, xr,
    ctx, loc, ssem, rsem, qsend, qrecv, ksend, krecv, dsend, drecv, steps,
):
    g = lax.axis_index("groups")
    yy = lax.axis_index("kv_0")
    xx = lax.axis_index("kv_1")
    c = lax.axis_index("kv_2")
    chip = yy * SIDE + xx
    dev = chip * 2 + c
    a = xx + c * (yy - xx)
    b = yy + c * (xx - yy)
    half_x = lax.rem(xx, 2)
    half, ctx_dev = cache.shape[1], cache.shape[3]
    seqs = 2 * half
    width = w.shape[2]
    tiles = width // 128
    cols = SIDE * width

    def first(p):
        return (g, yy + c * (p - yy), xx + (1 - c) * (p - xx), c)

    def second(p):
        return (g, yy + (1 - c) * (p - yy), xx + c * (p - xx), c)

    def across(p):
        return (g, yy + (1 - c) * (p - yy), xx + c * (p - xx), 1 - c)

    partner = (g, yy, xx, 1 - c)
    neighbour = (g, yy, xx + 1 - 2 * half_x, c)

    def rcopy(src, dst, phase, to, frm, device, recv_phase=None, recv_from=None):
        recv = (phase, frm) if recv_phase is None else (recv_phase, recv_from)
        return pltpu.make_async_remote_copy(
            src_ref=src, dst_ref=dst, send_sem=ssem.at[phase, to], recv_sem=rsem.at[recv],
            device_id=device, device_id_type=MESH,
        )

    def dcopy(src, dst, which, device):
        return pltpu.make_async_remote_copy(
            src_ref=src, dst_ref=dst, send_sem=dsend.at[which], recv_sem=drecv.at[which],
            device_id=device, device_id_type=MESH,
        )

    def peers(me, body):
        for d in FAR_FIRST:
            body(lax.rem(me + d, SIDE))

    def peers_loop(me, body):
        def one(i):
            body(lax.rem(me + far_first(i), SIDE))

        loop(SIDE - 1, one)

    def local(src, dst, k):
        return pltpu.make_async_copy(src, dst, loc.at[k])

    w_row = pl.multiple_of(half_x * 64 + c * 32, 32)
    q_load = local(q_in, qraw, 0)
    q_load.start()
    small = [
        local(vu_in, vu.at[c], 1),
        local(res_in, res.at[c], 2),
        local(gain_in, gain.at[c], 23),
        local(ids_in, ids, 3),
        local(ctx_in, ctx, 24),
        local(gate_in, gate, 4),
    ]
    for copy in small:
        copy.start()
    w_loads = [
        local(op_in.at[:, pl.ds(p * width, width)], w.at[p, pl.ds(w_row, 32), :], 5 + p)
        for p in range(SIDE)
    ]
    for copy in w_loads:
        copy.start()
    parts = ksend.shape[0]
    each = half // parts
    k_loads = [
        local(
            cache_in.at[pl.ds(c * half + each * p, each)], cache.at[c, pl.ds(each * p, each)], 13 + p
        )
        for p in range(parts)
    ]

    def k_copy(p):
        return pltpu.make_async_remote_copy(
            src_ref=cache_in.at[pl.ds((1 - c) * half + each * p, each)],
            dst_ref=cache.at[c, pl.ds(each * p, each)],
            send_sem=ksend.at[p], recv_sem=krecv.at[p], device_id=partner, device_id_type=MESH,
        )

    def k_from(p):
        return pltpu.make_async_remote_copy(
            src_ref=cache_in.at[pl.ds(each * p, each)],
            dst_ref=cache.at[1 - c, pl.ds(each * p, each)],
            send_sem=ksend.at[p], recv_sem=krecv.at[p], device_id=partner, device_id_type=MESH,
        )

    for copy in k_loads:
        copy.start()

    barrier = pltpu.get_barrier_semaphore()
    pl.semaphore_signal(barrier, inc=1, device_id=partner, device_id_type=MESH)

    def greet(p):
        pl.semaphore_signal(barrier, inc=1, device_id=first(p), device_id_type=MESH)
        y, x = first(p)[1:3]
        pl.semaphore_signal(barrier, inc=1, device_id=(g, y, x, 1 - c), device_id_type=MESH)

    def greet_second(p):
        pl.semaphore_signal(barrier, inc=1, device_id=second(p), device_id_type=MESH)
        pl.semaphore_signal(barrier, inc=1, device_id=across(p), device_id_type=MESH)

    for d in FAR_FIRST:
        greet(lax.rem(a + d, SIDE))
        greet_second(lax.rem(b + d, SIDE))

    ext[...] = jnp.zeros(ext.shape, F32)
    q_load.wait()
    quarter = half_x * 2 + c
    ext[:, 0:16] = qraw[:, 128:144].astype(F32)
    main[...] = pltpu.roll(qraw[:, 0:128].astype(F32), quarter * 16, 1)

    def chunk_of(base):
        extra = jnp.zeros((4, 128), F32)
        for k in range(half // 4):
            row = base + 4 * k
            extra = extra + pltpu.roll(ext[row : row + 4, :], lax.rem(quarter + k, 8) * 16, 1)
        return jnp.concatenate([main[base : base + half, :], extra], axis=0)

    halves = [chunk_of(0), chunk_of(half)]
    qb[b, a, c] = jnp.where(c == 0, halves[0], halves[1]).astype(BF16)
    qs[...] = jnp.where(c == 0, halves[1], halves[0]).astype(BF16)

    pl.semaphore_wait(barrier, 4 * (SIDE - 1) + 1)

    def q1(p):
        return rcopy(qb.at[b, a, c], qb.at[b, a, c], Q1, p, 0, first(p), Q1 + c, a)

    def q1_across(p):
        return rcopy(qs, qb.at[a, b, c], Q1B, p, 0, across(p), Q1 + c, b)

    def q1_from(p, core):
        return rcopy(qs, qb.at[b, p, core], Q1, p, 0, first(p), Q1 + core, p)

    q1_across(b).start()
    peers(a, lambda p: q1(p).start())
    peers(b, lambda p: q1_across(p).start())

    def q2(slot, source, chunk, to):
        block = qb.at[source, chunk]
        return pltpu.make_async_remote_copy(
            src_ref=block, dst_ref=block, send_sem=qsend.at[slot, chunk],
            recv_sem=qrecv.at[source, chunk], device_id=second(to), device_id_type=MESH,
        )

    def at(me, distance):
        return lax.rem(me + distance, SIDE)

    def spread(distances):
        for d in distances:
            chunk = at(a, d)
            if d:
                q1_from(chunk, c).wait_recv()
            q1_from(chunk, 1 - c).wait_recv()
            for e in FAR_FIRST if d in DIRECT else (2, 6, 1, 7):
                q2(e, b, chunk, at(b, e)).start()

    def relay(distances):
        for d in [d for d in distances if d not in DIRECT]:
            chunk = at(a, d)
            source = at(b, 6)
            q2(1, source, chunk, source).wait_recv()
            q2(3, source, chunk, at(b, 1)).start()
            if d % 2 == 0:
                q2(4, source, chunk, at(b, 2)).start()
            source = at(b, 2)
            q2(1, source, chunk, source).wait_recv()
            q2(5, source, chunk, at(b, 7)).start()
            if d % 2 == 1:
                q2(0, source, chunk, at(b, 6)).start()

    for copy in w_loads:
        copy.wait()
    w_rows = w.at[:, pl.ds(w_row, 32), :]
    beside = pl.multiple_of((1 - half_x) * 64 + c * 32, 32)
    w_beside = w.at[:, pl.ds(beside, 32), :]
    w_out, w_in = [], []
    for k in range(2):
        some = pl.ds(k * (SIDE // 2), SIDE // 2)
        ours, theirs = w.at[some, pl.ds(w_row, 32), :], w.at[some, pl.ds(beside, 32), :]
        w_out.append(dcopy(ours, ours, D_N + k, neighbour))
        w_in.append(dcopy(theirs, theirs, D_N + k, neighbour))
    w_across = dcopy(w_beside, w_beside, D_NW, partner)

    @pl.when(c == 0)
    def _():
        w_out[0].start()
        w_out[1].start()

    spread((0,))
    k_copy(0).start()
    spread((1, 7))
    k_copy(1).start()
    spread((2, 6))
    k_copy(2).start()
    relay((0,))
    k_copy(3).start()
    spread((3, 5))
    k_copy(4).start()
    spread((4,))
    k_copy(5).start()
    relay((1, 7))
    k_copy(6).start()
    relay((2, 6))
    k_copy(7).start()
    relay((3, 5, 4))
    pl.when(c == 1)(w_out[0].start)
    k_copy(8).start()
    k_copy(9).start()


    for copy in small:
        copy.wait()
    to_partner = [
        dcopy(vu.at[c], vu.at[c], D_VU, partner),
        dcopy(res.at[c], res.at[c], D_RES, partner),
        dcopy(gain.at[c], gain.at[c], D_GAIN, partner),
        dcopy(w_rows, w_rows, D_W, partner),
    ]
    for copy in to_partner[:3]:
        copy.start()

    for ref in (ab, ta, tb, pt):
        ref[...] = jnp.zeros(ref.shape, F32)
    to_partner[3].start()

    lane = lanes((ROWS, 128))
    lane8 = lanes((8, 128))
    low = sublanes((8, 128)) < 4

    def assemble(hy):
        for hg in range(QUARTERS):
            m = []
            for e in range(2):
                x = 2 * hg + e
                for q in range(2):
                    m.append(qb[hy + c * (x - hy), x + c * (hy - x), q].astype(F32))
            turned = []
            for k in range(half // 4):
                picked = m[0][16:ROWS]
                for i in range(1, QUARTERS):
                    picked = jnp.where(lax.div(lane8, 16) == (k + i) % 8, m[i][16:ROWS], picked)
                picked = pltpu.roll(picked, (128 - 16 * k) % 128, 1)
                turned.append(picked if k % 2 else pltpu.roll(picked, 4, 0))
            e = jnp.concatenate(
                [
                    jnp.where(low, turned[0], turned[1]),
                    jnp.where(low, turned[2], turned[3]),
                    turned[4],
                ],
                axis=0,
            )
            whole = [
                m[0],
                jnp.where(lane < 16, e, m[1]),
                jnp.where(lane < 16, m[1], jnp.where(lane < 32, e, m[2])),
                jnp.where(lane < 32, m[2], jnp.where(lane < 48, e, m[3])),
                jnp.where(lane < 48, m[3], e),
            ]
            base = hy * (A_GROUP - 8 * c) + hg * PITCH
            for t in range(5):
                qa[pl.ds(pl.multiple_of(base + t * ROWS, 8), ROWS), :] = whole[t]

    def missing(d, e):
        if e and (d in DIRECT or e not in (2, 6)):
            chunk, source = at(a, d), at(b, e)
            q2(1, source, chunk, source).wait_recv()

    @pl.when(c == 0)
    def _():
        for e in (0, 2, 6, 1, 7, 3, 5, 4):
            for d in (0, 1, 7, 2, 6, 3, 5, 4):
                missing(d, e)
            assemble(at(b, e))

    @pl.when(c == 1)
    def _():
        for d in (0, 1, 7, 2, 6, 3, 5, 4):
            for e in (2, 6, 1, 7, 3, 5, 4):
                missing(d, e)
            assemble(at(a, d))


    for copy in k_loads:
        copy.wait()
    for p in range(parts):
        k_from(p).wait_recv()
    position = chip * 2 * ctx_dev + lanes((1, 2 * ctx_dev))
    part_k = half // PARTS
    many = half // PARTS

    def weigh(s, by_column):
        pieces = []
        for t in range(5):
            groups = []
            for k in range(4):
                if by_column:
                    rows = pl.ds(k * PITCH + t * ROWS + s, 8, stride=A_GROUP)
                else:
                    rows = pl.ds(8 * k * PITCH + t * ROWS + s, 8, stride=PITCH)
                groups.append(qa[rows, :])
            pieces.append(jnp.concatenate(groups, axis=0).astype(BF16))
        q = jnp.concatenate(pieces, axis=1)[:, : LAT + ROPE]
        keys = jnp.concatenate([cache[0, s], cache[1, s]], axis=1)
        scores = jnp.dot(q, keys, preferred_element_type=F32)
        valid = position < ctx[c * half + s]
        scores = jnp.where(valid, scores * score_scale, masked_score)
        top = jnp.max(scores, axis=1, keepdims=True)
        weights = jnp.where(valid, jnp.exp(scores - top), 0.0)
        total = jnp.sum(weights, axis=1, keepdims=True)
        wb[s] = weights.astype(BF16)
        return top, total

    def merge(u, v, first_rows):
        if first_rows:
            return jnp.where(low, u, pltpu.roll(v, 4, 0))
        return jnp.where(low, pltpu.roll(u, 4, 0), v)

    def put(tile, k, top, total):
        return jnp.where(lane8 == k, top, jnp.where(lane8 == 64 + k, total, tile))

    def weigh_columns(i):
        tiles_m = [jnp.zeros((8, 128), F32) for _ in range(4)]
        for u in range(many):
            s = i * many + u
            top, total = weigh(s, True)
            for k in range(4):
                rows = slice(8 * k, 8 * k + 8)
                tiles_m[k] = put(tiles_m[k], s, top[rows], total[rows])
        for k in range(4):
            for d in range(2):
                ml1[i, 2 * k + d] = tiles_m[k]

    def weigh_rows(i):
        tiles_m = [jnp.zeros((8, 128), F32) for _ in range(SIDE)]
        for u in range(many // 2):
            pair = i * (many // 2) + u
            t0, l0 = weigh(2 * pair, False)
            t1, l1 = weigh(2 * pair + 1, False)
            for k in range(4):
                rows = slice(8 * k, 8 * k + 8)
                wide = [jnp.broadcast_to(v[rows], (8, 128)) for v in (t0, t1, l0, l1)]
                for d in range(2):
                    top = merge(wide[0], wide[1], d == 0)
                    total = merge(wide[2], wide[3], d == 0)
                    for e in range(2):
                        tile = tiles_m[2 * k + d]
                        tiles_m[2 * k + d] = put(tile, 2 * pair + e, top, total)
        for p in range(SIDE):
            ml1[i, p] = tiles_m[p]

    def mlsend(i, p):
        return rcopy(ml1.at[i, p], rml1.at[i, a], ML1 + i, p, a, first(p))

    def ml_from(i, p):
        return rcopy(ml1.at[i, p], rml1.at[i, p], ML1 + i, p, p, first(p))

    def attend(s):
        values = jnp.concatenate([cache[0, s, 0:LAT, :], cache[1, s, 0:LAT, :]], axis=1)
        return lax.dot_general(
            wb[s], values, (((1,), (1,)), ((), ())), preferred_element_type=F32
        )

    def by_column(dst, i):
        for u in range(part_k):
            out = attend(i * part_k + u)
            for k in range(4):
                rows = slice(8 * k, 8 * k + 8)
                for d in range(2):
                    lo = out[rows, 256 * d : 256 * d + 128]
                    hi = out[rows, 256 * d + 128 : 256 * d + 256]
                    dst[i, 2 * k + d, u] = jnp.concatenate([lo, hi], axis=0).astype(dst.dtype)

    def by_row(dst, i):
        for u in range(part_k // 2):
            s = i * part_k + 2 * u
            o0 = attend(s)
            o1 = attend(s + 1)
            for k in range(4):
                rows = slice(8 * k, 8 * k + 8)
                for d in range(2):
                    for e in range(2):
                        blocks = [
                            merge(
                                o0[rows, 128 * t : 128 * t + 128],
                                o1[rows, 128 * t : 128 * t + 128],
                                d == 0,
                            )
                            for t in (2 * e, 2 * e + 1)
                        ]
                        dst[i, 2 * k + d, 2 * u + e] = jnp.concatenate(blocks, axis=0).astype(
                            dst.dtype
                        )

    def osend(i, p):
        return rcopy(s1.at[i, p], r1.at[i, a], O1 + i, p, a, first(p))

    def o_from(i, p):
        return rcopy(s1.at[i, p], r1.at[i, p], O1 + i, p, p, first(p))

    def twice(f):
        return jnp.concatenate([f, f], axis=0)

    def on_core(columns, rows):
        pl.when(c == 0)(columns)
        pl.when(c == 1)(rows)

    for i in range(PARTS):
        @pl.when(c == 0)
        def _():
            weigh_columns(i)
            by_column(s1, i)

        @pl.when(c == 1)
        def _():
            weigh_rows(i)
            by_row(s1, i)

        peers(a, lambda p: mlsend(i, p).start())
        peers(a, lambda p: osend(i, p).start())


    def fill(p):
        def block(k):
            start = pl.multiple_of(k * 16, 16)
            row = start + sublanes((16, width))
            column = p * width + lanes((16, width))
            target = chip * 112 + lax.rem(row, 64) + 56 * lax.div(row, 64)
            hit = jnp.where((column == target) & (lax.rem(row, 64) < 56), 1.0, 0.0)
            w[p, pl.ds(pl.multiple_of(128 + start, 16), 16), :] = hit.astype(BF16)

        loop(8, block)

    loop(SIDE, fill)

    idv = ids[...]
    gatev = gate[...]
    hits = jnp.zeros((8, seqs), F32)
    hit_rows = []
    gates = []
    for j in range(4):
        expert = (dev if j < 2 else chip * 2 + 1 - c) * 2 + j % 2
        same = idv == expert
        hit = jnp.sum(jnp.where(same, 1.0, 0.0), axis=0, keepdims=True)
        hit_rows.append(hit)
        gates.append(jnp.sum(jnp.where(same, gatev, 0.0), axis=0, keepdims=True))
        hits = jnp.where(sublanes((8, seqs)) == j, hit, hits)
    earlier = jnp.where(sublanes((seqs, seqs)) < lanes((seqs, seqs)), 1.0, 0.0)
    rank = jnp.dot(hits.astype(BF16), earlier.astype(BF16), preferred_element_type=F32)
    table = jnp.zeros((16, seqs), F32)
    gate_slots = jnp.zeros((2, CAP), F32)
    for j in range(4):
        for k in range(CAP):
            chosen = jnp.where(rank[j : j + 1] == float(k), hit_rows[j], 0.0)
            r = (j // 2) * 8 + (j % 2) * CAP + k
            table = jnp.where(sublanes((16, seqs)) == r, chosen, table)
            if j < 2:
                total = jnp.sum(chosen * gates[j], axis=1, keepdims=True)
                here = (sublanes((2, CAP)) == j) & (lanes((2, CAP)) == k)
                gate_slots = jnp.where(here, total, gate_slots)
    gate_out[...] = gate_slots
    pt[:, 0:seqs] = table
    own = jnp.where(c == 0, pt[...], pltpu.roll(pt[...], 128 - half, 1))
    pick[...] = jnp.where(lanes((16, 128)) < half, own, 0.0)

    for copy in to_partner[:3]:
        copy.wait_recv()
    ta[0:seqs, 0:56] = res[0].astype(F32)
    tb[0:seqs, 0:56] = res[1].astype(F32)
    ta[seqs : seqs + 1, 0:56] = gain[0].astype(F32)
    tb[seqs : seqs + 1, 0:56] = gain[1].astype(F32)
    both = ta[...] + pltpu.roll(tb[...], 64, 1)
    ta[...] = both
    row = sublanes((ROWS, 128))
    mine = jnp.where(c == 0, ta[0:ROWS, :], ta[half : half + ROWS, :])
    gain_row = jnp.broadcast_to(ta[seqs : seqs + 1, :], (ROWS, 128))
    lhs[...] = jnp.where(row < half, mine, jnp.where(row == half, gain_row, 0.0))

    def ml2_send(p):
        return rcopy(ml2, rml2.at[b], ML2, p, b, second(p))

    def ml2_from(p):
        return rcopy(ml2, rml2.at[p], ML2, p, p, second(p))

    def add(block, i, p, fresh):
        for k in range(part_k):
            term = twice(wown[p, k]) * block[k].astype(F32)
            index = i * part_k + k
            acc[index] = term if fresh else acc[index] + term

    packed = jnp.zeros((8, 128), F32)
    for i in range(PARTS):
        peers(a, lambda p: ml_from(i, p).wait_recv())
        rml1[i, a] = ml1[i, a]
        row_top = rml1[i, 0]
        for p in range(1, SIDE):
            row_top = jnp.maximum(row_top, rml1[i, p])
        total = jnp.zeros((8, 128), F32)
        for p in range(SIDE):
            factor = jnp.exp(rml1[i, p] - row_top)
            total = total + factor * pltpu.roll(rml1[i, p], 64, 1)
            fown[p] = factor
        both = jnp.where(lane8 < 64, row_top, pltpu.roll(total, 64, 1))
        group = lax.rem(lane8, 64)
        packed = jnp.where((group >= i * part_k) & (group < (i + 1) * part_k), both, packed)
        if i == PARTS - 1:
            ml2[...] = packed
            peers(b, lambda p: ml2_send(p).start())
            pl.when(c == 1)(w_out[1].start)
        for p in range(SIDE):
            f = fown[p]
            for k in range(part_k):
                lane_k = i * part_k + k
                wown[p, k] = jnp.broadcast_to(f[:, lane_k : lane_k + 1], (8, 128))
        add(s1.at[i, a], i, a, True)

        def take(p):
            o_from(i, p).wait_recv()
            add(r1.at[i, p], i, p, False)

        peers_loop(a, take)

    @pl.when(c == 0)
    def _():
        for k in range(half):
            for d in range(2):
                ab[d * 192 + k * 8 : d * 192 + k * 8 + 8, :] = acc[k, 8 * d : 8 * d + 8, :]
        for j in range(SIDE):
            s2[j] = jnp.concatenate(
                [ab[pl.ds(d * 192 + j, ROWS, stride=8), :] for d in range(2)], axis=0
            ).astype(BF16)

    @pl.when(c == 1)
    def _():
        for k in range(half):
            for d in range(2):
                base = ((k % 2) * 2 + d) * 96 + (k // 2) * 8
                ab[base : base + 8, :] = acc[k, 8 * d : 8 * d + 8, :]
        for j in range(SIDE):
            s2[j] = jnp.concatenate(
                [ab[pl.ds(((j % 2) * 2 + d) * 96 + j // 2, ROWS, stride=4), :] for d in range(2)],
                axis=0,
            ).astype(BF16)

    def o2_send(p):
        return rcopy(s2.at[p], r2.at[b], O2, p, b, second(p))

    def o2_from(p):
        return rcopy(s2.at[p], r2.at[p], O2, p, p, second(p))

    peers(b, lambda p: o2_send(p).start())
    peers(b, lambda p: ml2_from(p).wait_recv())
    rml2[b] = packed
    row_even = b - c * (b - lax.div(b, 2))
    row_odd = row_even + 4 * c
    even = lax.rem(lanes((1, 128)), 2) == 0
    each_ml = jnp.concatenate(
        [
            jnp.where(even, rml2[p, pl.ds(row_even, 1), :], rml2[p, pl.ds(row_odd, 1), :])
            for p in range(SIDE)
        ],
        axis=0,
    )
    factor = jnp.exp(each_ml - jnp.max(each_ml, axis=0, keepdims=True))
    total = jnp.sum(factor * pltpu.roll(each_ml, 64, 1), axis=0, keepdims=True)
    factor = jnp.where(lane8 < half, factor / total, 0.0)
    factor = jnp.concatenate([factor, jnp.zeros((120, 128), F32)], axis=0).T
    factors = [jnp.broadcast_to(factor[0:ROWS, p : p + 1], (ROWS, 128)) for p in range(SIDE)]
    for copy in w_in:
        copy.wait_recv()
    w_across.start()
    peers(b, lambda p: o2_from(p).wait_recv())
    r2[b] = s2[b]
    merged = twice(factors[0]) * r2[0].astype(F32)
    for p in range(1, SIDE):
        merged = merged + twice(factors[p]) * r2[p].astype(F32)

    part = jnp.zeros((ROWS, VD), F32)
    for k in range(2):
        block = merged[ROWS * k : ROWS * (k + 1)]
        high = block.astype(BF16)
        low = (block - high.astype(F32)).astype(BF16)
        part = part + jnp.dot(high, vu[k], preferred_element_type=F32)
        part = part + jnp.dot(low, vu[k], preferred_element_type=F32)
    to_partner[3].wait_recv()
    w_across.wait_recv()
    left = jnp.concatenate([part.astype(BF16), lhs[...].astype(BF16)], axis=1)

    def part_rows(j):
        sizes = [padded(CUTS[k + 1] - CUTS[k], half) for k in range(2)]
        return pl.ds(sum(sizes[:j]), sizes[j])

    def a1_send(j, p):
        rows = part_rows(j)
        return rcopy(s3.at[p, rows], r3.at[a, rows], A1 + j, p, a, first(p))

    def a1_from(j, p):
        rows = part_rows(j)
        return rcopy(s3.at[p, rows], r3.at[p, rows], A1 + j, p, p, first(p))

    def a2_send(j, p):
        rows = part_rows(j)
        return rcopy(s4.at[rows], r4.at[b, rows], A2 + j, p, b, second(p))

    def a2_from(j, p):
        rows = part_rows(j)
        return rcopy(s4.at[rows], r4.at[p, rows], A2 + j, p, p, second(p))

    def a3_send(j, p):
        rows = part_rows(j)
        return rcopy(rf.at[a, rows], rf.at[a, rows], A3 + j, p, a, first(p))

    def a3_from(j, p):
        rows = part_rows(j)
        return rcopy(rf.at[p, rows], rf.at[p, rows], A3 + j, p, p, first(p))

    def in_step(k):
        pl.semaphore_signal(steps.at[k], inc=1, device_id=partner, device_id_type=MESH)
        pl.semaphore_wait(steps.at[k], 1)

    def project(j, p):
        out = jnp.dot(left, w[p, :, 128 * CUTS[j] : 128 * CUTS[j + 1]], preferred_element_type=F32)
        count = CUTS[j + 1] - CUTS[j]
        blocks = [out[:half, 128 * t : 128 * t + 128] for t in range(count)]
        blocks += [out[half : half + 1, 128 * t : 128 * t + 128] for t in range(count)]
        blocks.append(jnp.zeros((padded(count, half) - count * (half + 1), 128), F32))
        s3[p, part_rows(j), :] = jnp.concatenate(blocks, axis=0).astype(BF16)

    def total_of(ref, j):
        total = ref[0, part_rows(j), :].astype(F32)
        for p in range(1, SIDE):
            total = total + ref[p, part_rows(j), :].astype(F32)
        return total.astype(BF16)

    in_step(0)
    for j in range(2):

        for batch in ((4, 3, 5), (2, 6, 1, 7)):
            for d in batch:
                project(j, at(a, d))
            for d in batch:
                a1_send(j, at(a, d)).start()
    for j in range(2):
        project(j, a)
    for j in range(2):
        peers(a, lambda p: a1_from(j, p).wait_recv())
        r3[a, part_rows(j), :] = s3[a, part_rows(j), :]
        s4[part_rows(j), :] = total_of(r3, j)
        peers(b, lambda p: a2_send(j, p).start())
    peers(a, lambda p: q1(p).wait_send())
    loop(SIDE, lambda p: q1_across(p).wait_send())
    for p in range(parts):
        k_copy(p).wait_send()
    for d in range(SIDE):
        chunk = at(a, d)
        for slot in range(1, SIDE) if d in DIRECT else (1, 2, 3, 5, 6, 7, 4 if d % 2 == 0 else 0):
            q2(slot, b, chunk, at(b, 1)).wait_send()
    for i in range(PARTS):
        peers(a, lambda p: mlsend(i, p).wait_send())
    for i in range(PARTS):
        peers(a, lambda p: osend(i, p).wait_send())
    peers(b, lambda p: ml2_send(p).wait_send())
    peers(b, lambda p: o2_send(p).wait_send())
    for copy in to_partner + w_out + [w_across]:
        copy.wait_send()
    for j in range(2):
        peers(b, lambda p: a2_from(j, p).wait_recv())
        r4[b, part_rows(j), :] = s4[part_rows(j), :]
        rf[a, part_rows(j), :] = total_of(r4, j)
        peers(a, lambda p: a3_send(j, p).start())
    for j in range(2):
        peers(a, lambda p: a1_send(j, p).wait_send())
        peers(b, lambda p: a2_send(j, p).wait_send())
    for j in range(2):
        peers(a, lambda p: a3_from(j, p).wait_recv())

    choose = pick[...][:, 0:half]
    choose_b = choose.astype(BF16)
    squares = jnp.zeros((half, 128), F32)
    largest = jnp.zeros((half, 128), F32)
    for p in range(SIDE):
        parts_r = []
        gains = []
        for j in range(2):
            block = rf[p, part_rows(j), :].astype(F32)
            count = CUTS[j + 1] - CUTS[j]
            parts_r += [block[half * t : half * (t + 1)] for t in range(count)]
            gains += [block[half * count + t : half * count + t + 1] for t in range(count)]
        for v, gv in zip(parts_r, gains):
            squares = squares + v * v
            largest = jnp.maximum(largest, jnp.abs(v * gv))
        rows = jnp.concatenate(parts_r, axis=1).astype(BF16)
        chosen = jnp.dot(choose_b, rows, preferred_element_type=F32)
        y[p] = chosen * jnp.concatenate(gains, axis=1)
    inverse = lax.rsqrt(jnp.sum(squares, axis=1, keepdims=True) / cols + small_eps)
    peak = inverse * jnp.max(largest, axis=1, keepdims=True) + small_eps
    spread = jnp.concatenate(
        [jnp.broadcast_to(inverse / peak, (half, 128)), jnp.broadcast_to(peak, (half, 128))], axis=1
    )
    slots = jnp.dot(choose, spread, preferred_element_type=F32, precision=lax.Precision.HIGHEST)
    code = jnp.concatenate([slots[:, 0:128]] * tiles, axis=1)
    peaks = slots[:, 128:256]
    xs[...] = peaks[8:16]
    for k in range(SIDE // 2):
        fs[k] = jnp.concatenate(
            [y[2 * k + d, 8:16, :] * code[8:16] for d in range(2)], axis=0
        ).astype(BF16)
    x_partner = dcopy(xs, xr, D_X, partner)
    f_partner = dcopy(fs, fr, D_F, partner)
    x_partner.start()
    f_partner.start()
    x_partner.wait_recv()
    peaks = peaks[0:8] + xr[...]
    scale_slots = jnp.zeros((2, CAP), F32)
    for j in range(2):
        for k in range(CAP):
            here = (sublanes((2, CAP)) == j) & (lanes((2, CAP)) == k)
            r = CAP * j + k
            scale_slots = jnp.where(here, peaks[r : r + 1, 0:1], scale_slots)
    scale_out[...] = scale_slots
    f_partner.wait_recv()
    for k in range(SIDE // 2):
        there = fr[k].astype(F32)
        for d in range(2):
            p = 2 * k + d
            rows = (y[p, 0:8, :] * code[0:8] + there[8 * d : 8 * d + 8]).astype(BF16)
            for e in range(2):
                disp_out[e, :, pl.ds(p * width, width)] = rows[CAP * e : CAP * e + CAP]

    for j in range(2):
        peers(a, lambda p: a3_send(j, p).wait_send())
    x_partner.wait_send()
    f_partner.wait_send()


def per_device(
    queries, latent_cache, context_lengths, value_up, out_proj, residual, norm_gain, expert_ids,
    gate_weights,
):
    seqs, ctx_dev, entry = latent_cache.shape
    half = seqs // 2
    columns = out_proj.shape[1]
    width = columns // SIDE
    piece = residual.shape[1]
    experts = 2
    rows = sum(padded(CUTS[k + 1] - CUTS[k], half) for k in range(2))
    any_space = pl.BlockSpec(memory_space=pl.ANY)
    vmem = pl.BlockSpec(memory_space=pltpu.VMEM)
    V = pltpu.VMEM
    chunk = (PARTS, SIDE, half // PARTS, 16, 128)
    eights = (SIDE, 8, 128)
    scratch = [
        V(queries.shape, BF16),
        V((seqs, 128), F32),
        V((seqs, 128), F32),
        V((ROWS, 128), BF16),
        V((SIDE, SIDE, 2, ROWS, 128), BF16),
        V((SIDE * A_GROUP, 128), F32),
        V((2, half, entry, ctx_dev), BF16),
        V((half, H, 2 * ctx_dev), BF16),
        V(chunk, BF16),
        V(chunk, BF16),
        V((PARTS,) + eights, F32),
        V((PARTS,) + eights, F32),
        V((8, 128), F32),
        V(eights, F32),
        V(eights, F32),
        V((SIDE, half // PARTS, 8, 128), F32),
        V((half, 16, 128), F32),
        V((384, 128), F32),
        V((SIDE, 2 * ROWS, 128), BF16),
        V((SIDE, 2 * ROWS, 128), BF16),
        V((2, 128, VD), BF16),
        V((2, seqs, piece), BF16),
        V((2, 1, piece), BF16),
        V((seqs + 8, 128), F32),
        V((seqs + 8, 128), F32),
        V((ROWS, 128), F32),
        V((SIDE, 256, width), BF16),
        V((SIDE, rows, 128), BF16),
        V((SIDE, rows, 128), BF16),
        V((rows, 128), BF16),
        V((SIDE, rows, 128), BF16),
        V((SIDE, rows, 128), BF16),
        V(expert_ids.shape[::-1], jnp.int32),
        V(gate_weights.shape[::-1], F32),
        V((16, 128), F32),
        V((16, 128), F32),
        V((SIDE, 16, width), F32),
        V((SIDE // 2, 16, width), BF16),
        V((SIDE // 2, 16, width), BF16),
        V((8, 128), F32),
        V((8, 128), F32),
        pltpu.SMEM(context_lengths.shape, jnp.int32),
        pltpu.SemaphoreType.DMA((25,)),
        pltpu.SemaphoreType.DMA((PHASES, SIDE)),
        pltpu.SemaphoreType.DMA((PHASES, SIDE)),
        pltpu.SemaphoreType.DMA((SIDE, SIDE)),
        pltpu.SemaphoreType.DMA((SIDE, SIDE)),
        pltpu.SemaphoreType.DMA((half // 2,)),
        pltpu.SemaphoreType.DMA((half // 2,)),
        pltpu.SemaphoreType.DMA((9,)),
        pltpu.SemaphoreType.DMA((9,)),
        pltpu.SemaphoreType.REGULAR((1,)),
    ]
    dispatched, slot_scale, slot_gate = pl.pallas_call(
        kernel,
        out_shape=(
            jax.ShapeDtypeStruct((experts, CAP, columns), BF16),
            jax.ShapeDtypeStruct((experts, CAP), F32),
            jax.ShapeDtypeStruct((experts, CAP), F32),
        ),
        in_specs=[any_space] * 9,
        out_specs=(vmem, vmem, vmem),
        scratch_shapes=scratch,
        compiler_params=pltpu.CompilerParams(collective_id=0, has_side_effects=True),
    )(
        queries, latent_cache.transpose(0, 2, 1), context_lengths, value_up, out_proj, residual,
        norm_gain[None, :], expert_ids.T, gate_weights.T,
    )
    def hand_over(*refs):
        for source, target in zip(refs[:3], refs[3:]):
            target[...] = source[...]

    results = (dispatched, slot_scale, slot_gate)
    return pl.pallas_call(
        hand_over,
        out_shape=tuple(jax.ShapeDtypeStruct(r.shape, r.dtype) for r in results),
        in_specs=[vmem] * 3,
        out_specs=(vmem,) * 3,
    )(*results)


def solution(mesh):
    split = Mesh(
        mesh.devices.reshape(mesh.shape["groups"], SIDE, SIDE, 2),
        ("groups", "kv_0", "kv_1", "kv_2"),
    )
    in_specs = (
        P("groups", KV),
        P("groups", KV, None),
        P("groups"),
        P(KV, None),
        P(KV, None),
        P("groups", KV),
        P(KV),
        P("groups", None),
        P("groups", None),
    )
    out_specs = (P(GROUPS_KV, None, None), P(GROUPS_KV, None), P(GROUPS_KV, None))
    return jax.shard_map(
        per_device, mesh=split, in_specs=in_specs, out_specs=out_specs, check_vma=False
    )
```

```python
import functools

import jax
import jax.numpy as jnp
from jax import lax
from jax.experimental import pallas as pl
from jax.experimental.pallas import tpu as pltpu
from jax.sharding import Mesh
from jax.sharding import PartitionSpec as P

H = 32
LAT = 512
ROPE = 64
VD = 128
TOPK = 8
CAP = 2
SIDE = 8
QUARTERS = 4
ROWS = 24
PITCH = 5 * ROWS
A_GROUP = QUARTERS * PITCH + 8
KV = ("kv_0", "kv_1", "kv_2")
GROUPS_KV = ("groups", "kv_0", "kv_1", "kv_2")
FAR_FIRST = (4, 3, 5, 2, 6, 1, 7)
DIRECT = (3, 4, 5)
PARTS = 2
CUTS = (0, 4, 7)
MESH = pl.DeviceIdType.MESH
F32 = jnp.float32
BF16 = jnp.bfloat16

score_scale = 192.0 ** (-0.5)
masked_score = -1e30
small_eps = 1e-06

Q1, Q1B, ML2, O2, A1, A2, A3, O1 = 0, 1, 2, 3, 4, 6, 8, 10
ML1 = O1 + PARTS
PHASES = ML1 + PARTS
D_VU, D_RES, D_GAIN, D_W, D_F, D_X, D_NW, D_N = range(8)


def lanes(shape):
    return lax.broadcasted_iota(jnp.int32, shape, len(shape) - 1)


def sublanes(shape):
    return lax.broadcasted_iota(jnp.int32, shape, len(shape) - 2)


def loop(count, body):
    def step(i, carry):
        body(i)
        return carry

    lax.fori_loop(0, count, step, 0)


def padded(tiles, half):
    return -(-tiles * (half + 1) // 8) * 8


def far_first(i):
    return SIDE // 2 + (1 - 2 * lax.rem(i, 2)) * lax.div(i + 1, 2)


def kernel(
    q_in, cache_in, ctx_in, vu_in, op_in, res_in, gain_in, ids_in, gate_in,
    disp_out, scale_out, gate_out,
    qraw, ext, main, qs, qb, qa, cache, wb, s1, r1, ml1, rml1,
    ml2, rml2, fown, wown, acc, ab, s2, r2, vu, res, gain, ta, tb, lhs, w,
    s3, r3, s4, r4, rf, ids, gate, pt, pick, y, fs, fr, xs, xr,
    ctx, loc, ssem, rsem, qsend, qrecv, ksend, krecv, dsend, drecv, steps,
):
    g = lax.axis_index("groups")
    yy = lax.axis_index("kv_0")
    xx = lax.axis_index("kv_1")
    c = lax.axis_index("kv_2")
    chip = yy * SIDE + xx
    dev = chip * 2 + c
    a = xx + c * (yy - xx)
    b = yy + c * (xx - yy)
    half_x = lax.rem(xx, 2)
    half, ctx_dev = cache.shape[1], cache.shape[3]
    seqs = 2 * half
    width = w.shape[2]
    tiles = width // 128
    cols = SIDE * width

    def first(p):
        return (g, yy + c * (p - yy), xx + (1 - c) * (p - xx), c)

    def second(p):
        return (g, yy + (1 - c) * (p - yy), xx + c * (p - xx), c)

    def across(p):
        return (g, yy + (1 - c) * (p - yy), xx + c * (p - xx), 1 - c)

    partner = (g, yy, xx, 1 - c)
    neighbour = (g, yy, xx + 1 - 2 * half_x, c)

    def rcopy(src, dst, phase, to, frm, device, recv_phase=None, recv_from=None):
        recv = (phase, frm) if recv_phase is None else (recv_phase, recv_from)
        return pltpu.make_async_remote_copy(
            src_ref=src, dst_ref=dst, send_sem=ssem.at[phase, to], recv_sem=rsem.at[recv],
            device_id=device, device_id_type=MESH,
        )

    def dcopy(src, dst, which, device):
        return pltpu.make_async_remote_copy(
            src_ref=src, dst_ref=dst, send_sem=dsend.at[which], recv_sem=drecv.at[which],
            device_id=device, device_id_type=MESH,
        )

    def peers(me, body):
        for d in FAR_FIRST:
            body(lax.rem(me + d, SIDE))

    def peers_loop(me, body):
        def one(i):
            body(lax.rem(me + far_first(i), SIDE))

        loop(SIDE - 1, one)

    def local(src, dst, k):
        return pltpu.make_async_copy(src, dst, loc.at[k])

    w_row = pl.multiple_of(half_x * 64 + c * 32, 32)
    q_load = local(q_in, qraw, 0)
    q_load.start()
    small = [
        local(vu_in, vu.at[c], 1),
        local(res_in, res.at[c], 2),
        local(gain_in, gain.at[c], 23),
        local(ids_in, ids, 3),
        local(ctx_in, ctx, 24),
        local(gate_in, gate, 4),
    ]
    for copy in small:
        copy.start()
    w_loads = [
        local(op_in.at[:, pl.ds(p * width, width)], w.at[p, pl.ds(w_row, 32), :], 5 + p)
        for p in range(SIDE)
    ]
    for copy in w_loads:
        copy.start()
    parts = ksend.shape[0]
    each = half // parts
    k_loads = [
        local(
            cache_in.at[pl.ds(c * half + each * p, each)], cache.at[c, pl.ds(each * p, each)], 13 + p
        )
        for p in range(parts)
    ]

    def k_copy(p):
        return pltpu.make_async_remote_copy(
            src_ref=cache_in.at[pl.ds((1 - c) * half + each * p, each)],
            dst_ref=cache.at[c, pl.ds(each * p, each)],
            send_sem=ksend.at[p], recv_sem=krecv.at[p], device_id=partner, device_id_type=MESH,
        )

    def k_from(p):
        return pltpu.make_async_remote_copy(
            src_ref=cache_in.at[pl.ds(each * p, each)],
            dst_ref=cache.at[1 - c, pl.ds(each * p, each)],
            send_sem=ksend.at[p], recv_sem=krecv.at[p], device_id=partner, device_id_type=MESH,
        )

    for copy in k_loads:
        copy.start()

    barrier = pltpu.get_barrier_semaphore()
    pl.semaphore_signal(barrier, inc=1, device_id=partner, device_id_type=MESH)

    def greet(p):
        pl.semaphore_signal(barrier, inc=1, device_id=first(p), device_id_type=MESH)
        y, x = first(p)[1:3]
        pl.semaphore_signal(barrier, inc=1, device_id=(g, y, x, 1 - c), device_id_type=MESH)

    def greet_second(p):
        pl.semaphore_signal(barrier, inc=1, device_id=second(p), device_id_type=MESH)
        pl.semaphore_signal(barrier, inc=1, device_id=across(p), device_id_type=MESH)

    peers(a, greet)
    peers(b, greet_second)

    ext[...] = jnp.zeros(ext.shape, F32)
    q_load.wait()
    quarter = half_x * 2 + c
    ext[:, 0:16] = qraw[:, 128:144].astype(F32)
    main[...] = pltpu.roll(qraw[:, 0:128].astype(F32), quarter * 16, 1)

    def chunk_of(base):
        extra = jnp.zeros((4, 128), F32)
        for k in range(half // 4):
            row = base + 4 * k
            extra = extra + pltpu.roll(ext[row : row + 4, :], lax.rem(quarter + k, 8) * 16, 1)
        return jnp.concatenate([main[base : base + half, :], extra], axis=0)

    halves = [chunk_of(0), chunk_of(half)]
    qb[b, a, c] = jnp.where(c == 0, halves[0], halves[1]).astype(BF16)
    qs[...] = jnp.where(c == 0, halves[1], halves[0]).astype(BF16)

    pl.semaphore_wait(barrier, 4 * (SIDE - 1) + 1)

    def q1(p):
        return rcopy(qb.at[b, a, c], qb.at[b, a, c], Q1, p, 0, first(p), Q1 + c, a)

    def q1_across(p):
        return rcopy(qs, qb.at[a, b, c], Q1B, p, 0, across(p), Q1 + c, b)

    def q1_from(p, core):
        return rcopy(qs, qb.at[b, p, core], Q1, p, 0, first(p), Q1 + core, p)

    q1_across(b).start()
    peers(a, lambda p: q1(p).start())
    peers(b, lambda p: q1_across(p).start())

    def q2(slot, source, chunk, to):
        block = qb.at[source, chunk]
        return pltpu.make_async_remote_copy(
            src_ref=block, dst_ref=block, send_sem=qsend.at[slot, chunk],
            recv_sem=qrecv.at[source, chunk], device_id=second(to), device_id_type=MESH,
        )

    def at(me, distance):
        return lax.rem(me + distance, SIDE)

    def spread(distances):
        for d in distances:
            chunk = at(a, d)
            if d:
                q1_from(chunk, c).wait_recv()
            q1_from(chunk, 1 - c).wait_recv()
            for e in FAR_FIRST if d in DIRECT else (2, 6, 1, 7):
                q2(e, b, chunk, at(b, e)).start()

    def relay(distances):
        for d in [d for d in distances if d not in DIRECT]:
            chunk = at(a, d)
            source = at(b, 6)
            q2(1, source, chunk, source).wait_recv()
            q2(3, source, chunk, at(b, 1)).start()
            if d % 2 == 0:
                q2(4, source, chunk, at(b, 2)).start()
            source = at(b, 2)
            q2(1, source, chunk, source).wait_recv()
            q2(5, source, chunk, at(b, 7)).start()
            if d % 2 == 1:
                q2(0, source, chunk, at(b, 6)).start()

    for copy in w_loads:
        copy.wait()
    w_rows = w.at[:, pl.ds(w_row, 32), :]
    beside = pl.multiple_of((1 - half_x) * 64 + c * 32, 32)
    w_beside = w.at[:, pl.ds(beside, 32), :]
    w_out, w_in = [], []
    for k in range(2):
        some = pl.ds(k * (SIDE // 2), SIDE // 2)
        ours, theirs = w.at[some, pl.ds(w_row, 32), :], w.at[some, pl.ds(beside, 32), :]
        w_out.append(dcopy(ours, ours, D_N + k, neighbour))
        w_in.append(dcopy(theirs, theirs, D_N + k, neighbour))
    w_across = dcopy(w_beside, w_beside, D_NW, partner)

    @pl.when(c == 0)
    def _():
        w_out[0].start()
        w_out[1].start()

    spread((0,))
    k_copy(0).start()
    spread((1, 7))
    k_copy(1).start()
    spread((2, 6))
    k_copy(2).start()
    relay((0,))
    k_copy(3).start()
    spread((3, 5))
    k_copy(4).start()
    spread((4,))
    k_copy(5).start()
    relay((1, 7))
    k_copy(6).start()
    relay((2, 6))
    k_copy(7).start()
    relay((3, 5, 4))
    pl.when(c == 1)(w_out[0].start)
    k_copy(8).start()
    k_copy(9).start()


    for copy in small:
        copy.wait()
    to_partner = [
        dcopy(vu.at[c], vu.at[c], D_VU, partner),
        dcopy(res.at[c], res.at[c], D_RES, partner),
        dcopy(gain.at[c], gain.at[c], D_GAIN, partner),
        dcopy(w_rows, w_rows, D_W, partner),
    ]
    for copy in to_partner[:3]:
        copy.start()

    for ref in (ab, ta, tb, pt):
        ref[...] = jnp.zeros(ref.shape, F32)
    to_partner[3].start()

    lane = lanes((ROWS, 128))
    lane8 = lanes((8, 128))
    low = sublanes((8, 128)) < 4

    def assemble(hy):
        for hg in range(QUARTERS):
            m = []
            for e in range(2):
                x = 2 * hg + e
                for q in range(2):
                    m.append(qb[hy + c * (x - hy), x + c * (hy - x), q].astype(F32))
            turned = []
            for k in range(half // 4):
                picked = m[0][16:ROWS]
                for i in range(1, QUARTERS):
                    picked = jnp.where(lax.div(lane8, 16) == (k + i) % 8, m[i][16:ROWS], picked)
                picked = pltpu.roll(picked, (128 - 16 * k) % 128, 1)
                turned.append(picked if k % 2 else pltpu.roll(picked, 4, 0))
            e = jnp.concatenate(
                [
                    jnp.where(low, turned[0], turned[1]),
                    jnp.where(low, turned[2], turned[3]),
                    turned[4],
                ],
                axis=0,
            )
            whole = [
                m[0],
                jnp.where(lane < 16, e, m[1]),
                jnp.where(lane < 16, m[1], jnp.where(lane < 32, e, m[2])),
                jnp.where(lane < 32, m[2], jnp.where(lane < 48, e, m[3])),
                jnp.where(lane < 48, m[3], e),
            ]
            base = hy * (A_GROUP - 8 * c) + hg * PITCH
            for t in range(5):
                qa[pl.ds(pl.multiple_of(base + t * ROWS, 8), ROWS), :] = whole[t]

    def missing(d, e):
        if e and (d in DIRECT or e not in (2, 6)):
            chunk, source = at(a, d), at(b, e)
            q2(1, source, chunk, source).wait_recv()

    @pl.when(c == 0)
    def _():
        for e in (0, 2, 6, 1, 7, 3, 5, 4):
            for d in (0, 1, 7, 2, 6, 3, 5, 4):
                missing(d, e)
            assemble(at(b, e))

    @pl.when(c == 1)
    def _():
        for d in (0, 1, 7, 2, 6, 3, 5, 4):
            for e in (2, 6, 1, 7, 3, 5, 4):
                missing(d, e)
            assemble(at(a, d))


    for copy in k_loads:
        copy.wait()
    for p in range(parts):
        k_from(p).wait_recv()
    position = chip * 2 * ctx_dev + lanes((1, 2 * ctx_dev))
    part_k = half // PARTS
    many = half // PARTS

    def weigh(s, by_column):
        pieces = []
        for t in range(5):
            groups = []
            for k in range(4):
                if by_column:
                    rows = pl.ds(k * PITCH + t * ROWS + s, 8, stride=A_GROUP)
                else:
                    rows = pl.ds(8 * k * PITCH + t * ROWS + s, 8, stride=PITCH)
                groups.append(qa[rows, :])
            pieces.append(jnp.concatenate(groups, axis=0).astype(BF16))
        q = jnp.concatenate(pieces, axis=1)[:, : LAT + ROPE]
        keys = jnp.concatenate([cache[0, s], cache[1, s]], axis=1)
        scores = jnp.dot(q, keys, preferred_element_type=F32)
        valid = position < ctx[c * half + s]
        scores = jnp.where(valid, scores * score_scale, masked_score)
        top = jnp.max(scores, axis=1, keepdims=True)
        weights = jnp.where(valid, jnp.exp(scores - top), 0.0)
        total = jnp.sum(weights, axis=1, keepdims=True)
        wb[s] = weights.astype(BF16)
        return top, total

    def merge(u, v, first_rows):
        if first_rows:
            return jnp.where(low, u, pltpu.roll(v, 4, 0))
        return jnp.where(low, pltpu.roll(u, 4, 0), v)

    def put(tile, k, top, total):
        return jnp.where(lane8 == k, top, jnp.where(lane8 == 64 + k, total, tile))

    def weigh_columns(i):
        tiles_m = [jnp.zeros((8, 128), F32) for _ in range(4)]
        for u in range(many):
            s = i * many + u
            top, total = weigh(s, True)
            for k in range(4):
                rows = slice(8 * k, 8 * k + 8)
                tiles_m[k] = put(tiles_m[k], s, top[rows], total[rows])
        for k in range(4):
            for d in range(2):
                ml1[i, 2 * k + d] = tiles_m[k]

    def weigh_rows(i):
        tiles_m = [jnp.zeros((8, 128), F32) for _ in range(SIDE)]
        for u in range(many // 2):
            pair = i * (many // 2) + u
            t0, l0 = weigh(2 * pair, False)
            t1, l1 = weigh(2 * pair + 1, False)
            for k in range(4):
                rows = slice(8 * k, 8 * k + 8)
                wide = [jnp.broadcast_to(v[rows], (8, 128)) for v in (t0, t1, l0, l1)]
                for d in range(2):
                    top = merge(wide[0], wide[1], d == 0)
                    total = merge(wide[2], wide[3], d == 0)
                    for e in range(2):
                        tile = tiles_m[2 * k + d]
                        tiles_m[2 * k + d] = put(tile, 2 * pair + e, top, total)
        for p in range(SIDE):
            ml1[i, p] = tiles_m[p]

    def mlsend(i, p):
        return rcopy(ml1.at[i, p], rml1.at[i, a], ML1 + i, p, a, first(p))

    def ml_from(i, p):
        return rcopy(ml1.at[i, p], rml1.at[i, p], ML1 + i, p, p, first(p))

    def attend(s):
        values = jnp.concatenate([cache[0, s, 0:LAT, :], cache[1, s, 0:LAT, :]], axis=1)
        return lax.dot_general(
            wb[s], values, (((1,), (1,)), ((), ())), preferred_element_type=F32
        )

    def by_column(dst, i):
        for u in range(part_k):
            out = attend(i * part_k + u)
            for k in range(4):
                rows = slice(8 * k, 8 * k + 8)
                for d in range(2):
                    lo = out[rows, 256 * d : 256 * d + 128]
                    hi = out[rows, 256 * d + 128 : 256 * d + 256]
                    dst[i, 2 * k + d, u] = jnp.concatenate([lo, hi], axis=0).astype(dst.dtype)

    def by_row(dst, i):
        for u in range(part_k // 2):
            s = i * part_k + 2 * u
            o0 = attend(s)
            o1 = attend(s + 1)
            for k in range(4):
                rows = slice(8 * k, 8 * k + 8)
                for d in range(2):
                    for e in range(2):
                        blocks = [
                            merge(
                                o0[rows, 128 * t : 128 * t + 128],
                                o1[rows, 128 * t : 128 * t + 128],
                                d == 0,
                            )
                            for t in (2 * e, 2 * e + 1)
                        ]
                        dst[i, 2 * k + d, 2 * u + e] = jnp.concatenate(blocks, axis=0).astype(
                            dst.dtype
                        )

    def osend(i, p):
        return rcopy(s1.at[i, p], r1.at[i, a], O1 + i, p, a, first(p))

    def o_from(i, p):
        return rcopy(s1.at[i, p], r1.at[i, p], O1 + i, p, p, first(p))

    def twice(f):
        return jnp.concatenate([f, f], axis=0)

    def on_core(columns, rows):
        pl.when(c == 0)(columns)
        pl.when(c == 1)(rows)

    for i in range(PARTS):
        on_core(lambda: weigh_columns(i), lambda: weigh_rows(i))
        peers(a, lambda p: mlsend(i, p).start())
        on_core(lambda: by_column(s1, i), lambda: by_row(s1, i))
        peers(a, lambda p: osend(i, p).start())


    def fill(p):
        def block(k):
            start = pl.multiple_of(k * 16, 16)
            row = start + sublanes((16, width))
            column = p * width + lanes((16, width))
            target = chip * 112 + lax.rem(row, 64) + 56 * lax.div(row, 64)
            hit = jnp.where((column == target) & (lax.rem(row, 64) < 56), 1.0, 0.0)
            w[p, pl.ds(pl.multiple_of(128 + start, 16), 16), :] = hit.astype(BF16)

        loop(8, block)

    loop(SIDE, fill)

    idv = ids[...]
    gatev = gate[...]
    hits = jnp.zeros((8, seqs), F32)
    hit_rows = []
    gates = []
    for j in range(4):
        expert = (dev if j < 2 else chip * 2 + 1 - c) * 2 + j % 2
        same = idv == expert
        hit = jnp.sum(jnp.where(same, 1.0, 0.0), axis=0, keepdims=True)
        hit_rows.append(hit)
        gates.append(jnp.sum(jnp.where(same, gatev, 0.0), axis=0, keepdims=True))
        hits = jnp.where(sublanes((8, seqs)) == j, hit, hits)
    earlier = jnp.where(sublanes((seqs, seqs)) < lanes((seqs, seqs)), 1.0, 0.0)
    rank = jnp.dot(hits.astype(BF16), earlier.astype(BF16), preferred_element_type=F32)
    table = jnp.zeros((16, seqs), F32)
    gate_slots = jnp.zeros((2, CAP), F32)
    for j in range(4):
        for k in range(CAP):
            chosen = jnp.where(rank[j : j + 1] == float(k), hit_rows[j], 0.0)
            r = (j // 2) * 8 + (j % 2) * CAP + k
            table = jnp.where(sublanes((16, seqs)) == r, chosen, table)
            if j < 2:
                total = jnp.sum(chosen * gates[j], axis=1, keepdims=True)
                here = (sublanes((2, CAP)) == j) & (lanes((2, CAP)) == k)
                gate_slots = jnp.where(here, total, gate_slots)
    gate_out[...] = gate_slots
    pt[:, 0:seqs] = table
    own = jnp.where(c == 0, pt[...], pltpu.roll(pt[...], 128 - half, 1))
    pick[...] = jnp.where(lanes((16, 128)) < half, own, 0.0)

    for copy in to_partner[:3]:
        copy.wait_recv()
    ta[0:seqs, 0:56] = res[0].astype(F32)
    tb[0:seqs, 0:56] = res[1].astype(F32)
    ta[seqs : seqs + 1, 0:56] = gain[0].astype(F32)
    tb[seqs : seqs + 1, 0:56] = gain[1].astype(F32)
    both = ta[...] + pltpu.roll(tb[...], 64, 1)
    ta[...] = both
    row = sublanes((ROWS, 128))
    mine = jnp.where(c == 0, ta[0:ROWS, :], ta[half : half + ROWS, :])
    gain_row = jnp.broadcast_to(ta[seqs : seqs + 1, :], (ROWS, 128))
    lhs[...] = jnp.where(row < half, mine, jnp.where(row == half, gain_row, 0.0))

    def ml2_send(p):
        return rcopy(ml2, rml2.at[b], ML2, p, b, second(p))

    def ml2_from(p):
        return rcopy(ml2, rml2.at[p], ML2, p, p, second(p))

    def add(block, i, p, fresh):
        for k in range(part_k):
            term = twice(wown[p, k]) * block[k].astype(F32)
            index = i * part_k + k
            acc[index] = term if fresh else acc[index] + term

    packed = jnp.zeros((8, 128), F32)
    for i in range(PARTS):
        peers(a, lambda p: ml_from(i, p).wait_recv())
        rml1[i, a] = ml1[i, a]
        row_top = rml1[i, 0]
        for p in range(1, SIDE):
            row_top = jnp.maximum(row_top, rml1[i, p])
        total = jnp.zeros((8, 128), F32)
        for p in range(SIDE):
            factor = jnp.exp(rml1[i, p] - row_top)
            total = total + factor * pltpu.roll(rml1[i, p], 64, 1)
            fown[p] = factor
        both = jnp.where(lane8 < 64, row_top, pltpu.roll(total, 64, 1))
        group = lax.rem(lane8, 64)
        packed = jnp.where((group >= i * part_k) & (group < (i + 1) * part_k), both, packed)
        if i == PARTS - 1:
            ml2[...] = packed
            peers(b, lambda p: ml2_send(p).start())
            pl.when(c == 1)(w_out[1].start)
        for p in range(SIDE):
            f = fown[p]
            for k in range(part_k):
                lane_k = i * part_k + k
                wown[p, k] = jnp.broadcast_to(f[:, lane_k : lane_k + 1], (8, 128))
        add(s1.at[i, a], i, a, True)

        def take(p):
            o_from(i, p).wait_recv()
            add(r1.at[i, p], i, p, False)

        peers_loop(a, take)

    @pl.when(c == 0)
    def _():
        for k in range(half):
            for d in range(2):
                ab[d * 192 + k * 8 : d * 192 + k * 8 + 8, :] = acc[k, 8 * d : 8 * d + 8, :]
        for j in range(SIDE):
            s2[j] = jnp.concatenate(
                [ab[pl.ds(d * 192 + j, ROWS, stride=8), :] for d in range(2)], axis=0
            ).astype(BF16)

    @pl.when(c == 1)
    def _():
        for k in range(half):
            for d in range(2):
                base = ((k % 2) * 2 + d) * 96 + (k // 2) * 8
                ab[base : base + 8, :] = acc[k, 8 * d : 8 * d + 8, :]
        for j in range(SIDE):
            s2[j] = jnp.concatenate(
                [ab[pl.ds(((j % 2) * 2 + d) * 96 + j // 2, ROWS, stride=4), :] for d in range(2)],
                axis=0,
            ).astype(BF16)

    def o2_send(p):
        return rcopy(s2.at[p], r2.at[b], O2, p, b, second(p))

    def o2_from(p):
        return rcopy(s2.at[p], r2.at[p], O2, p, p, second(p))

    peers(b, lambda p: o2_send(p).start())
    peers(b, lambda p: ml2_from(p).wait_recv())
    rml2[b] = packed
    row_even = b - c * (b - lax.div(b, 2))
    row_odd = row_even + 4 * c
    even = lax.rem(lanes((1, 128)), 2) == 0
    each_ml = jnp.concatenate(
        [
            jnp.where(even, rml2[p, pl.ds(row_even, 1), :], rml2[p, pl.ds(row_odd, 1), :])
            for p in range(SIDE)
        ],
        axis=0,
    )
    factor = jnp.exp(each_ml - jnp.max(each_ml, axis=0, keepdims=True))
    total = jnp.sum(factor * pltpu.roll(each_ml, 64, 1), axis=0, keepdims=True)
    factor = jnp.where(lane8 < half, factor / total, 0.0)
    factor = jnp.concatenate([factor, jnp.zeros((120, 128), F32)], axis=0).T
    factors = [jnp.broadcast_to(factor[0:ROWS, p : p + 1], (ROWS, 128)) for p in range(SIDE)]
    for copy in w_in:
        copy.wait_recv()
    w_across.start()
    peers(b, lambda p: o2_from(p).wait_recv())
    r2[b] = s2[b]
    merged = twice(factors[0]) * r2[0].astype(F32)
    for p in range(1, SIDE):
        merged = merged + twice(factors[p]) * r2[p].astype(F32)

    part = jnp.zeros((ROWS, VD), F32)
    for k in range(2):
        block = merged[ROWS * k : ROWS * (k + 1)]
        high = block.astype(BF16)
        low = (block - high.astype(F32)).astype(BF16)
        part = part + jnp.dot(high, vu[k], preferred_element_type=F32)
        part = part + jnp.dot(low, vu[k], preferred_element_type=F32)
    to_partner[3].wait_recv()
    w_across.wait_recv()
    left = jnp.concatenate([part.astype(BF16), lhs[...].astype(BF16)], axis=1)

    def part_rows(j):
        sizes = [padded(CUTS[k + 1] - CUTS[k], half) for k in range(2)]
        return pl.ds(sum(sizes[:j]), sizes[j])

    def a1_send(j, p):
        rows = part_rows(j)
        return rcopy(s3.at[p, rows], r3.at[a, rows], A1 + j, p, a, first(p))

    def a1_from(j, p):
        rows = part_rows(j)
        return rcopy(s3.at[p, rows], r3.at[p, rows], A1 + j, p, p, first(p))

    def a2_send(j, p):
        rows = part_rows(j)
        return rcopy(s4.at[rows], r4.at[b, rows], A2 + j, p, b, second(p))

    def a2_from(j, p):
        rows = part_rows(j)
        return rcopy(s4.at[rows], r4.at[p, rows], A2 + j, p, p, second(p))

    def a3_send(j, p):
        rows = part_rows(j)
        return rcopy(rf.at[a, rows], rf.at[a, rows], A3 + j, p, a, first(p))

    def a3_from(j, p):
        rows = part_rows(j)
        return rcopy(rf.at[p, rows], rf.at[p, rows], A3 + j, p, p, first(p))

    def in_step(k):
        pl.semaphore_signal(steps.at[k], inc=1, device_id=partner, device_id_type=MESH)
        pl.semaphore_wait(steps.at[k], 1)

    def project(j, p):
        out = jnp.dot(left, w[p, :, 128 * CUTS[j] : 128 * CUTS[j + 1]], preferred_element_type=F32)
        count = CUTS[j + 1] - CUTS[j]
        blocks = [out[:half, 128 * t : 128 * t + 128] for t in range(count)]
        blocks += [out[half : half + 1, 128 * t : 128 * t + 128] for t in range(count)]
        blocks.append(jnp.zeros((padded(count, half) - count * (half + 1), 128), F32))
        s3[p, part_rows(j), :] = jnp.concatenate(blocks, axis=0).astype(BF16)

    def total_of(ref, j):
        total = ref[0, part_rows(j), :].astype(F32)
        for p in range(1, SIDE):
            total = total + ref[p, part_rows(j), :].astype(F32)
        return total.astype(BF16)

    in_step(0)
    for j in range(2):

        for batch in ((4, 3, 5), (2, 6, 1, 7)):
            for d in batch:
                project(j, at(a, d))
            for d in batch:
                a1_send(j, at(a, d)).start()
    for j in range(2):
        project(j, a)
    for j in range(2):
        peers(a, lambda p: a1_from(j, p).wait_recv())
        r3[a, part_rows(j), :] = s3[a, part_rows(j), :]
        s4[part_rows(j), :] = total_of(r3, j)
        peers(b, lambda p: a2_send(j, p).start())
    peers(a, lambda p: q1(p).wait_send())
    loop(SIDE, lambda p: q1_across(p).wait_send())
    for p in range(parts):
        k_copy(p).wait_send()
    for d in range(SIDE):
        chunk = at(a, d)
        for slot in range(1, SIDE) if d in DIRECT else (1, 2, 3, 5, 6, 7, 4 if d % 2 == 0 else 0):
            q2(slot, b, chunk, at(b, 1)).wait_send()
    for i in range(PARTS):
        peers(a, lambda p: mlsend(i, p).wait_send())
    for i in range(PARTS):
        peers(a, lambda p: osend(i, p).wait_send())
    peers(b, lambda p: ml2_send(p).wait_send())
    peers(b, lambda p: o2_send(p).wait_send())
    for copy in to_partner + w_out + [w_across]:
        copy.wait_send()
    for j in range(2):
        peers(b, lambda p: a2_from(j, p).wait_recv())
        r4[b, part_rows(j), :] = s4[part_rows(j), :]
        rf[a, part_rows(j), :] = total_of(r4, j)
        peers(a, lambda p: a3_send(j, p).start())
    for j in range(2):
        peers(a, lambda p: a1_send(j, p).wait_send())
        peers(b, lambda p: a2_send(j, p).wait_send())
    for j in range(2):
        peers(a, lambda p: a3_from(j, p).wait_recv())

    choose = pick[...][:, 0:half]
    choose_b = choose.astype(BF16)
    squares = jnp.zeros((half, 128), F32)
    largest = jnp.zeros((half, 128), F32)
    for p in range(SIDE):
        parts_r = []
        gains = []
        for j in range(2):
            block = rf[p, part_rows(j), :].astype(F32)
            count = CUTS[j + 1] - CUTS[j]
            parts_r += [block[half * t : half * (t + 1)] for t in range(count)]
            gains += [block[half * count + t : half * count + t + 1] for t in range(count)]
        for v, gv in zip(parts_r, gains):
            squares = squares + v * v
            largest = jnp.maximum(largest, jnp.abs(v * gv))
        rows = jnp.concatenate(parts_r, axis=1).astype(BF16)
        chosen = jnp.dot(choose_b, rows, preferred_element_type=F32)
        y[p] = chosen * jnp.concatenate(gains, axis=1)
    inverse = lax.rsqrt(jnp.sum(squares, axis=1, keepdims=True) / cols + small_eps)
    peak = inverse * jnp.max(largest, axis=1, keepdims=True) + small_eps
    spread = jnp.concatenate(
        [jnp.broadcast_to(inverse / peak, (half, 128)), jnp.broadcast_to(peak, (half, 128))], axis=1
    )
    slots = jnp.dot(choose, spread, preferred_element_type=F32, precision=lax.Precision.HIGHEST)
    code = jnp.concatenate([slots[:, 0:128]] * tiles, axis=1)
    peaks = slots[:, 128:256]
    xs[...] = peaks[8:16]
    for k in range(SIDE // 2):
        fs[k] = jnp.concatenate(
            [y[2 * k + d, 8:16, :] * code[8:16] for d in range(2)], axis=0
        ).astype(BF16)
    x_partner = dcopy(xs, xr, D_X, partner)
    f_partner = dcopy(fs, fr, D_F, partner)
    x_partner.start()
    f_partner.start()
    x_partner.wait_recv()
    peaks = peaks[0:8] + xr[...]
    scale_slots = jnp.zeros((2, CAP), F32)
    for j in range(2):
        for k in range(CAP):
            here = (sublanes((2, CAP)) == j) & (lanes((2, CAP)) == k)
            r = CAP * j + k
            scale_slots = jnp.where(here, peaks[r : r + 1, 0:1], scale_slots)
    scale_out[...] = scale_slots
    f_partner.wait_recv()
    for k in range(SIDE // 2):
        there = fr[k].astype(F32)
        for d in range(2):
            p = 2 * k + d
            rows = (y[p, 0:8, :] * code[0:8] + there[8 * d : 8 * d + 8]).astype(BF16)
            for e in range(2):
                disp_out[e, :, pl.ds(p * width, width)] = rows[CAP * e : CAP * e + CAP]

    for j in range(2):
        peers(a, lambda p: a3_send(j, p).wait_send())
    x_partner.wait_send()
    f_partner.wait_send()


def per_device(
    queries, latent_cache, context_lengths, value_up, out_proj, residual, norm_gain, expert_ids,
    gate_weights,
):
    seqs, ctx_dev, entry = latent_cache.shape
    half = seqs // 2
    columns = out_proj.shape[1]
    width = columns // SIDE
    piece = residual.shape[1]
    experts = 2
    rows = sum(padded(CUTS[k + 1] - CUTS[k], half) for k in range(2))
    any_space = pl.BlockSpec(memory_space=pl.ANY)
    vmem = pl.BlockSpec(memory_space=pltpu.VMEM)
    V = pltpu.VMEM
    chunk = (PARTS, SIDE, half // PARTS, 16, 128)
    eights = (SIDE, 8, 128)
    scratch = [
        V(queries.shape, BF16),
        V((seqs, 128), F32),
        V((seqs, 128), F32),
        V((ROWS, 128), BF16),
        V((SIDE, SIDE, 2, ROWS, 128), BF16),
        V((SIDE * A_GROUP, 128), F32),
        V((2, half, entry, ctx_dev), BF16),
        V((half, H, 2 * ctx_dev), BF16),
        V(chunk, BF16),
        V(chunk, BF16),
        V((PARTS,) + eights, F32),
        V((PARTS,) + eights, F32),
        V((8, 128), F32),
        V(eights, F32),
        V(eights, F32),
        V((SIDE, half // PARTS, 8, 128), F32),
        V((half, 16, 128), F32),
        V((384, 128), F32),
        V((SIDE, 2 * ROWS, 128), BF16),
        V((SIDE, 2 * ROWS, 128), BF16),
        V((2, 128, VD), BF16),
        V((2, seqs, piece), BF16),
        V((2, 1, piece), BF16),
        V((seqs + 8, 128), F32),
        V((seqs + 8, 128), F32),
        V((ROWS, 128), F32),
        V((SIDE, 256, width), BF16),
        V((SIDE, rows, 128), BF16),
        V((SIDE, rows, 128), BF16),
        V((rows, 128), BF16),
        V((SIDE, rows, 128), BF16),
        V((SIDE, rows, 128), BF16),
        V(expert_ids.shape[::-1], jnp.int32),
        V(gate_weights.shape[::-1], F32),
        V((16, 128), F32),
        V((16, 128), F32),
        V((SIDE, 16, width), F32),
        V((SIDE // 2, 16, width), BF16),
        V((SIDE // 2, 16, width), BF16),
        V((8, 128), F32),
        V((8, 128), F32),
        pltpu.SMEM(context_lengths.shape, jnp.int32),
        pltpu.SemaphoreType.DMA((25,)),
        pltpu.SemaphoreType.DMA((PHASES, SIDE)),
        pltpu.SemaphoreType.DMA((PHASES, SIDE)),
        pltpu.SemaphoreType.DMA((SIDE, SIDE)),
        pltpu.SemaphoreType.DMA((SIDE, SIDE)),
        pltpu.SemaphoreType.DMA((half // 2,)),
        pltpu.SemaphoreType.DMA((half // 2,)),
        pltpu.SemaphoreType.DMA((9,)),
        pltpu.SemaphoreType.DMA((9,)),
        pltpu.SemaphoreType.REGULAR((1,)),
    ]
    dispatched, slot_scale, slot_gate = pl.pallas_call(
        kernel,
        out_shape=(
            jax.ShapeDtypeStruct((experts, CAP, columns), BF16),
            jax.ShapeDtypeStruct((experts, CAP), F32),
            jax.ShapeDtypeStruct((experts, CAP), F32),
        ),
        in_specs=[any_space] * 9,
        out_specs=(vmem, vmem, vmem),
        scratch_shapes=scratch,
        compiler_params=pltpu.CompilerParams(collective_id=0, has_side_effects=True),
    )(
        queries, latent_cache.transpose(0, 2, 1), context_lengths, value_up, out_proj, residual,
        norm_gain[None, :], expert_ids.T, gate_weights.T,
    )
    def hand_over(*refs):
        for source, target in zip(refs[:3], refs[3:]):
            target[...] = source[...]

    results = (dispatched, slot_scale, slot_gate)
    return pl.pallas_call(
        hand_over,
        out_shape=tuple(jax.ShapeDtypeStruct(r.shape, r.dtype) for r in results),
        in_specs=[vmem] * 3,
        out_specs=(vmem,) * 3,
    )(*results)


def solution(mesh):
    split = Mesh(
        mesh.devices.reshape(mesh.shape["groups"], SIDE, SIDE, 2),
        ("groups", "kv_0", "kv_1", "kv_2"),
    )
    in_specs = (
        P("groups", KV),
        P("groups", KV, None),
        P("groups"),
        P(KV, None),
        P(KV, None),
        P("groups", KV),
        P(KV),
        P("groups", None),
        P("groups", None),
    )
    out_specs = (P(GROUPS_KV, None, None), P(GROUPS_KV, None), P(GROUPS_KV, None))
    return jax.shard_map(
        per_device, mesh=split, in_specs=in_specs, out_specs=out_specs, check_vma=False
    )
```
